128 devices in a mesh: seq: 16 (over y, x), ctx: 8 (over z, core).
Axes of the slice: x: 4, y: 4, z: 4, core: 2. Of those that a mesh axis runs over, the one named last changes fastest.
Arguments:
- tokens: bfloat16 [16384, 4096], P(('seq', 'ctx')), may hold values from -30 to 30
- modality: int32 [16384], P(('seq', 'ctx')), may hold values from 0 to 1, as said below
- keep_mask: int32 [16384], P(('seq', 'ctx')), may hold values from 0 to 1, as said below
- positions: int32 [16384], P(('seq', 'ctx')), may hold values from 0 to 16383
- modal_table: float32 [2, 4096], replicated, may hold values from -3 to 3
- norm_gain: float32 [4096], replicated, may hold values from 0.1 to 1.9
- norm_bias: float32 [4096], replicated, may hold values from -3 to 3
- qkv_weight: bfloat16 [3, 4096, 4096], P(None, None, 'seq'), may hold values from -1 to 1
- out_weight: bfloat16 [4096, 4096], P('seq'), may hold values from -0.09375 to 0.09375
- mask_token: float32 [4096], replicated, may hold values from -4 to 4
Outputs:
- encoded: float32 [16384, 4096], P(('seq', 'ctx'))
The draws below stay inside these ranges and needn't reach their ends.
Inputs may be any that keep to these rules, and one draw needn't show every extreme that they name: `modality`: 0 marks a video token and 1 a taxel token; ids come in aligned runs of 16 tokens; five eighths of the tokens are video, and all tokens of at least one device are taxel. `keep_mask`: exactly 1024 video tokens and 3072 taxel tokens are kept, 4096 in all; on at least one device every token is kept.
All inputs are finite; a program needn't handle non-finite values.
Results may differ from the reference program's by a relative error of at most 0.0075.
Values may be sent and summed in bfloat16 or wider, within the bound.
No kernel may reach another device: no remote copies, remote signals or barrier semaphores. Data moves between devices by JAX's collectives and lax.ppermute only.
A program may use at most 64 MiB of HBM per device.

```python
import math
import jax
import jax.numpy as jnp
from jax import lax

HEADS = 32
HEAD_DIM = 128
D = 4096
TOK_DEV = 128
TOKENS = 16384
VISIBLE = 4096


def clip_layout(key):
    base_key = jax.random.fold_in(key, 5)
    key_dense, key_blocks, key_keep = jax.random.split(base_key, 3)
    blocks = TOKENS // 16
    per_shard = TOK_DEV // 16
    dense = jax.random.randint(key_dense, (), 0, TOKENS // TOK_DEV)
    block_index = jnp.arange(blocks, dtype=jnp.int32)
    in_dense = block_index // per_shard == dense
    order = jax.random.permutation(key_blocks, blocks).astype(jnp.int32)
    block_score = jnp.where(in_dense, -1 - block_index, order)
    block_rank = jnp.argsort(jnp.argsort(-block_score))
    video_block = block_rank < 5 * blocks // 8
    modality = jnp.repeat(jnp.where(video_block, 0, 1).astype(jnp.int32), 16)
    token_index = jnp.arange(TOKENS, dtype=jnp.int32)
    token_order = jax.random.permutation(key_keep, TOKENS).astype(jnp.int32)
    dense_token = token_index // TOK_DEV == dense
    token_score = jnp.where(dense_token, -1 - token_index, token_order)
    composite = modality * (2 * TOKENS) + token_score
    token_rank = jnp.argsort(jnp.argsort(composite))
    video_total = 5 * TOKENS // 8
    chosen = (token_rank < TOKENS // 16) | (token_rank >= video_total) & (token_rank < video_total + 3 * TOKENS // 16)
    return (modality, chosen.astype(jnp.int32))


def draw_modality(key, part):
    return clip_layout(key)[0]


def draw_keep_mask(key, part):
    return clip_layout(key)[1]


def draw_tokens(key, part):
    key_base, key_rows, key_cols = jax.random.split(jax.random.fold_in(key, 11), 3)
    row_scale = jnp.exp(jax.random.uniform(key_rows, (TOKENS, 1), jnp.float32, math.log(0.25), math.log(2.5)))
    col_scale = jnp.exp(jax.random.uniform(key_cols, (1, D), jnp.float32, math.log(0.3), math.log(3.0)))
    values = jnp.clip(jax.random.normal(key_base, (TOKENS, D), jnp.float32), -4.0, 4.0) * row_scale * col_scale
    return values.astype(jnp.bfloat16)


def draw_qkv_weight(key, part):
    key_base = jax.random.fold_in(jax.random.fold_in(key, 23), 0)
    lift = jnp.array([1.3, 1.3, 1.0], jnp.float32).reshape(3, 1, 1)
    values = jnp.clip(jax.random.normal(key_base, (3, D, D), jnp.float32), -4.0, 4.0) * D ** (-0.5) * lift
    return values.astype(jnp.bfloat16)


def with_ends(entries, rng, least, top_value):
    extent = entries.shape
    index_at = [jax.random.randint(jax.random.fold_in(rng, axis), (), 0, extent[axis]) for axis in range(len(extent))]
    entries = entries.at[tuple(index_at)].set(least)
    longest = extent.index(max(extent))
    index_at[longest] = (index_at[longest] + 1) % extent[longest]
    return entries.at[tuple(index_at)].set(top_value)


def level_of(key, shape, cuts, least, largest):
    level, own = 1.0, jax.random.fold_in(key, 6)
    for axis_at, blocks in cuts:
        heights = jnp.exp(jax.random.uniform(jax.random.fold_in(own, axis_at), (blocks,), jnp.float32, least / len(cuts), largest / len(cuts)))
        level = level * jnp.repeat(heights, shape[axis_at] // blocks).reshape([-1 if axis == axis_at else 1 for axis in range(len(shape))])
    return level


def normal_values(rng, dims, scale, most, cuts=(), held_as=jnp.bfloat16):
    factor_of = level_of(rng, dims, cuts, -0.22, 0.18) if cuts else 1.0
    result = jax.random.normal(rng, dims, jnp.float32) * scale * factor_of
    return jnp.minimum(jnp.maximum(result, -most), most).astype(held_as)


def setup_inputs(seed: int = 0) -> dict:
    seeds = jax.random.split(jax.random.key(seed), 11)
    tokens = draw_tokens(jax.random.fold_in(seeds[10], 71), 0)
    modality = draw_modality(jax.random.fold_in(seeds[10], 71), 0)
    keep_mask = draw_keep_mask(jax.random.fold_in(seeds[10], 71), 0)
    positions = with_ends(jax.random.randint(seeds[3], (TOKENS,), 0, TOKENS), jax.random.fold_in(seeds[3], 1), 0, TOKENS - 1).astype(jnp.int32)
    modal_table = normal_values(seeds[4], (2, D), 0.5, 3.0, (), jnp.float32)
    norm_gain = jnp.clip(1.0 + 0.18 * jax.random.normal(seeds[5], (D,), jnp.float32), 0.1, 1.9)
    norm_bias = normal_values(seeds[6], (D,), 0.5, 3.0, (), jnp.float32)
    qkv_weight = draw_qkv_weight(jax.random.fold_in(seeds[10], 71), 0)
    out_weight = normal_values(seeds[8], (D, D), D ** -0.5, 0.09375, ((0, 16),))
    mask_token = normal_values(seeds[9], (D,), 1.0, 4.0, (), jnp.float32)
    return {"tokens": tokens, "modality": modality, "keep_mask": keep_mask, "positions": positions, "modal_table": modal_table, "norm_gain": norm_gain, "norm_bias": norm_bias, "qkv_weight": qkv_weight, "out_weight": out_weight, "mask_token": mask_token}


EPSILON = 1e-06

def position_table(positions, feature_width):
    half_width = feature_width // 2
    frequency = jnp.exp(-math.log(10000.0) * jnp.arange(half_width, dtype=jnp.float32) / half_width)
    angles = positions.astype(jnp.float32)[:, None] * frequency[None, :]
    return jnp.concatenate([jnp.sin(angles), jnp.cos(angles)], axis=1)

def embed(tokens, modality, positions, modal_table):
    table_rows = jnp.where(modality[:, None] == 1, modal_table[1][None, :], modal_table[0][None, :])
    summed = tokens.astype(jnp.float32) + position_table(positions, tokens.shape[1]) + table_rows
    return summed.astype(jnp.bfloat16)

def layer_norm(embedded, norm_gain, norm_bias):
    values = embedded.astype(jnp.float32)
    row_mean = lax.optimization_barrier(jnp.mean(values, axis=1, keepdims=True))
    centered = values - row_mean
    row_var = lax.optimization_barrier(jnp.mean(centered * centered, axis=1, keepdims=True))
    return (centered * lax.rsqrt(row_var + EPSILON) * norm_gain + norm_bias).astype(jnp.bfloat16)

def reference(tokens, modality, keep_mask, positions, modal_table, norm_gain, norm_bias, qkv_weight, out_weight, mask_token):
    embedded = embed(tokens, modality, positions, modal_table)
    visible = jnp.nonzero(keep_mask == 1, size=VISIBLE, fill_value=0)[0].astype(jnp.int32)
    balanced = embedded[visible]
    normed = layer_norm(balanced, norm_gain, norm_bias)
    triple = jnp.einsum('rd,tdc->trc', normed.astype(jnp.float32), qkv_weight.astype(jnp.float32), precision=lax.Precision.HIGHEST).astype(jnp.bfloat16)
    queries = triple[0].reshape(VISIBLE, HEADS, HEAD_DIM).transpose(1, 0, 2)
    key_rows = triple[1].reshape(VISIBLE, HEADS, HEAD_DIM).transpose(1, 0, 2)
    values = triple[2].reshape(VISIBLE, HEADS, HEAD_DIM).transpose(1, 0, 2)
    score_scale = 1.0 / math.sqrt(HEAD_DIM)

    def one_head(parts):
        query_head, key_head, value_head = parts
        scores = jnp.dot(query_head, key_head.T, preferred_element_type=jnp.float32) * score_scale
        row_top = lax.optimization_barrier(jnp.max(scores, axis=1, keepdims=True))
        expanded = jnp.exp(scores - row_top)
        denominator = lax.optimization_barrier(jnp.sum(expanded, axis=1, keepdims=True))
        weights = expanded.astype(jnp.bfloat16)
        summed = jnp.dot(weights, value_head, preferred_element_type=jnp.float32)
        return (summed / denominator).astype(jnp.bfloat16)
    attended = lax.map(one_head, (queries, key_rows, values))
    attended = attended.transpose(1, 0, 2).reshape(VISIBLE, D)
    projected = jnp.dot(attended, out_weight, preferred_element_type=jnp.float32)
    finished = balanced.astype(jnp.float32) + projected
    filler = jnp.broadcast_to(mask_token[None, :], (TOKENS, D)).astype(jnp.float32)
    return filler.at[visible].set(finished)
```

```python
import math

import jax
import jax.numpy as jnp
from jax import lax
from jax.experimental import pallas as pl
from jax.experimental.pallas import tpu as pltpu
from jax.sharding import PartitionSpec as P

HEAD_DIM = 128
EPSILON = 1e-06
SIDE = 4
MIB = 1 << 20


def y_shift(d):
    return [(y * SIDE + x, (y + d) % SIDE * SIDE + x) for y in range(SIDE) for x in range(SIDE)]


def x_shift(d):
    return [(y * SIDE + x, y * SIDE + (x + d) % SIDE) for y in range(SIDE) for x in range(SIDE)]


def z_shift(d):
    return [(z * 2 + k, (z + d) % SIDE * 2 + k) for z in range(SIDE) for k in range(2)]


CORE_SWAP = [(z * 2 + k, z * 2 + 1 - k) for z in range(SIDE) for k in range(2)]


def ring_of_four(block, axis, shift):
    behind = lax.ppermute(block, axis, shift(1))
    ahead = lax.ppermute(block, axis, shift(-1))
    half = block.shape[0] // 2
    far_top = lax.ppermute(behind[:half], axis, shift(1))
    far_bottom = lax.ppermute(ahead[half:], axis, shift(-1))
    return block, ahead, (far_top, far_bottom), behind


def gather_plane(block):
    half = block.shape[0] // 2
    chunks = []
    for part, first, second in (
        (block[:half], y_shift, x_shift),
        (block[half:], x_shift, y_shift),
    ):
        own, ahead, far, behind = ring_of_four(part, "seq", first)
        line = jnp.concatenate([own, ahead, jnp.concatenate(far, axis=0), behind], axis=1)
        own, ahead, far, behind = ring_of_four(line, "seq", second)
        chunks += [own, ahead, *far, behind]
    return chunks


def call(body, outs, *args, scratch=(), limit=40, flops=0, in_specs=None):
    vmem = pl.BlockSpec(memory_space=pltpu.VMEM)
    many = isinstance(outs, (tuple, list))
    return pl.pallas_call(
        body,
        out_shape=outs,
        in_specs=in_specs,
        out_specs=[vmem] * len(outs) if many else vmem,
        scratch_shapes=list(scratch),
        compiler_params=pltpu.CompilerParams(vmem_limit_bytes=limit * MIB),
        cost_estimate=pl.CostEstimate(
            flops=flops, transcendentals=0, bytes_accessed=sum(a.size * 2 for a in args)
        ),
    )(*args)


VMEM = pl.BlockSpec(memory_space=pltpu.VMEM)
SMEM = pl.BlockSpec(memory_space=pltpu.SMEM)
ANY = pl.BlockSpec(memory_space=pl.ANY)


def dot(a, b, dims=((1,), (0,))):
    return lax.dot_general(a, b, (dims, ((), ())), preferred_element_type=jnp.float32)


def iota(shape, dim):
    return lax.broadcasted_iota(jnp.int32, shape, dim)


def as_bf16(flag):
    return jnp.where(flag, 1.0, 0.0).astype(jnp.bfloat16)


def counts_in_lanes(masks):
    return dot(jnp.ones((8, masks.shape[1]), jnp.bfloat16), masks, ((1,), (1,)))


def dispatch_body(where_ref, masks_ref, own_ref, normed_ref, out_ref, pick_ref):
    tokens = own_ref.shape[1]
    masks = masks_ref[...].astype(jnp.float32).astype(jnp.bfloat16)
    counts = counts_in_lanes(masks)[0:1]
    start = jnp.sum(
        jnp.where(iota(counts.shape, 1) < where_ref[0], counts, 0.0), axis=1, keepdims=True
    ).astype(jnp.int32)
    own = own_ref[...]
    wide = jnp.broadcast_to(own.astype(jnp.float32).astype(jnp.bfloat16), (8, tokens))
    upto = as_bf16(iota((tokens, tokens), 0) <= iota((tokens, tokens), 1))
    rank = dot(wide, upto)[0:1].astype(jnp.int32) - 1
    slot = ((start + rank) & 7) * (tokens // 8) + (rank >> 3)
    slot = jnp.where(own == 1, slot, -1)
    pick = as_bf16(iota((tokens, tokens), 0) == slot)
    pick_ref[...] = pick
    width = out_ref.shape[2]
    for s in range(out_ref.shape[0]):
        out_ref[s] = dot(pick, normed_ref[:, s * width : (s + 1) * width]).astype(jnp.bfloat16)


def compact_body(where_ref, masks_ref, arrived_ref, out_ref):
    devices = masks_ref.shape[0]
    slots = arrived_ref.shape[0]
    per = slots // devices
    masks = masks_ref[...].astype(jnp.float32).astype(jnp.bfloat16)
    counts = counts_in_lanes(masks).astype(jnp.bfloat16)
    sender = iota((devices, slots), 1) // per
    device = iota((devices, slots), 0)
    start = dot(counts, as_bf16(device < sender))[0:1].astype(jnp.int32)
    count = dot(counts, as_bf16(device == sender))[0:1].astype(jnp.int32)
    offset = ((where_ref[1] - start) & 7) + 8 * (iota((1, slots), 1) % per)
    row = jnp.where(offset < count, (start + offset) >> 3, -1)
    arrived = arrived_ref[...]
    for r in range(0, out_ref.shape[0], 128):
        pick = as_bf16(iota((128, slots), 0) + r == row)
        out_ref[r : r + 128] = dot(pick, arrived).astype(jnp.bfloat16)


def side_by_side(chunk_refs, all_ref, width):
    half = all_ref.shape[0] // 2
    quarter = half // 2
    rows = (
        (0, half),
        (0, half),
        (0, quarter),
        (quarter, half),
        (0, half),
    )
    ring = (0, 1, 2, 2, 3)
    for part in range(2):
        for piece in range(5):
            ref = chunk_refs[part * 5 + piece]
            first, last = rows[piece]
            for inner in range(SIDE):
                x, y = (ring[piece], inner) if part == 0 else (inner, ring[piece])
                at = (x * SIDE + y) * width
                all_ref[part * half + first : part * half + last, at : at + width] = ref[
                    :, inner * width : (inner + 1) * width
                ]


def weight_block(where_ref, i):
    y = (where_ref[2] + i % SIDE) % SIDE
    x = (where_ref[3] + i // SIDE) % SIDE
    return y * SIDE + x


def qkv_body(where_ref, weight_ref, *refs):
    chunk_refs, (mine_ref, other_ref, all_ref, w_ref, sems) = refs[:10], refs[10:]
    width = w_ref.shape[2]
    copies = []
    for i in range(SIDE * SIDE):
        at = pl.multiple_of(weight_block(where_ref, i) * width, width)
        copies.append(
            pltpu.make_async_copy(
                weight_ref.at[:, pl.ds(at, width), :],
                w_ref.at[:, i * width : (i + 1) * width, :],
                sems.at[i],
            )
        )
        copies[-1].start()
    side_by_side(chunk_refs, all_ref, width)
    for copy in copies:
        copy.wait()
    second = where_ref[4] == 1
    for t in range(3):
        both = dot(all_ref[...], w_ref[t]).astype(jnp.bfloat16)
        left, right = both[:, :HEAD_DIM], both[:, HEAD_DIM:]
        cols = slice(t * HEAD_DIM, (t + 1) * HEAD_DIM)
        mine_ref[:, cols] = jnp.where(second, right, left)
        other_ref[:, cols] = jnp.where(second, left, right)


def attend_body(has_state, is_last, keys, q_ref, *refs):
    kv_refs, refs = refs[:keys], refs[keys:]
    q = q_ref[...]
    scale = math.log2(math.e) / math.sqrt(HEAD_DIM)
    if has_state:
        acc, top, total = (r[...] for r in refs[:3])
        top, total = top[:, 0:1], total[:, 0:1]
        refs = refs[3:]
    for i, kv_ref in enumerate(kv_refs):
        scores = dot(q, kv_ref[:, :HEAD_DIM], ((1,), (1,)))
        block_top = jnp.max(scores, axis=1, keepdims=True)
        first = not has_state and i == 0
        new_top = block_top if first else jnp.maximum(top, block_top)
        expanded = jnp.exp2((scores - new_top) * scale)
        block_total = jnp.sum(expanded, axis=1, keepdims=True)
        product = dot(expanded.astype(jnp.bfloat16), kv_ref[:, HEAD_DIM:])
        if first:
            acc, total = product, block_total
        else:
            factor = jnp.exp2((top - new_top) * scale)
            acc = acc * factor + product
            total = total * factor + block_total
        top = new_top
    if is_last:
        refs[0][...] = (acc / total).astype(jnp.bfloat16)
    else:
        refs[0][...] = acc
        refs[1][...] = jnp.broadcast_to(top, acc.shape)
        refs[2][...] = jnp.broadcast_to(total, acc.shape)


def attend(q, kv_blocks, state, is_last):
    rows = q.shape[0]
    tile = 256
    state = tuple(state or ())
    spec = pl.BlockSpec((tile, HEAD_DIM), lambda i: (i, 0))
    kv_specs = [pl.BlockSpec(b.shape, lambda i: (0, 0)) for b in kv_blocks]
    key_rows = sum(b.shape[0] for b in kv_blocks)
    out = jax.ShapeDtypeStruct((rows, HEAD_DIM), jnp.bfloat16 if is_last else jnp.float32)
    return pl.pallas_call(
        lambda *refs: attend_body(bool(state), is_last, len(kv_blocks), *refs),
        grid=(rows // tile,),
        out_shape=out if is_last else (out, out, out),
        in_specs=[spec, *kv_specs, *[spec for _ in state]],
        out_specs=spec if is_last else (spec, spec, spec),
        compiler_params=pltpu.CompilerParams(vmem_limit_bytes=32 * MIB),
        cost_estimate=pl.CostEstimate(
            flops=8 * rows * key_rows * HEAD_DIM,
            transcendentals=rows * key_rows,
            bytes_accessed=key_rows * 512,
        ),
    )(q, *kv_blocks, *state)


def project_body(where_ref, masks_ref, weight_ref, *refs):
    chunk_refs, (out_ref, all_ref, w_ref, sems) = refs[:10], refs[10:]
    width = w_ref.shape[1]
    copies = []
    for i in range(SIDE * SIDE):
        at = pl.multiple_of(weight_block(where_ref, i) * width, width)
        copies.append(
            pltpu.make_async_copy(
                weight_ref.at[pl.ds(at, width), :],
                w_ref.at[i * width : (i + 1) * width, :],
                sems.at[i],
            )
        )
        copies[-1].start()
    side_by_side(chunk_refs, all_ref, width)
    devices = masks_ref.shape[0]
    slots = out_ref.shape[0]
    per = slots // devices
    masks = masks_ref[...].astype(jnp.float32).astype(jnp.bfloat16)
    counts = dot(masks, jnp.ones((devices, 128), jnp.bfloat16)).astype(jnp.bfloat16)
    sender = iota((slots, devices), 0) // per
    device = iota((slots, devices), 1)
    start = dot(as_bf16(device < sender), counts).astype(jnp.int32)
    count = dot(as_bf16(device == sender), counts).astype(jnp.int32)
    offset = ((where_ref[1] - start) & 7) + 8 * (iota((slots, 128), 0) % per)
    row = jnp.where(offset < count, (start + offset) >> 3, -1)
    rows = all_ref.shape[0]
    picks = [as_bf16(row == iota((slots, 128), 1) + r) for r in range(0, rows, 128)]
    pick = jnp.concatenate(picks, axis=1)
    for copy in copies:
        copy.wait()
    projected = dot(all_ref[...], w_ref[...]).astype(jnp.bfloat16)
    out_ref[...] = dot(pick, projected).astype(jnp.bfloat16)


def finish_body(pick_ref, returned_ref, embedded_ref, filler_ref, out_ref):
    pick = pick_ref[...]
    width = returned_ref.shape[2]
    kept = dot(pick, jnp.ones((pick.shape[0], width), jnp.bfloat16), ((0,), (0,))) > 0.5
    for s in range(returned_ref.shape[0]):
        cols = slice(s * width, (s + 1) * width)
        projected = dot(pick, returned_ref[s], ((0,), (0,)))
        finished = embedded_ref[:, cols].astype(jnp.float32) + projected
        out_ref[:, cols] = jnp.where(kept, finished, filler_ref[:, cols])


def position_table(positions, feature_width):
    half_width = feature_width // 2
    frequency = jnp.exp(-math.log(10000.0) * jnp.arange(half_width, dtype=jnp.float32) / half_width)
    angles = positions.astype(jnp.float32)[:, None] * frequency[None, :]
    return jnp.concatenate([jnp.sin(angles), jnp.cos(angles)], axis=1)


def embed(tokens, modality, positions, modal_table):
    table_rows = jnp.where(modality[:, None] == 1, modal_table[1][None, :], modal_table[0][None, :])
    summed = tokens.astype(jnp.float32) + position_table(positions, tokens.shape[1]) + table_rows
    return summed.astype(jnp.bfloat16)


def layer_norm(embedded, norm_gain, norm_bias):
    values = embedded.astype(jnp.float32)
    row_mean = jnp.mean(values, axis=1, keepdims=True)
    centered = values - row_mean
    row_var = jnp.mean(centered * centered, axis=1, keepdims=True)
    return (centered * lax.rsqrt(row_var + EPSILON) * norm_gain + norm_bias).astype(jnp.bfloat16)


def local(
    tokens,
    modality,
    keep_mask,
    positions,
    modal_table,
    norm_gain,
    norm_bias,
    qkv_weight,
    out_weight,
    mask_token,
):
    tok_rows, feature_width = tokens.shape
    seq_count = lax.axis_size("seq")
    ctx_count = lax.axis_size("ctx")
    devices = seq_count * ctx_count
    everyone = ("seq", "ctx")
    seq, ctx = lax.axis_index("seq"), lax.axis_index("ctx")
    core = ctx % 2
    where = jnp.stack([seq * ctx_count + ctx, ctx, seq // SIDE, seq % SIDE, core]).astype(jnp.int32)
    group_rows = tok_rows * seq_count // 4
    width = feature_width // seq_count
    per = tok_rows // ctx_count
    bf16 = lambda *shape: jax.ShapeDtypeStruct(shape, jnp.bfloat16)

    masks = lax.all_to_all(
        jnp.broadcast_to(keep_mask[None, :], (devices, tok_rows)), everyone, 0, 0, tiled=True
    )
    embedded = embed(tokens, modality, positions, modal_table)
    normed = layer_norm(embedded, norm_gain, norm_bias)
    outgoing, pick = call(
        dispatch_body,
        (bf16(seq_count, tok_rows, width), bf16(tok_rows, tok_rows)),
        where,
        masks,
        keep_mask[None, :],
        normed,
        in_specs=[SMEM, VMEM, VMEM, VMEM],
        flops=2 * tok_rows * tok_rows * feature_width,
    )
    arrived = lax.all_to_all(outgoing.reshape(devices, per, width), everyone, 0, 0, tiled=True)
    block = call(
        compact_body,
        bf16(group_rows, width),
        where,
        masks,
        arrived.reshape(devices * per, width),
        in_specs=[SMEM, VMEM, VMEM],
        flops=2 * group_rows * devices * per * width,
    )
    chunks = gather_plane(block)
    mine, other = call(
        qkv_body,
        (bf16(group_rows, 3 * HEAD_DIM), bf16(group_rows, 3 * HEAD_DIM)),
        where,
        qkv_weight,
        *chunks,
        in_specs=[SMEM, ANY, *[VMEM] * 10],
        scratch=(
            pltpu.VMEM((group_rows, feature_width), jnp.bfloat16),
            pltpu.VMEM(qkv_weight.shape, jnp.bfloat16),
            pltpu.SemaphoreType.DMA((SIDE * SIDE,)),
        ),
        flops=6 * group_rows * feature_width * width,
    )
    weight_columns = jnp.moveaxis(
        out_weight.reshape(out_weight.shape[0], seq_count, width), 1, 0
    )
    weight_columns = lax.all_to_all(weight_columns, "seq", 0, 0, tiled=True)
    weight_columns = weight_columns.reshape(feature_width, width)

    theirs = lax.ppermute(other, "ctx", CORE_SWAP)
    both = jnp.concatenate([mine, theirs], axis=0)
    q, kv = both[:, :HEAD_DIM], both[:, HEAD_DIM:]
    own, ahead, far, behind = ring_of_four(kv, "ctx", z_shift)
    state = attend(q, [own], None, False)
    state = attend(q, [ahead, behind], state, False)
    attended = attend(q, list(far), state, True)
    from_other = lax.ppermute(attended[group_rows:], "ctx", CORE_SWAP)
    own_head = attended[:group_rows]
    attended = jnp.where(
        core == 0,
        jnp.concatenate([own_head, from_other], axis=1),
        jnp.concatenate([from_other, own_head], axis=1),
    )
    chunks = gather_plane(attended)
    returning = call(
        project_body,
        bf16(devices * per, width),
        where,
        masks,
        weight_columns,
        *chunks,
        in_specs=[SMEM, VMEM, ANY, *[VMEM] * 10],
        scratch=(
            pltpu.VMEM((group_rows, feature_width), jnp.bfloat16),
            pltpu.VMEM((feature_width, width), jnp.bfloat16),
            pltpu.SemaphoreType.DMA((SIDE * SIDE,)),
        ),
        flops=2 * group_rows * feature_width * width,
    )
    returned = lax.all_to_all(returning.reshape(devices, per, width), everyone, 0, 0, tiled=True)
    return call(
        finish_body,
        jax.ShapeDtypeStruct((tok_rows, feature_width), jnp.float32),
        pick,
        returned.reshape(seq_count, tok_rows, width),
        embedded,
        mask_token[None, :],
        in_specs=[VMEM] * 4,
        flops=2 * tok_rows * tok_rows * feature_width,
    )


def solution(mesh):
    in_specs = (
        P(("seq", "ctx"), None),
        P(("seq", "ctx")),
        P(("seq", "ctx")),
        P(("seq", "ctx")),
        P(),
        P(),
        P(),
        P(None, None, "seq"),
        P("seq", None),
        P(),
    )
    out_specs = P(("seq", "ctx"), None)
    return jax.shard_map(local, mesh=mesh, in_specs=in_specs, out_specs=out_specs, check_vma=False)
```

```python
import math

import jax
import jax.numpy as jnp
from jax import lax
from jax.experimental import pallas as pl
from jax.experimental.pallas import tpu as pltpu
from jax.sharding import PartitionSpec as P

HEAD_DIM = 128
EPSILON = 1e-06
SIDE = 4
MIB = 1 << 20


def y_shift(d):
    return [(y * SIDE + x, (y + d) % SIDE * SIDE + x) for y in range(SIDE) for x in range(SIDE)]


def x_shift(d):
    return [(y * SIDE + x, y * SIDE + (x + d) % SIDE) for y in range(SIDE) for x in range(SIDE)]


def z_shift(d):
    return [(z * 2 + k, (z + d) % SIDE * 2 + k) for z in range(SIDE) for k in range(2)]


CORE_SWAP = [(z * 2 + k, z * 2 + 1 - k) for z in range(SIDE) for k in range(2)]


def ring_of_four(top, bottom, axis, shift):
    behind_top = lax.ppermute(top, axis, shift(1))
    ahead_bottom = lax.ppermute(bottom, axis, shift(-1))
    behind_bottom = lax.ppermute(bottom, axis, shift(1))
    ahead_top = lax.ppermute(top, axis, shift(-1))
    far_top = lax.ppermute(behind_top, axis, shift(1))
    far_bottom = lax.ppermute(ahead_bottom, axis, shift(-1))
    return (
        (top, bottom),
        (ahead_top, ahead_bottom),
        (far_top, far_bottom),
        (behind_top, behind_bottom),
    )


RING = (0, 1, 3, 2)
ORDERS = ((y_shift, x_shift), (x_shift, y_shift))


def gather_line(block, shift):
    return [block] + [lax.ppermute(block, "seq", shift(-d)) for d in RING[1:]]


def gather_plane(parts):
    lines = [
        jnp.concatenate(gather_line(part, first), axis=1) for part, (first, _) in zip(parts, ORDERS)
    ]
    return [gather_line(line, second) for line, (_, second) in zip(lines, ORDERS)]


def scatter_line(blocks, shift):
    return [blocks[0]] + [
        lax.ppermute(block, "seq", shift(d)) for d, block in zip(RING[1:], blocks[1:])
    ]


def call(body, outs, *args, scratch=(), limit=16, flops=0, in_specs=None):
    vmem = pl.BlockSpec(memory_space=pltpu.VMEM)
    many = isinstance(outs, (tuple, list))
    return pl.pallas_call(
        body,
        out_shape=outs,
        in_specs=in_specs,
        out_specs=[vmem] * len(outs) if many else vmem,
        scratch_shapes=list(scratch),
        compiler_params=pltpu.CompilerParams(vmem_limit_bytes=limit * MIB),
        cost_estimate=pl.CostEstimate(
            flops=flops, transcendentals=0, bytes_accessed=sum(a.size * 2 for a in args)
        ),
    )(*args)


VMEM = pl.BlockSpec(memory_space=pltpu.VMEM)
SMEM = pl.BlockSpec(memory_space=pltpu.SMEM)
ANY = pl.BlockSpec(memory_space=pl.ANY)
HBM = pl.BlockSpec(memory_space=pltpu.HBM)


def dot(a, b, dims=((1,), (0,))):
    return lax.dot_general(a, b, (dims, ((), ())), preferred_element_type=jnp.float32)


def iota(shape, dim):
    return lax.broadcasted_iota(jnp.int32, shape, dim)


def as_bf16(flag):
    return jnp.where(flag, 1.0, 0.0).astype(jnp.bfloat16)


def counts_in_lanes(masks):
    return dot(jnp.ones((8, masks.shape[1]), jnp.bfloat16), masks, ((1,), (1,)))


def dispatch_body(where_ref, masks_ref, own_ref, normed_ref, out_ref, pick_ref):
    tokens = own_ref.shape[1]
    masks = masks_ref[...].astype(jnp.float32).astype(jnp.bfloat16)
    counts = counts_in_lanes(masks)[0:1]
    start = jnp.sum(
        jnp.where(iota(counts.shape, 1) < where_ref[0], counts, 0.0), axis=1, keepdims=True
    ).astype(jnp.int32)
    own = own_ref[...]
    wide = jnp.broadcast_to(own.astype(jnp.float32).astype(jnp.bfloat16), (8, tokens))
    upto = as_bf16(iota((tokens, tokens), 0) <= iota((tokens, tokens), 1))
    rank = dot(wide, upto)[0:1].astype(jnp.int32) - 1
    slot = ((start + rank) & 7) * (tokens // 8) + (rank >> 3)
    slot = jnp.where(own == 1, slot, -1)
    pick = as_bf16(iota((tokens, tokens), 0) == slot)
    pick_ref[...] = pick
    width = out_ref.shape[2]
    for s in range(out_ref.shape[0]):
        out_ref[s] = dot(pick, normed_ref[:, s * width : (s + 1) * width]).astype(jnp.bfloat16)


def compact_body(where_ref, masks_ref, arrived_ref, top_ref, bottom_ref):
    devices = masks_ref.shape[0]
    slots = arrived_ref.shape[0]
    per = slots // devices
    masks = masks_ref[...].astype(jnp.float32).astype(jnp.bfloat16)
    counts = counts_in_lanes(masks).astype(jnp.bfloat16)
    sender = iota((devices, slots), 1) // per
    device = iota((devices, slots), 0)
    start = dot(counts, as_bf16(device < sender))[0:1].astype(jnp.int32)
    count = dot(counts, as_bf16(device == sender))[0:1].astype(jnp.int32)
    offset = ((where_ref[1] - start) & 7) + 8 * (iota((1, slots), 1) % per)
    row = jnp.where(offset < count, (start + offset) >> 3, -1)
    arrived = arrived_ref[...]
    half = top_ref.shape[0]
    for r in range(0, 2 * half, 128):
        pick = as_bf16(iota((128, slots), 0) + r == row)
        out_ref = top_ref if r < half else bottom_ref
        out_ref[r % half : r % half + 128] = dot(pick, arrived).astype(jnp.bfloat16)


def plane_block(where_ref, part, outer, inner):
    y, x = (inner, outer) if part == 0 else (outer, inner)
    return (where_ref[2] + RING[y]) % SIDE * SIDE + (where_ref[3] + RING[x]) % SIDE


def reorder_body(where_ref, weight_ref, top_ref, bottom_ref, sems):
    width = weight_ref.shape[2]
    copies = []
    for part, out_ref in enumerate((top_ref, bottom_ref)):
        for outer in range(SIDE):
            for inner in range(SIDE):
                i = outer * SIDE + inner
                at = plane_block(where_ref, part, outer, inner) * width
                copies.append(
                    pltpu.make_async_copy(
                        weight_ref.at[:, pl.ds(pl.multiple_of(at, width), width), :],
                        out_ref.at[:, i * width : (i + 1) * width, :],
                        sems.at[part * SIDE * SIDE + i],
                    )
                )
                copies[-1].start()
    for copy in copies:
        copy.wait()


def qkv_near_body(top_ref, bottom_ref, *refs):
    lines, out_ref = refs[:-1], refs[-1]
    half, long = lines[0].shape
    near = len(lines) // 2
    for part, w_ref in enumerate((top_ref, bottom_ref)):
        for t in range(3):
            total = None
            for i in range(near):
                product = dot(lines[part * near + i][...], w_ref[t, i * long : (i + 1) * long])
                total = product if total is None else total + product
            out_ref[t, part * half : (part + 1) * half] = total


def qkv_far_body(where_ref, near_ref, top_ref, bottom_ref, *refs):
    lines, (my_q, my_kv, other_q, other_kv) = refs[:2], refs[2:]
    half, long = lines[0].shape
    second = where_ref[4] == 1
    for part, w_ref in enumerate((top_ref, bottom_ref)):
        rows = slice(part * half, (part + 1) * half)
        for t in range(3):
            total = near_ref[t, rows] + dot(lines[part][...], w_ref[t, 3 * long :])
            both = total.astype(jnp.bfloat16)
            left, right = both[:, :HEAD_DIM], both[:, HEAD_DIM:]
            mine, other = (my_q, other_q) if t == 0 else (my_kv, other_kv)
            cols = slice(0, HEAD_DIM) if t < 2 else slice(HEAD_DIM, 2 * HEAD_DIM)
            mine[rows, cols] = jnp.where(second, right, left)
            other[rows, cols] = jnp.where(second, left, right)


def attend_body(has_state, is_last, keys, *refs):
    q_refs, kv_refs, refs = refs[:2], refs[2 : 2 + keys], refs[2 + keys :]
    state_refs, out_refs = (refs[:3], refs[3:]) if has_state else ((), refs)
    scale = math.log2(math.e) / math.sqrt(HEAD_DIM)
    rows = q_refs[0].shape[0]
    tile = 256
    per_side = rows // tile

    def one_tile(i):
        at = pl.ds(pl.multiple_of(i * tile, tile), tile)
        here = pl.ds(pl.multiple_of(i % per_side * tile, tile), tile)
        first = i < per_side
        q = jnp.where(first, q_refs[0][here], q_refs[1][here])
        scores = [dot(q, kv_ref[:, :HEAD_DIM], ((1,), (1,))) for kv_ref in kv_refs]
        tops = [jnp.max(s, axis=1, keepdims=True) for s in scores]
        if has_state:
            acc = state_refs[0][at]
            top = state_refs[1][at][:, 0:1]
            total = state_refs[2][at][:, 0:1]
            tops.append(top)
        new_top = tops[0]
        for t in tops[1:]:
            new_top = jnp.maximum(new_top, t)
        product = block_total = None
        for s, kv_ref in zip(scores, kv_refs):
            expanded = jnp.exp2((s - new_top) * scale)
            part_total = jnp.sum(expanded, axis=1, keepdims=True)
            part = dot(expanded.astype(jnp.bfloat16), kv_ref[:, HEAD_DIM:])
            product = part if product is None else product + part
            block_total = part_total if block_total is None else block_total + part_total
        if has_state:
            factor = jnp.exp2((top - new_top) * scale)
            product = acc * factor + product
            block_total = total * factor + block_total
        if is_last:
            result = (product / block_total).astype(jnp.bfloat16)

            @pl.when(first)
            def _():
                out_refs[0][here] = result

            @pl.when(jnp.logical_not(first))
            def _():
                out_refs[1][here] = result
        else:
            out_refs[0][at] = product
            out_refs[1][at] = jnp.broadcast_to(new_top, product.shape)
            out_refs[2][at] = jnp.broadcast_to(block_total, product.shape)

    lax.fori_loop(0, 2 * per_side, lambda i, _: one_tile(i), None)


def attend(q, kv_blocks, state, is_last):
    rows = q[0].shape[0]
    state = tuple(state or ())
    key_rows = sum(b.shape[0] for b in kv_blocks)
    kept = jax.ShapeDtypeStruct((2 * rows, HEAD_DIM), jnp.float32)
    last = jax.ShapeDtypeStruct((rows, HEAD_DIM), jnp.bfloat16)
    return call(
        lambda *refs: attend_body(bool(state), is_last, len(kv_blocks), *refs),
        (last, last) if is_last else (kept, kept, kept),
        *q,
        *kv_blocks,
        *state,
        in_specs=[VMEM] * (2 + len(kv_blocks) + len(state)),
        flops=16 * rows * key_rows * HEAD_DIM,
    )


def return_pick_body(where_ref, masks_ref, pick_ref):
    devices = masks_ref.shape[0]
    slots, rows = pick_ref.shape
    per = slots // devices
    masks = masks_ref[...].astype(jnp.float32).astype(jnp.bfloat16)
    counts = dot(masks, jnp.ones((devices, 128), jnp.bfloat16)).astype(jnp.bfloat16)
    sender = iota((slots, devices), 0) // per
    device = iota((slots, devices), 1)
    start = dot(as_bf16(device < sender), counts).astype(jnp.int32)
    count = dot(as_bf16(device == sender), counts).astype(jnp.int32)
    offset = ((where_ref[1] - start) & 7) + 8 * (iota((slots, 128), 0) % per)
    row = jnp.where(offset < count, (start + offset) >> 3, -1)
    for r in range(0, rows, 128):
        pick_ref[:, r : r + 128] = as_bf16(row == iota((slots, 128), 1) + r)


def partial_body(where_ref, own_ref, other_ref, weight_ref, *out_refs):
    first = where_ref[4] == 0
    own, other = own_ref[...], other_ref[...]
    heads = jnp.concatenate([jnp.where(first, own, other), jnp.where(first, other, own)], axis=1)
    half = heads.shape[0] // 2
    width = out_refs[0].shape[1] // SIDE
    for part in range(2):
        rows = heads[part * half : (part + 1) * half]
        for outer in range(SIDE):
            for inner in range(SIDE):
                at = pl.multiple_of(plane_block(where_ref, part, outer, inner) * width, width)
                product = dot(rows, weight_ref[:, pl.ds(at, width)])
                out_refs[part * SIDE + outer][:, inner * width : (inner + 1) * width] = (
                    product.astype(jnp.bfloat16)
                )


def add_line_body(*refs):
    lines, out_refs = refs[:SIDE], refs[SIDE:]
    width = out_refs[0].shape[1]
    for i, out_ref in enumerate(out_refs):
        cols = slice(i * width, (i + 1) * width)
        a, b, c, d = (line[:, cols].astype(jnp.float32) for line in lines)
        out_ref[...] = ((a + b) + (c + d)).astype(out_ref.dtype)


def send_back_body(pick_ref, *refs):
    blocks, out_ref = refs[:-1], refs[-1]
    parts = []
    for part in range(2):
        a, b, c, d = (r[...].astype(jnp.float32) for r in blocks[part * SIDE : (part + 1) * SIDE])
        parts.append(((a + b) + (c + d)).astype(jnp.bfloat16))
    projected = jnp.concatenate(parts, axis=0)
    out_ref[...] = dot(pick_ref[...], projected).astype(jnp.bfloat16)


def finish_body(pick_ref, returned_ref, embedded_ref, filler_ref, out_ref):
    pick = pick_ref[...]
    width = returned_ref.shape[2]
    kept = dot(pick, jnp.ones((pick.shape[0], width), jnp.bfloat16), ((0,), (0,))) > 0.5
    for s in range(returned_ref.shape[0]):
        cols = slice(s * width, (s + 1) * width)
        projected = dot(pick, returned_ref[s], ((0,), (0,)))
        finished = embedded_ref[:, cols].astype(jnp.float32) + projected
        out_ref[:, cols] = jnp.where(kept, finished, filler_ref[:, cols])


def position_table(positions, feature_width):
    half_width = feature_width // 2
    frequency = jnp.exp(-math.log(10000.0) * jnp.arange(half_width, dtype=jnp.float32) / half_width)
    angles = positions.astype(jnp.float32)[:, None] * frequency[None, :]
    return jnp.concatenate([jnp.sin(angles), jnp.cos(angles)], axis=1)


def embed(tokens, modality, positions, modal_table):
    table_rows = jnp.where(modality[:, None] == 1, modal_table[1][None, :], modal_table[0][None, :])
    summed = tokens.astype(jnp.float32) + position_table(positions, tokens.shape[1]) + table_rows
    return summed.astype(jnp.bfloat16)


def layer_norm(embedded, norm_gain, norm_bias):
    values = embedded.astype(jnp.float32)
    row_mean = jnp.mean(values, axis=1, keepdims=True)
    centered = values - row_mean
    row_var = jnp.mean(centered * centered, axis=1, keepdims=True)
    return (centered * lax.rsqrt(row_var + EPSILON) * norm_gain + norm_bias).astype(jnp.bfloat16)


def local(
    tokens,
    modality,
    keep_mask,
    positions,
    modal_table,
    norm_gain,
    norm_bias,
    qkv_weight,
    out_weight,
    mask_token,
):
    tok_rows, feature_width = tokens.shape
    seq_count = lax.axis_size("seq")
    ctx_count = lax.axis_size("ctx")
    devices = seq_count * ctx_count
    everyone = ("seq", "ctx")
    seq, ctx = lax.axis_index("seq"), lax.axis_index("ctx")
    core = ctx % 2
    where = jnp.stack([seq * ctx_count + ctx, ctx, seq // SIDE, seq % SIDE, core]).astype(jnp.int32)
    group_rows = tok_rows * seq_count // 4
    width = feature_width // seq_count
    per = tok_rows // ctx_count
    bf16 = lambda *shape: jax.ShapeDtypeStruct(shape, jnp.bfloat16)

    masks = lax.all_to_all(
        jnp.broadcast_to(keep_mask[None, :], (devices, tok_rows)), everyone, 0, 0, tiled=True
    )
    embedded = embed(tokens, modality, positions, modal_table)
    normed = layer_norm(embedded, norm_gain, norm_bias)
    outgoing, pick = call(
        dispatch_body,
        (bf16(seq_count, tok_rows, width), bf16(tok_rows, tok_rows)),
        where,
        masks,
        keep_mask[None, :],
        normed,
        in_specs=[SMEM, VMEM, VMEM, VMEM],
        flops=2 * tok_rows * tok_rows * feature_width,
    )
    arrived = lax.all_to_all(outgoing.reshape(devices, per, width), everyone, 0, 0, tiled=True)
    half = bf16(group_rows // 2, width)
    parts = call(
        compact_body,
        (half, half),
        where,
        masks,
        arrived.reshape(devices * per, width),
        in_specs=[SMEM, VMEM, VMEM],
        flops=2 * group_rows * devices * per * width,
    )
    qkv_weight, parts = lax.optimization_barrier((qkv_weight, parts))
    ordered = call(
        reorder_body,
        (bf16(*qkv_weight.shape), bf16(*qkv_weight.shape)),
        where,
        qkv_weight,
        in_specs=[SMEM, HBM],
        scratch=(pltpu.SemaphoreType.DMA((2 * SIDE * SIDE,)),),
        flops=1 << 32,
    )
    lines = gather_plane(parts)
    near = call(
        qkv_near_body,
        jax.ShapeDtypeStruct((3, group_rows, width), jnp.float32),
        *ordered,
        *lines[0][:3],
        *lines[1][:3],
        in_specs=[VMEM] * 8,
        flops=6 * group_rows * feature_width * width * 3 // 4,
    )
    row_q, row_kv = bf16(group_rows, HEAD_DIM), bf16(group_rows, 2 * HEAD_DIM)
    my_q, my_kv, other_q, other_kv = call(
        qkv_far_body,
        (row_q, row_kv, row_q, row_kv),
        where,
        near,
        *ordered,
        lines[0][3],
        lines[1][3],
        in_specs=[SMEM] + [VMEM] * 5,
        flops=6 * group_rows * feature_width * width // 4,
    )
    their_kv = lax.ppermute(other_kv, "ctx", CORE_SWAP)
    their_q = lax.ppermute(other_q, "ctx", CORE_SWAP)
    own, ahead, far, behind = ring_of_four(my_kv, their_kv, "ctx", z_shift)

    q = (my_q, their_q)
    state = attend(q, own, None, False)
    state = attend(q, (behind[0], ahead[1]), state, False)
    state = attend(q, (behind[1], ahead[0]), state, False)
    own_head, for_other = attend(q, far, state, True)
    from_other = lax.ppermute(for_other, "ctx", CORE_SWAP)
    line = bf16(group_rows // 2, SIDE * width)
    partial = call(
        partial_body,
        [line] * (2 * SIDE),
        where,
        own_head,
        from_other,
        out_weight,
        in_specs=[SMEM, VMEM, VMEM, VMEM],
        flops=2 * group_rows * feature_width * width,
    )
    masks, _ = lax.optimization_barrier((masks, own_head))
    return_pick = call(
        return_pick_body,
        bf16(devices * per, group_rows),
        where,
        masks,
        in_specs=[SMEM, VMEM],
        flops=2 * devices * per * tok_rows * group_rows,
    )
    kept = jax.ShapeDtypeStruct(half.shape, jnp.float32)
    blocks = []
    for part, (last, first) in enumerate(ORDERS):
        arrived = scatter_line(partial[part * SIDE : (part + 1) * SIDE], first)
        sums = call(
            add_line_body, [kept, half, half, half], *arrived, in_specs=[VMEM] * SIDE
        )
        blocks += scatter_line(sums, last)
    returning = call(
        send_back_body,
        bf16(devices * per, width),
        return_pick,
        *blocks,
        in_specs=[VMEM] * (1 + 2 * SIDE),
        flops=2 * devices * per * group_rows * width,
    )
    returned = lax.all_to_all(returning.reshape(devices, per, width), everyone, 0, 0, tiled=True)
    return call(
        finish_body,
        jax.ShapeDtypeStruct((tok_rows, feature_width), jnp.float32),
        pick,
        returned.reshape(seq_count, tok_rows, width),
        embedded,
        mask_token[None, :],
        in_specs=[VMEM] * 4,
        flops=2 * tok_rows * tok_rows * feature_width,
    )


def solution(mesh):
    in_specs = (
        P(("seq", "ctx"), None),
        P(("seq", "ctx")),
        P(("seq", "ctx")),
        P(("seq", "ctx")),
        P(),
        P(),
        P(),
        P(None, None, "seq"),
        P("seq", None),
        P(),
    )
    out_specs = P(("seq", "ctx"), None)
    return jax.shard_map(local, mesh=mesh, in_specs=in_specs, out_specs=out_specs, check_vma=False)
```

```python
import functools
import math

import jax
import jax.numpy as jnp
from jax import lax
from jax.experimental import pallas as pl
from jax.experimental.pallas import tpu as pltpu
from jax.sharding import PartitionSpec as P

HEAD_DIM = 128
EPSILON = 1e-06
SIDE = 4
MIB = 1 << 20


def y_shift(d):
    return [(y * SIDE + x, (y + d) % SIDE * SIDE + x) for y in range(SIDE) for x in range(SIDE)]


def x_shift(d):
    return [(y * SIDE + x, y * SIDE + (x + d) % SIDE) for y in range(SIDE) for x in range(SIDE)]


def z_shift(d):
    return [(z * 2 + k, (z + d) % SIDE * 2 + k) for z in range(SIDE) for k in range(2)]


CORE_SWAP = [(z * 2 + k, z * 2 + 1 - k) for z in range(SIDE) for k in range(2)]


RING = (0, 1, 3, 2)
ORDERS = ((y_shift, x_shift), (x_shift, y_shift))


def halves(line):
    half = line.shape[0] // 2
    return line[:half], line[half:]


def gather_line(block, shift):
    return [block] + [lax.ppermute(block, "seq", shift(-d)) for d in RING[1:]]


def gather_long_line(line, shift, meanwhile):
    behind = lax.ppermute(line, "seq", shift(1))
    ahead = lax.ppermute(line, "seq", shift(-1))
    behind, ahead, *meanwhile = lax.optimization_barrier((behind, ahead, *meanwhile))
    far_top = lax.ppermute(halves(behind)[0], "seq", shift(1))
    far_bottom = lax.ppermute(halves(ahead)[1], "seq", shift(-1))
    return (line, ahead, behind, far_top, far_bottom), meanwhile


def gather_plane(parts, meanwhile):
    lines = [
        jnp.concatenate(gather_line(part, first), axis=1) for part, (first, _) in zip(parts, ORDERS)
    ]
    gathered = []
    for line, (_, second) in zip(lines, ORDERS):
        pieces, meanwhile = gather_long_line(line, second, meanwhile)
        gathered.append(pieces)
    return gathered, meanwhile


def scatter_line(blocks, shift):
    return [blocks[0]] + [
        lax.ppermute(block, "seq", shift(d)) for d, block in zip(RING[1:], blocks[1:])
    ]


def call(body, outs, *args, scratch=(), limit=16, flops=0, in_specs=None):
    vmem = pl.BlockSpec(memory_space=pltpu.VMEM)
    many = isinstance(outs, (tuple, list))
    return pl.pallas_call(
        body,
        out_shape=outs,
        in_specs=in_specs,
        out_specs=[vmem] * len(outs) if many else vmem,
        scratch_shapes=list(scratch),
        compiler_params=pltpu.CompilerParams(vmem_limit_bytes=limit * MIB),
        cost_estimate=pl.CostEstimate(
            flops=flops, transcendentals=0, bytes_accessed=sum(a.size * 2 for a in args)
        ),
    )(*args)


VMEM = pl.BlockSpec(memory_space=pltpu.VMEM)
SMEM = pl.BlockSpec(memory_space=pltpu.SMEM)
ANY = pl.BlockSpec(memory_space=pl.ANY)
HBM = pl.BlockSpec(memory_space=pltpu.HBM)


def dot(a, b, dims=((1,), (0,))):
    return lax.dot_general(a, b, (dims, ((), ())), preferred_element_type=jnp.float32)


def iota(shape, dim):
    return lax.broadcasted_iota(jnp.int32, shape, dim)


def as_bf16(flag):
    return jnp.where(flag, 1.0, 0.0).astype(jnp.bfloat16)


def counts_in_lanes(masks):
    return dot(jnp.ones((8, masks.shape[1]), jnp.bfloat16), masks, ((1,), (1,)))


def dispatch_body(where_ref, masks_ref, own_ref, normed_ref, out_ref, pick_ref):
    tokens = own_ref.shape[1]
    masks = masks_ref[...].astype(jnp.float32).astype(jnp.bfloat16)
    counts = counts_in_lanes(masks)[0:1]
    start = jnp.sum(
        jnp.where(iota(counts.shape, 1) < where_ref[0], counts, 0.0), axis=1, keepdims=True
    ).astype(jnp.int32)
    own = own_ref[...]
    wide = jnp.broadcast_to(own.astype(jnp.float32).astype(jnp.bfloat16), (8, tokens))
    upto = as_bf16(iota((tokens, tokens), 0) <= iota((tokens, tokens), 1))
    rank = dot(wide, upto)[0:1].astype(jnp.int32) - 1
    slot = ((start + rank) & 7) * (tokens // 8) + (rank >> 3)
    slot = jnp.where(own == 1, slot, -1)
    pick = as_bf16(iota((tokens, tokens), 0) == slot)
    pick_ref[...] = pick
    width = out_ref.shape[2]
    for s in range(out_ref.shape[0]):
        out_ref[s] = dot(pick, normed_ref[:, s * width : (s + 1) * width]).astype(jnp.bfloat16)


def compact_body(where_ref, masks_ref, arrived_ref, top_ref, bottom_ref):
    devices = masks_ref.shape[0]
    slots = arrived_ref.shape[0]
    per = slots // devices
    masks = masks_ref[...].astype(jnp.float32).astype(jnp.bfloat16)
    counts = counts_in_lanes(masks).astype(jnp.bfloat16)
    sender = iota((devices, slots), 1) // per
    device = iota((devices, slots), 0)
    start = dot(counts, as_bf16(device < sender))[0:1].astype(jnp.int32)
    count = dot(counts, as_bf16(device == sender))[0:1].astype(jnp.int32)
    offset = ((where_ref[1] - start) & 7) + 8 * (iota((1, slots), 1) % per)
    row = jnp.where(offset < count, (start + offset) >> 3, -1)
    arrived = arrived_ref[...]
    half = top_ref.shape[0]
    for r in range(0, 2 * half, 128):
        pick = as_bf16(iota((128, slots), 0) + r == row)
        out_ref = top_ref if r < half else bottom_ref
        out_ref[r % half : r % half + 128] = dot(pick, arrived).astype(jnp.bfloat16)


def plane_block(where_ref, part, outer, inner):
    y, x = (inner, outer) if part == 0 else (outer, inner)
    return (where_ref[2] + RING[y]) % SIDE * SIDE + (where_ref[3] + RING[x]) % SIDE


def reorder_body(where_ref, weight_ref, top_ref, bottom_ref, sems):
    width = weight_ref.shape[2]
    copies = []
    for part, out_ref in enumerate((top_ref, bottom_ref)):
        for outer in range(SIDE):
            for inner in range(SIDE):
                i = outer * SIDE + inner
                at = plane_block(where_ref, part, outer, inner) * width
                copies.append(
                    pltpu.make_async_copy(
                        weight_ref.at[:, pl.ds(pl.multiple_of(at, width), width), :],
                        out_ref.at[:, i * width : (i + 1) * width, :],
                        sems.at[part * SIDE * SIDE + i],
                    )
                )
                copies[-1].start()
    for copy in copies:
        copy.wait()


def qkv_near_body(top_ref, bottom_ref, *refs):
    lines, out_ref = refs[:-1], refs[-1]
    half, long = lines[0].shape
    near = len(lines) // 2
    for part, w_ref in enumerate((top_ref, bottom_ref)):
        for t in range(3):
            total = None
            for i in range(near):
                product = dot(lines[part * near + i][...], w_ref[t, i * long : (i + 1) * long])
                total = product if total is None else total + product
            out_ref[t, part * half : (part + 1) * half] = total


def qkv_far_body(where_ref, near_ref, top_ref, bottom_ref, *refs):
    lines, (my_q, my_kv, other_q, other_kv) = refs[:4], refs[4:]
    rows_each, long = lines[0].shape
    second = where_ref[4] == 1
    for i, line in enumerate(lines):
        w_ref = (top_ref, bottom_ref)[i // 2]
        rows = slice(i * rows_each, (i + 1) * rows_each)
        for t in range(3):
            total = near_ref[t, rows] + dot(line[...], w_ref[t, 3 * long :])
            both = total.astype(jnp.bfloat16)
            left, right = both[:, :HEAD_DIM], both[:, HEAD_DIM:]
            mine, other = (my_q, other_q) if t == 0 else (my_kv, other_kv)
            cols = slice(0, HEAD_DIM) if t < 2 else slice(HEAD_DIM, 2 * HEAD_DIM)
            mine[rows, cols] = jnp.where(second, right, left)
            other[rows, cols] = jnp.where(second, left, right)


def attend_body(has_state, is_last, keys, *refs):
    q_refs, kv_refs, refs = refs[:2], refs[2 : 2 + keys], refs[2 + keys :]
    state_refs, out_refs = (refs[:3], refs[3:]) if has_state else ((), refs)
    scale = math.log2(math.e) / math.sqrt(HEAD_DIM)
    rows = q_refs[0].shape[0]
    tile = 256
    per_side = rows // tile

    def one_tile(i):
        at = pl.ds(pl.multiple_of(i * tile, tile), tile)
        here = pl.ds(pl.multiple_of(i % per_side * tile, tile), tile)
        first = i < per_side
        q = jnp.where(first, q_refs[0][here], q_refs[1][here])
        scores = [dot(q, kv_ref[:, :HEAD_DIM], ((1,), (1,))) for kv_ref in kv_refs]
        tops = [jnp.max(s, axis=1, keepdims=True) for s in scores]
        if has_state:
            acc = state_refs[0][at]
            top = state_refs[1][at][:, 0:1]
            total = state_refs[2][at][:, 0:1]
            tops.append(top)
        new_top = tops[0]
        for t in tops[1:]:
            new_top = jnp.maximum(new_top, t)
        product = block_total = None
        for s, kv_ref in zip(scores, kv_refs):
            expanded = jnp.exp2((s - new_top) * scale)
            part_total = jnp.sum(expanded, axis=1, keepdims=True)
            part = dot(expanded.astype(jnp.bfloat16), kv_ref[:, HEAD_DIM:])
            product = part if product is None else product + part
            block_total = part_total if block_total is None else block_total + part_total
        if has_state:
            factor = jnp.exp2((top - new_top) * scale)
            product = acc * factor + product
            block_total = total * factor + block_total
        if is_last:
            result = (product / block_total).astype(jnp.bfloat16)

            @pl.when(first)
            def _():
                out_refs[0][here] = result

            @pl.when(jnp.logical_not(first))
            def _():
                out_refs[1][here] = result
        else:
            out_refs[0][at] = product
            out_refs[1][at] = jnp.broadcast_to(new_top, product.shape)
            out_refs[2][at] = jnp.broadcast_to(block_total, product.shape)

    lax.fori_loop(0, 2 * per_side, lambda i, _: one_tile(i), None)


def attend(q, kv_blocks, state, is_last):
    rows = q[0].shape[0]
    state = tuple(state or ())
    key_rows = sum(b.shape[0] for b in kv_blocks)
    kept = jax.ShapeDtypeStruct((2 * rows, HEAD_DIM), jnp.float32)
    last = jax.ShapeDtypeStruct((rows, HEAD_DIM), jnp.bfloat16)
    return call(
        lambda *refs: attend_body(bool(state), is_last, len(kv_blocks), *refs),
        (last, last) if is_last else (kept, kept, kept),
        *q,
        *kv_blocks,
        *state,
        in_specs=[VMEM] * (2 + len(kv_blocks) + len(state)),
        flops=16 * rows * key_rows * HEAD_DIM,
    )


def return_pick_body(where_ref, masks_ref, pick_ref):
    devices = masks_ref.shape[0]
    slots, rows = pick_ref.shape
    per = slots // devices
    masks = masks_ref[...].astype(jnp.float32).astype(jnp.bfloat16)
    counts = dot(masks, jnp.ones((devices, 128), jnp.bfloat16)).astype(jnp.bfloat16)
    sender = iota((slots, devices), 0) // per
    device = iota((slots, devices), 1)
    start = dot(as_bf16(device < sender), counts).astype(jnp.int32)
    count = dot(as_bf16(device == sender), counts).astype(jnp.int32)
    offset = ((where_ref[1] - start) & 7) + 8 * (iota((slots, 128), 0) % per)
    row = jnp.where(offset < count, (start + offset) >> 3, -1)
    for r in range(0, rows, 128):
        pick_ref[:, r : r + 128] = as_bf16(row == iota((slots, 128), 1) + r)


def partial_line(where_ref, own_ref, other_ref, weight_ref, part, outer):
    first = where_ref[4] == 0
    half = own_ref.shape[0] // 2
    own, other = (r[part * half : (part + 1) * half] for r in (own_ref, other_ref))
    heads = jnp.concatenate([jnp.where(first, own, other), jnp.where(first, other, own)], axis=1)
    width = heads.shape[1]
    for inner in range(SIDE):
        at = pl.multiple_of(plane_block(where_ref, part, outer, inner) * width, width)
        cols = slice(inner * width, (inner + 1) * width)
        yield cols, dot(heads, weight_ref[:, pl.ds(at, width)])


def far_partial_body(where_ref, own_ref, other_ref, weight_ref, *out_refs):
    for part in range(2):
        top_ref, bottom_ref = out_refs[2 * part : 2 * part + 2]
        rows = top_ref.shape[0]
        for cols, product in partial_line(where_ref, own_ref, other_ref, weight_ref, part, 3):
            product = product.astype(jnp.bfloat16)
            top_ref[:, cols] = product[:rows]
            bottom_ref[:, cols] = product[rows:]


def near_partial_body(part, where_ref, own_ref, other_ref, weight_ref, up_ref, down_ref, *out_refs):
    kept_ref, ahead_ref, behind_ref = out_refs
    rows = up_ref.shape[0]
    args = (where_ref, own_ref, other_ref, weight_ref, part)
    for cols, product in partial_line(*args, 0):
        kept_ref[:, cols] = product
    for cols, product in partial_line(*args, 1):
        top = product[:rows] + up_ref[:, cols].astype(jnp.float32)
        ahead_ref[:rows, cols] = top.astype(jnp.bfloat16)
        ahead_ref[rows:, cols] = product[rows:].astype(jnp.bfloat16)
    for cols, product in partial_line(*args, 2):
        bottom = product[rows:] + down_ref[:, cols].astype(jnp.float32)
        behind_ref[:rows, cols] = product[:rows].astype(jnp.bfloat16)
        behind_ref[rows:, cols] = bottom.astype(jnp.bfloat16)


def add_line_body(kept_ref, one_ref, two_ref, *out_refs):
    width = out_refs[0].shape[1]
    for i, out_ref in enumerate(out_refs):
        cols = slice(i * width, (i + 1) * width)
        one, two = one_ref[:, cols].astype(jnp.float32), two_ref[:, cols].astype(jnp.float32)
        out_ref[...] = (kept_ref[:, cols] + (one + two)).astype(out_ref.dtype)


def send_back_body(pick_ref, *refs):
    blocks, out_ref = refs[:-1], refs[-1]
    parts = []
    for part in range(2):
        a, b, c, d = (r[...].astype(jnp.float32) for r in blocks[part * SIDE : (part + 1) * SIDE])
        parts.append(((a + b) + (c + d)).astype(jnp.bfloat16))
    projected = jnp.concatenate(parts, axis=0)
    out_ref[...] = dot(pick_ref[...], projected).astype(jnp.bfloat16)


def finish_body(pick_ref, returned_ref, embedded_ref, filler_ref, out_ref):
    pick = pick_ref[...]
    width = returned_ref.shape[2]
    kept = dot(pick, jnp.ones((pick.shape[0], width), jnp.bfloat16), ((0,), (0,))) > 0.5
    for s in range(returned_ref.shape[0]):
        cols = slice(s * width, (s + 1) * width)
        projected = dot(pick, returned_ref[s], ((0,), (0,)))
        finished = embedded_ref[:, cols].astype(jnp.float32) + projected
        out_ref[:, cols] = jnp.where(kept, finished, filler_ref[:, cols])


def position_table(positions, feature_width):
    half_width = feature_width // 2
    frequency = jnp.exp(-math.log(10000.0) * jnp.arange(half_width, dtype=jnp.float32) / half_width)
    angles = positions.astype(jnp.float32)[:, None] * frequency[None, :]
    return jnp.concatenate([jnp.sin(angles), jnp.cos(angles)], axis=1)


def embed(tokens, modality, positions, modal_table):
    table_rows = jnp.where(modality[:, None] == 1, modal_table[1][None, :], modal_table[0][None, :])
    summed = tokens.astype(jnp.float32) + position_table(positions, tokens.shape[1]) + table_rows
    return summed.astype(jnp.bfloat16)


def layer_norm(embedded, norm_gain, norm_bias):
    values = embedded.astype(jnp.float32)
    row_mean = jnp.mean(values, axis=1, keepdims=True)
    centered = values - row_mean
    row_var = jnp.mean(centered * centered, axis=1, keepdims=True)
    return (centered * lax.rsqrt(row_var + EPSILON) * norm_gain + norm_bias).astype(jnp.bfloat16)


def local(
    tokens,
    modality,
    keep_mask,
    positions,
    modal_table,
    norm_gain,
    norm_bias,
    qkv_weight,
    out_weight,
    mask_token,
):
    tok_rows, feature_width = tokens.shape
    seq_count = lax.axis_size("seq")
    ctx_count = lax.axis_size("ctx")
    devices = seq_count * ctx_count
    everyone = ("seq", "ctx")
    seq, ctx = lax.axis_index("seq"), lax.axis_index("ctx")
    core = ctx % 2
    where = jnp.stack([seq * ctx_count + ctx, ctx, seq // SIDE, seq % SIDE, core]).astype(jnp.int32)
    group_rows = tok_rows * seq_count // 4
    width = feature_width // seq_count
    per = tok_rows // ctx_count
    bf16 = lambda *shape: jax.ShapeDtypeStruct(shape, jnp.bfloat16)

    masks = lax.all_to_all(
        jnp.broadcast_to(keep_mask[None, :], (devices, tok_rows)), everyone, 0, 0, tiled=True
    )
    embedded = embed(tokens, modality, positions, modal_table)
    normed = layer_norm(embedded, norm_gain, norm_bias)
    outgoing, pick = call(
        dispatch_body,
        (bf16(seq_count, tok_rows, width), bf16(tok_rows, tok_rows)),
        where,
        masks,
        keep_mask[None, :],
        normed,
        in_specs=[SMEM, VMEM, VMEM, VMEM],
        flops=2 * tok_rows * tok_rows * feature_width,
    )
    arrived = lax.all_to_all(outgoing.reshape(devices, per, width), everyone, 0, 0, tiled=True)
    half = bf16(group_rows // 2, width)
    parts = call(
        compact_body,
        (half, half),
        where,
        masks,
        arrived.reshape(devices * per, width),
        in_specs=[SMEM, VMEM, VMEM],
        flops=2 * group_rows * devices * per * width,
    )
    qkv_weight, parts = lax.optimization_barrier((qkv_weight, parts))
    ordered = call(
        reorder_body,
        (bf16(*qkv_weight.shape), bf16(*qkv_weight.shape)),
        where,
        qkv_weight,
        in_specs=[SMEM, HBM],
        scratch=(pltpu.SemaphoreType.DMA((2 * SIDE * SIDE,)),),
        flops=1 << 32,
    )
    lines, ordered = gather_plane(parts, ordered)
    near = call(
        qkv_near_body,
        jax.ShapeDtypeStruct((3, group_rows, width), jnp.float32),
        *ordered,
        *lines[0][:3],
        *lines[1][:3],
        in_specs=[VMEM] * 8,
        flops=6 * group_rows * feature_width * width * 3 // 4,
    )
    row_q, row_kv = bf16(group_rows, HEAD_DIM), bf16(group_rows, 2 * HEAD_DIM)
    my_q, my_kv, other_q, other_kv = call(
        qkv_far_body,
        (row_q, row_kv, row_q, row_kv),
        where,
        near,
        *ordered,
        *lines[0][3:],
        *lines[1][3:],
        in_specs=[SMEM] + [VMEM] * 7,
        flops=6 * group_rows * feature_width * width // 4,
    )
    their_kv = lax.ppermute(other_kv, "ctx", CORE_SWAP)
    their_q = lax.ppermute(other_q, "ctx", CORE_SWAP)
    behind_mine = lax.ppermute(my_kv, "ctx", z_shift(1))
    ahead_theirs = lax.ppermute(their_kv, "ctx", z_shift(-1))
    behind_theirs = lax.ppermute(their_kv, "ctx", z_shift(1))
    ahead_mine = lax.ppermute(my_kv, "ctx", z_shift(-1))
    q = (my_q, their_q)
    state = attend(q, (my_kv, their_kv), None, False)
    behind_mine, ahead_theirs, *state = lax.optimization_barrier(
        (behind_mine, ahead_theirs, *state)
    )
    far_mine = lax.ppermute(behind_mine, "ctx", z_shift(1))
    far_theirs = lax.ppermute(ahead_theirs, "ctx", z_shift(-1))
    state = attend(q, (behind_mine, ahead_theirs), state, False)
    state = attend(q, (behind_theirs, ahead_mine), state, False)
    own_head, for_other = attend(q, (far_mine, far_theirs), state, True)
    from_other = lax.ppermute(for_other, "ctx", CORE_SWAP)
    heads_args = (where, own_head, from_other, out_weight)
    heads_specs = [SMEM, VMEM, VMEM, VMEM]
    far_lines = call(
        far_partial_body,
        [bf16(group_rows // 4, SIDE * width)] * 4,
        *heads_args,
        in_specs=heads_specs,
        flops=group_rows * feature_width * width // 2,
    )
    masks, _ = lax.optimization_barrier((masks, own_head))
    return_pick = call(
        return_pick_body,
        bf16(devices * per, group_rows),
        where,
        masks,
        in_specs=[SMEM, VMEM],
        flops=2 * devices * per * tok_rows * group_rows,
    )
    kept = jax.ShapeDtypeStruct(half.shape, jnp.float32)
    blocks = []
    line = bf16(group_rows // 2, SIDE * width)
    kept_line = jax.ShapeDtypeStruct(line.shape, jnp.float32)
    for part, (last, first) in enumerate(ORDERS):
        up = lax.ppermute(far_lines[2 * part], "seq", first(1))
        down = lax.ppermute(far_lines[2 * part + 1], "seq", first(-1))
        own_line, for_ahead, for_behind = call(
            functools.partial(near_partial_body, part),
            [kept_line, line, line],
            *heads_args,
            up,
            down,
            in_specs=heads_specs + [VMEM] * 2,
            flops=group_rows * feature_width * width * 3 // 4,
        )
        sums = call(
            add_line_body,
            [kept, half, half, half],
            own_line,
            lax.ppermute(for_ahead, "seq", first(1)),
            lax.ppermute(for_behind, "seq", first(-1)),
            in_specs=[VMEM] * 3,
        )
        blocks += scatter_line(sums, last)
    returning = call(
        send_back_body,
        bf16(devices * per, width),
        return_pick,
        *blocks,
        in_specs=[VMEM] * (1 + 2 * SIDE),
        flops=2 * devices * per * group_rows * width,
    )
    returned = lax.all_to_all(returning.reshape(devices, per, width), everyone, 0, 0, tiled=True)
    return call(
        finish_body,
        jax.ShapeDtypeStruct((tok_rows, feature_width), jnp.float32),
        pick,
        returned.reshape(seq_count, tok_rows, width),
        embedded,
        mask_token[None, :],
        in_specs=[VMEM] * 4,
        flops=2 * tok_rows * tok_rows * feature_width,
    )


def solution(mesh):
    in_specs = (
        P(("seq", "ctx"), None),
        P(("seq", "ctx")),
        P(("seq", "ctx")),
        P(("seq", "ctx")),
        P(),
        P(),
        P(),
        P(None, None, "seq"),
        P("seq", None),
        P(),
    )
    out_specs = P(("seq", "ctx"), None)
    return jax.shard_map(local, mesh=mesh, in_specs=in_specs, out_specs=out_specs, check_vma=False)
```

```python
import itertools
import math

import jax
import jax.numpy as jnp
from jax import lax
from jax.experimental import pallas as pl
from jax.experimental.pallas import tpu as pltpu
from jax.sharding import PartitionSpec as P

HEAD_DIM = 128
EPSILON = 1e-06
SIDE = 4
MIB = 1 << 20


EVERYONE = ("seq", "ctx")


def plane_shift(leg, d):
    pairs = []
    for y, x, z, k in itertools.product(range(SIDE), range(SIDE), range(SIDE), range(2)):
        to = ((y + d) % SIDE, x) if leg == k else (y, (x + d) % SIDE)
        pairs.append(tuple(((v * SIDE + u) * SIDE + z) * 2 + k for v, u in ((y, x), to)))
    return pairs


def z_shift(d):
    return [(z * 2 + k, (z + d) % SIDE * 2 + k) for z in range(SIDE) for k in range(2)]


CORE_SWAP = [(z * 2 + k, z * 2 + 1 - k) for z in range(SIDE) for k in range(2)]


RING = (0, 1, 3, 2)


def send(block, leg, d):
    return lax.ppermute(block, EVERYONE, plane_shift(leg, d))


def gather_line(block):
    return [block] + [send(block, 0, -d) for d in RING[1:]]


def gather_long_line(top, bottom, meanwhile):
    behind_top, ahead_bottom = send(top, 1, 1), send(bottom, 1, -1)
    behind_bottom, ahead_top = send(bottom, 1, 1), send(top, 1, -1)
    behind_top, ahead_bottom, *meanwhile = lax.optimization_barrier(
        (behind_top, ahead_bottom, *meanwhile)
    )
    far_top, far_bottom = send(behind_top, 1, 1), send(ahead_bottom, 1, -1)
    near = (top, bottom, ahead_top, ahead_bottom, behind_top, behind_bottom)
    return near, (far_top, far_bottom), meanwhile


def scatter_line(blocks):
    return [blocks[0]] + [send(block, 0, d) for d, block in zip(RING[1:], blocks[1:])]


def call(body, outs, *args, scratch=(), limit=16, flops=0, in_specs=None):
    vmem = pl.BlockSpec(memory_space=pltpu.VMEM)
    many = isinstance(outs, (tuple, list))
    return pl.pallas_call(
        body,
        out_shape=outs,
        in_specs=in_specs,
        out_specs=[vmem] * len(outs) if many else vmem,
        scratch_shapes=list(scratch),
        compiler_params=pltpu.CompilerParams(vmem_limit_bytes=limit * MIB),
        cost_estimate=pl.CostEstimate(
            flops=flops, transcendentals=0, bytes_accessed=sum(a.size * 2 for a in args)
        ),
    )(*args)


VMEM = pl.BlockSpec(memory_space=pltpu.VMEM)
SMEM = pl.BlockSpec(memory_space=pltpu.SMEM)
ANY = pl.BlockSpec(memory_space=pl.ANY)
HBM = pl.BlockSpec(memory_space=pltpu.HBM)


def dot(a, b, dims=((1,), (0,))):
    return lax.dot_general(a, b, (dims, ((), ())), preferred_element_type=jnp.float32)


def iota(shape, dim):
    return lax.broadcasted_iota(jnp.int32, shape, dim)


def as_bf16(flag):
    return jnp.where(flag, 1.0, 0.0).astype(jnp.bfloat16)


def counts_in_lanes(masks):
    return dot(jnp.ones((8, masks.shape[1]), jnp.bfloat16), masks, ((1,), (1,)))


def dispatch_body(where_ref, masks_ref, own_ref, normed_ref, out_ref, pick_ref):
    tokens = own_ref.shape[1]
    masks = masks_ref[...].astype(jnp.float32).astype(jnp.bfloat16)
    counts = counts_in_lanes(masks)[0:1]
    start = jnp.sum(
        jnp.where(iota(counts.shape, 1) < where_ref[0], counts, 0.0), axis=1, keepdims=True
    ).astype(jnp.int32)
    own = own_ref[...]
    wide = jnp.broadcast_to(own.astype(jnp.float32).astype(jnp.bfloat16), (8, tokens))
    upto = as_bf16(iota((tokens, tokens), 0) <= iota((tokens, tokens), 1))
    rank = dot(wide, upto)[0:1].astype(jnp.int32) - 1
    slot = ((start + rank) & 7) * (tokens // 8) + (rank >> 3)
    slot = jnp.where(own == 1, slot, -1)
    pick = as_bf16(iota((tokens, tokens), 0) == slot)
    pick_ref[...] = pick
    width = out_ref.shape[2]
    for s in range(out_ref.shape[0]):
        out_ref[s] = dot(pick, normed_ref[:, s * width : (s + 1) * width]).astype(jnp.bfloat16)


def compact_body(where_ref, masks_ref, arrived_ref, out_ref):
    devices = masks_ref.shape[0]
    slots = arrived_ref.shape[0]
    per = slots // devices
    masks = masks_ref[...].astype(jnp.float32).astype(jnp.bfloat16)
    counts = counts_in_lanes(masks).astype(jnp.bfloat16)
    sender = iota((devices, slots), 1) // per
    device = iota((devices, slots), 0)
    start = dot(counts, as_bf16(device < sender))[0:1].astype(jnp.int32)
    count = dot(counts, as_bf16(device == sender))[0:1].astype(jnp.int32)
    offset = ((where_ref[1] - start) & 7) + 8 * (iota((1, slots), 1) % per)
    row = jnp.where(offset < count, (start + offset) >> 3, -1)
    arrived = arrived_ref[...]
    for r in range(0, out_ref.shape[0], 128):
        pick = as_bf16(iota((128, slots), 0) + r == row)
        out_ref[r : r + 128] = dot(pick, arrived).astype(jnp.bfloat16)


def line_body(*refs):
    blocks, (top_ref, bottom_ref) = refs[:-2], refs[-2:]
    half = top_ref.shape[0]
    width = blocks[0].shape[1]
    for i, block in enumerate(blocks):
        cols = slice(i * width, (i + 1) * width)
        top_ref[:, cols] = block[:half]
        bottom_ref[:, cols] = block[half:]


def plane_block(where_ref, outer, inner):
    first = where_ref[4] == 0
    y = jnp.where(first, RING[inner], RING[outer])
    x = jnp.where(first, RING[outer], RING[inner])
    return (where_ref[2] + y) % SIDE * SIDE + (where_ref[3] + x) % SIDE


def reorder_body(where_ref, weight_ref, out_ref, sems):
    width = weight_ref.shape[2]
    copies = []
    for outer in range(SIDE):
        for inner in range(SIDE):
            i = outer * SIDE + inner
            at = pl.multiple_of(plane_block(where_ref, outer, inner) * width, width)
            copies.append(
                pltpu.make_async_copy(
                    weight_ref.at[:, pl.ds(at, width), :],
                    out_ref.at[:, i * width : (i + 1) * width, :],
                    sems.at[i],
                )
            )
            copies[-1].start()
    for copy in copies:
        copy.wait()


def qkv_near_body(w_ref, *refs):
    lines, out_ref = refs[:-1], refs[-1]
    half, long = lines[0].shape
    for low in range(2):
        for t in range(3):
            total = None
            for i in range(3):
                product = dot(lines[2 * i + low][...], w_ref[t, i * long : (i + 1) * long])
                total = product if total is None else total + product
            out_ref[t, low * half : (low + 1) * half] = total


def qkv_far_body(where_ref, near_ref, w_ref, *refs):
    lines, (my_q, my_kv, other_q, other_kv) = refs[:2], refs[2:]
    half, long = lines[0].shape
    second = where_ref[4] == 1
    for low, line in enumerate(lines):
        rows = slice(low * half, (low + 1) * half)
        for t in range(3):
            total = near_ref[t, rows] + dot(line[...], w_ref[t, 3 * long :])
            both = total.astype(jnp.bfloat16)
            left, right = both[:, :HEAD_DIM], both[:, HEAD_DIM:]
            mine, other = (my_q, other_q) if t == 0 else (my_kv, other_kv)
            cols = slice(0, HEAD_DIM) if t < 2 else slice(HEAD_DIM, 2 * HEAD_DIM)
            mine[rows, cols] = jnp.where(second, right, left)
            other[rows, cols] = jnp.where(second, left, right)


def attend_body(has_state, is_last, keys, *refs):
    q_refs, kv_refs, refs = refs[:2], refs[2 : 2 + keys], refs[2 + keys :]
    state_refs, out_refs = (refs[:3], refs[3:]) if has_state else ((), refs)
    scale = math.log2(math.e) / math.sqrt(HEAD_DIM)
    rows = q_refs[0].shape[0]
    tile = 256
    per_side = rows // tile

    def one_tile(i):
        at = pl.ds(pl.multiple_of(i * tile, tile), tile)
        here = pl.ds(pl.multiple_of(i % per_side * tile, tile), tile)
        first = i < per_side
        q = jnp.where(first, q_refs[0][here], q_refs[1][here])
        scores = [dot(q, kv_ref[:, :HEAD_DIM], ((1,), (1,))) for kv_ref in kv_refs]
        tops = [jnp.max(s, axis=1, keepdims=True) for s in scores]
        if has_state:
            acc = state_refs[0][at]
            top = state_refs[1][at][:, 0:1]
            total = state_refs[2][at][:, 0:1]
            tops.append(top)
        new_top = tops[0]
        for t in tops[1:]:
            new_top = jnp.maximum(new_top, t)
        product = block_total = None
        for s, kv_ref in zip(scores, kv_refs):
            expanded = jnp.exp2((s - new_top) * scale)
            part_total = jnp.sum(expanded, axis=1, keepdims=True)
            part = dot(expanded.astype(jnp.bfloat16), kv_ref[:, HEAD_DIM:])
            product = part if product is None else product + part
            block_total = part_total if block_total is None else block_total + part_total
        if has_state:
            factor = jnp.exp2((top - new_top) * scale)
            product = acc * factor + product
            block_total = total * factor + block_total
        if is_last:
            result = (product / block_total).astype(jnp.bfloat16)

            @pl.when(first)
            def _():
                out_refs[0][here] = result

            @pl.when(jnp.logical_not(first))
            def _():
                out_refs[1][here] = result
        else:
            out_refs[0][at] = product
            out_refs[1][at] = jnp.broadcast_to(new_top, product.shape)
            out_refs[2][at] = jnp.broadcast_to(block_total, product.shape)

    lax.fori_loop(0, 2 * per_side, lambda i, _: one_tile(i), None)


def attend(q, kv_blocks, state, is_last):
    rows = q[0].shape[0]
    state = tuple(state or ())
    key_rows = sum(b.shape[0] for b in kv_blocks)
    kept = jax.ShapeDtypeStruct((2 * rows, HEAD_DIM), jnp.float32)
    last = jax.ShapeDtypeStruct((rows, HEAD_DIM), jnp.bfloat16)
    return call(
        lambda *refs: attend_body(bool(state), is_last, len(kv_blocks), *refs),
        (last, last) if is_last else (kept, kept, kept),
        *q,
        *kv_blocks,
        *state,
        in_specs=[VMEM] * (2 + len(kv_blocks) + len(state)),
        flops=16 * rows * key_rows * HEAD_DIM,
    )


def return_pick_body(where_ref, masks_ref, pick_ref):
    devices = masks_ref.shape[0]
    slots, rows = pick_ref.shape
    per = slots // devices
    masks = masks_ref[...].astype(jnp.float32).astype(jnp.bfloat16)
    counts = dot(masks, jnp.ones((devices, 128), jnp.bfloat16)).astype(jnp.bfloat16)
    sender = iota((slots, devices), 0) // per
    device = iota((slots, devices), 1)
    start = dot(as_bf16(device < sender), counts).astype(jnp.int32)
    count = dot(as_bf16(device == sender), counts).astype(jnp.int32)
    offset = ((where_ref[1] - start) & 7) + 8 * (iota((slots, 128), 0) % per)
    row = jnp.where(offset < count, (start + offset) >> 3, -1)
    for r in range(0, rows, 128):
        pick_ref[:, r : r + 128] = as_bf16(row == iota((slots, 128), 1) + r)


def partial_line(where_ref, own_ref, other_ref, weight_ref, outer, rows):
    first = where_ref[4] == 0
    own, other = own_ref[rows], other_ref[rows]
    heads = jnp.concatenate([jnp.where(first, own, other), jnp.where(first, other, own)], axis=1)
    width = heads.shape[1]
    for inner in range(SIDE):
        at = pl.multiple_of(plane_block(where_ref, outer, inner) * width, width)
        cols = slice(inner * width, (inner + 1) * width)
        yield cols, dot(heads, weight_ref[:, pl.ds(at, width)])


def far_partial_body(*refs):
    args, (top_ref, bottom_ref) = refs[:4], refs[4:]
    half = top_ref.shape[0]
    for cols, product in partial_line(*args, 3, slice(None)):
        product = product.astype(jnp.bfloat16)
        top_ref[:, cols] = product[:half]
        bottom_ref[:, cols] = product[half:]


def near_partial_body(*refs):
    args, (kept_ref, ahead_ref, behind_ref) = refs[:4], refs[4:]
    half = ahead_ref.shape[0]
    for cols, product in partial_line(*args, 1, slice(half, None)):
        ahead_ref[:, cols] = product.astype(jnp.bfloat16)
    for cols, product in partial_line(*args, 2, slice(0, half)):
        behind_ref[:, cols] = product.astype(jnp.bfloat16)
    for cols, product in partial_line(*args, 0, slice(None)):
        kept_ref[:, cols] = product


def relay_partial_body(*refs):
    args, (up_ref, down_ref), (ahead_ref, behind_ref) = refs[:4], refs[4:6], refs[6:]
    half = up_ref.shape[0]
    for cols, product in partial_line(*args, 1, slice(0, half)):
        ahead_ref[:, cols] = (product + up_ref[:, cols].astype(jnp.float32)).astype(jnp.bfloat16)
    for cols, product in partial_line(*args, 2, slice(half, None)):
        behind_ref[:, cols] = (product + down_ref[:, cols].astype(jnp.float32)).astype(
            jnp.bfloat16
        )


def add_line_body(kept_ref, *refs):
    tops, bottoms, out_refs = refs[:2], refs[2:4], refs[4:]
    half = tops[0].shape[0]
    width = out_refs[0].shape[1]
    for low, pair in enumerate((tops, bottoms)):
        rows = slice(low * half, (low + 1) * half)
        for i, out_ref in enumerate(out_refs):
            cols = slice(i * width, (i + 1) * width)
            one, two = (r[:, cols].astype(jnp.float32) for r in pair)
            out_ref[rows] = (kept_ref[rows, cols] + (one + two)).astype(out_ref.dtype)


def send_back_body(pick_ref, *refs):
    blocks, out_ref = refs[:-1], refs[-1]
    a, b, c, d = (r[...].astype(jnp.float32) for r in blocks)
    projected = ((a + b) + (c + d)).astype(jnp.bfloat16)
    out_ref[...] = dot(pick_ref[...], projected).astype(jnp.bfloat16)


def finish_body(pick_ref, returned_ref, embedded_ref, filler_ref, out_ref):
    pick = pick_ref[...]
    width = returned_ref.shape[2]
    kept = dot(pick, jnp.ones((pick.shape[0], width), jnp.bfloat16), ((0,), (0,))) > 0.5
    for s in range(returned_ref.shape[0]):
        cols = slice(s * width, (s + 1) * width)
        projected = dot(pick, returned_ref[s], ((0,), (0,)))
        finished = embedded_ref[:, cols].astype(jnp.float32) + projected
        out_ref[:, cols] = jnp.where(kept, finished, filler_ref[:, cols])


def position_table(positions, feature_width):
    half_width = feature_width // 2
    frequency = jnp.exp(-math.log(10000.0) * jnp.arange(half_width, dtype=jnp.float32) / half_width)
    angles = positions.astype(jnp.float32)[:, None] * frequency[None, :]
    return jnp.concatenate([jnp.sin(angles), jnp.cos(angles)], axis=1)


def embed(tokens, modality, positions, modal_table):
    table_rows = jnp.where(modality[:, None] == 1, modal_table[1][None, :], modal_table[0][None, :])
    summed = tokens.astype(jnp.float32) + position_table(positions, tokens.shape[1]) + table_rows
    return summed.astype(jnp.bfloat16)


def layer_norm(embedded, norm_gain, norm_bias):
    values = embedded.astype(jnp.float32)
    row_mean = jnp.mean(values, axis=1, keepdims=True)
    centered = values - row_mean
    row_var = jnp.mean(centered * centered, axis=1, keepdims=True)
    return (centered * lax.rsqrt(row_var + EPSILON) * norm_gain + norm_bias).astype(jnp.bfloat16)


def local(
    tokens,
    modality,
    keep_mask,
    positions,
    modal_table,
    norm_gain,
    norm_bias,
    qkv_weight,
    out_weight,
    mask_token,
):
    tok_rows, feature_width = tokens.shape
    seq_count = lax.axis_size("seq")
    ctx_count = lax.axis_size("ctx")
    devices = seq_count * ctx_count
    everyone = ("seq", "ctx")
    seq, ctx = lax.axis_index("seq"), lax.axis_index("ctx")
    core = ctx % 2
    where = jnp.stack([seq * ctx_count + ctx, ctx, seq // SIDE, seq % SIDE, core]).astype(jnp.int32)
    group_rows = tok_rows * seq_count // 4
    width = feature_width // seq_count
    per = tok_rows // ctx_count
    bf16 = lambda *shape: jax.ShapeDtypeStruct(shape, jnp.bfloat16)

    masks = lax.all_to_all(
        jnp.broadcast_to(keep_mask[None, :], (devices, tok_rows)), everyone, 0, 0, tiled=True
    )
    embedded = embed(tokens, modality, positions, modal_table)
    normed = layer_norm(embedded, norm_gain, norm_bias)
    outgoing, pick = call(
        dispatch_body,
        (bf16(seq_count, tok_rows, width), bf16(tok_rows, tok_rows)),
        where,
        masks,
        keep_mask[None, :],
        normed,
        in_specs=[SMEM, VMEM, VMEM, VMEM],
        flops=2 * tok_rows * tok_rows * feature_width,
    )
    arrived = lax.all_to_all(outgoing.reshape(devices, per, width), everyone, 0, 0, tiled=True)
    block = call(
        compact_body,
        bf16(group_rows, width),
        where,
        masks,
        arrived.reshape(devices * per, width),
        in_specs=[SMEM, VMEM, VMEM],
        flops=2 * group_rows * devices * per * width,
    )
    half_line = bf16(group_rows // 2, SIDE * width)
    line = call(line_body, (half_line, half_line), *gather_line(block), in_specs=[VMEM] * SIDE)
    qkv_weight, block = lax.optimization_barrier((qkv_weight, block))
    ordered = call(
        reorder_body,
        bf16(*qkv_weight.shape),
        where,
        qkv_weight,
        in_specs=[SMEM, HBM],
        scratch=(pltpu.SemaphoreType.DMA((SIDE * SIDE,)),),
        flops=1 << 32,
    )
    near_lines, far_lines, (ordered,) = gather_long_line(*line, (ordered,))
    near = call(
        qkv_near_body,
        jax.ShapeDtypeStruct((3, group_rows, width), jnp.float32),
        ordered,
        *near_lines,
        in_specs=[VMEM] * 7,
        flops=6 * group_rows * feature_width * width * 3 // 4,
    )
    row_q, row_kv = bf16(group_rows, HEAD_DIM), bf16(group_rows, 2 * HEAD_DIM)
    my_q, my_kv, other_q, other_kv = call(
        qkv_far_body,
        (row_q, row_kv, row_q, row_kv),
        where,
        near,
        ordered,
        *far_lines,
        in_specs=[SMEM] + [VMEM] * 4,
        flops=6 * group_rows * feature_width * width // 4,
    )
    their_kv = lax.ppermute(other_kv, "ctx", CORE_SWAP)
    their_q = lax.ppermute(other_q, "ctx", CORE_SWAP)
    behind_mine = lax.ppermute(my_kv, "ctx", z_shift(1))
    ahead_theirs = lax.ppermute(their_kv, "ctx", z_shift(-1))
    behind_theirs = lax.ppermute(their_kv, "ctx", z_shift(1))
    ahead_mine = lax.ppermute(my_kv, "ctx", z_shift(-1))
    q = (my_q, their_q)
    state = attend(q, (my_kv, their_kv), None, False)
    behind_mine, ahead_theirs, *state = lax.optimization_barrier(
        (behind_mine, ahead_theirs, *state)
    )
    far_mine = lax.ppermute(behind_mine, "ctx", z_shift(1))
    far_theirs = lax.ppermute(ahead_theirs, "ctx", z_shift(-1))
    state = attend(q, (behind_mine, ahead_theirs), state, False)
    state = attend(q, (behind_theirs, ahead_mine), state, False)
    own_head, for_other = attend(q, (far_mine, far_theirs), state, True)
    from_other = lax.ppermute(for_other, "ctx", CORE_SWAP)
    heads_args = (where, own_head, from_other, out_weight)
    heads_specs = [SMEM, VMEM, VMEM, VMEM]
    far_top, far_bottom = call(
        far_partial_body,
        (half_line, half_line),
        *heads_args,
        in_specs=heads_specs,
        flops=group_rows * feature_width * width // 2,
    )
    kept, ahead_bottom, behind_top = call(
        near_partial_body,
        (jax.ShapeDtypeStruct((group_rows, SIDE * width), jnp.float32), half_line, half_line),
        *heads_args,
        in_specs=heads_specs,
        flops=group_rows * feature_width * width,
    )
    ahead_top, behind_bottom = call(
        relay_partial_body,
        (half_line, half_line),
        *heads_args,
        send(far_top, 1, 1),
        send(far_bottom, 1, -1),
        in_specs=heads_specs + [VMEM] * 2,
        flops=group_rows * feature_width * width // 2,
    )
    sums = call(
        add_line_body,
        [jax.ShapeDtypeStruct((group_rows, width), jnp.float32)] + [bf16(group_rows, width)] * 3,
        kept,
        send(ahead_top, 1, 1),
        send(behind_top, 1, -1),
        send(ahead_bottom, 1, 1),
        send(behind_bottom, 1, -1),
        in_specs=[VMEM] * 5,
    )
    blocks = scatter_line(sums)
    masks, _ = lax.optimization_barrier((masks, own_head))
    return_pick = call(
        return_pick_body,
        bf16(devices * per, group_rows),
        where,
        masks,
        in_specs=[SMEM, VMEM],
        flops=2 * devices * per * tok_rows * group_rows,
    )
    returning = call(
        send_back_body,
        bf16(devices * per, width),
        return_pick,
        *blocks,
        in_specs=[VMEM] * (1 + SIDE),
        flops=2 * devices * per * group_rows * width,
    )
    returned = lax.all_to_all(returning.reshape(devices, per, width), everyone, 0, 0, tiled=True)
    return call(
        finish_body,
        jax.ShapeDtypeStruct((tok_rows, feature_width), jnp.float32),
        pick,
        returned.reshape(seq_count, tok_rows, width),
        embedded,
        mask_token[None, :],
        in_specs=[VMEM] * 4,
        flops=2 * tok_rows * tok_rows * feature_width,
    )


def solution(mesh):
    in_specs = (
        P(("seq", "ctx"), None),
        P(("seq", "ctx")),
        P(("seq", "ctx")),
        P(("seq", "ctx")),
        P(),
        P(),
        P(),
        P(None, None, "seq"),
        P("seq", None),
        P(),
    )
    out_specs = P(("seq", "ctx"), None)
    return jax.shard_map(local, mesh=mesh, in_specs=in_specs, out_specs=out_specs, check_vma=False)
```

```python
import functools
import itertools
import math

import jax
import jax.numpy as jnp
from jax import lax
from jax.experimental import pallas as pl
from jax.experimental.pallas import tpu as pltpu
from jax.sharding import PartitionSpec as P

HEAD_DIM = 128
EPSILON = 1e-06
SIDE = 4
MIB = 1 << 20


EVERYONE = ("seq", "ctx")


def plane_shift(leg, d):
    pairs = []
    for y, x, z, k in itertools.product(range(SIDE), range(SIDE), range(SIDE), range(2)):
        to = ((y + d) % SIDE, x) if leg == k else (y, (x + d) % SIDE)
        pairs.append(tuple(((v * SIDE + u) * SIDE + z) * 2 + k for v, u in ((y, x), to)))
    return pairs


def z_shift(d):
    return [(z * 2 + k, (z + d) % SIDE * 2 + k) for z in range(SIDE) for k in range(2)]


CORE_SWAP = [(z * 2 + k, z * 2 + 1 - k) for z in range(SIDE) for k in range(2)]


RING = (0, 1, 3, 2)


def send(block, leg, d):
    return lax.ppermute(block, EVERYONE, plane_shift(leg, d))


def gather_line(block):
    return [block] + [send(block, 0, -d) for d in RING[1:]]


def gather_long_line(top, bottom):
    behind_top, ahead_bottom = send(top, 1, 1), send(bottom, 1, -1)
    behind_bottom, ahead_top = send(bottom, 1, 1), send(top, 1, -1)
    far_top, far_bottom = send(behind_top, 1, 1), send(ahead_bottom, 1, -1)
    near = (top, bottom, ahead_top, ahead_bottom, behind_top, behind_bottom)
    return near, (far_top, far_bottom)


def scatter_line(blocks):
    return [blocks[0]] + [send(block, 0, d) for d, block in zip(RING[1:], blocks[1:])]


def call(body, outs, *args, scratch=(), limit=16, flops=0, in_specs=None):
    vmem = pl.BlockSpec(memory_space=pltpu.VMEM)
    many = isinstance(outs, (tuple, list))
    return pl.pallas_call(
        body,
        out_shape=outs,
        in_specs=in_specs,
        out_specs=[vmem] * len(outs) if many else vmem,
        scratch_shapes=list(scratch),
        compiler_params=pltpu.CompilerParams(vmem_limit_bytes=limit * MIB),
        cost_estimate=pl.CostEstimate(
            flops=flops, transcendentals=0, bytes_accessed=sum(a.size * 2 for a in args)
        ),
    )(*args)


VMEM = pl.BlockSpec(memory_space=pltpu.VMEM)
SMEM = pl.BlockSpec(memory_space=pltpu.SMEM)
ANY = pl.BlockSpec(memory_space=pl.ANY)
HBM = pl.BlockSpec(memory_space=pltpu.HBM)


def dot(a, b, dims=((1,), (0,))):
    return lax.dot_general(a, b, (dims, ((), ())), preferred_element_type=jnp.float32)


def iota(shape, dim):
    return lax.broadcasted_iota(jnp.int32, shape, dim)


def as_bf16(flag):
    return jnp.where(flag, 1.0, 0.0).astype(jnp.bfloat16)


def counts_in_lanes(masks):
    return dot(jnp.ones((8, masks.shape[1]), jnp.bfloat16), masks, ((1,), (1,)))


def repeat_body(row_ref, out_ref):
    out_ref[...] = jnp.broadcast_to(row_ref[...][None], out_ref.shape)


def dispatch_body(where_ref, masks_ref, own_ref, normed_ref, out_ref, pick_ref):
    tokens = own_ref.shape[1]
    masks = masks_ref[...].astype(jnp.float32).astype(jnp.bfloat16)
    counts = counts_in_lanes(masks)[0:1]
    start = jnp.sum(
        jnp.where(iota(counts.shape, 1) < where_ref[0], counts, 0.0), axis=1, keepdims=True
    ).astype(jnp.int32)
    own = own_ref[...]
    wide = jnp.broadcast_to(own.astype(jnp.float32).astype(jnp.bfloat16), (8, tokens))
    upto = as_bf16(iota((tokens, tokens), 0) <= iota((tokens, tokens), 1))
    rank = dot(wide, upto)[0:1].astype(jnp.int32) - 1
    slot = ((start + rank) & 7) * (tokens // 8) + (rank >> 3)
    slot = jnp.where(own == 1, slot, -1)
    pick = as_bf16(iota((tokens, tokens), 0) == slot)
    pick_ref[...] = pick
    width = out_ref.shape[2]
    for s in range(out_ref.shape[0]):
        out_ref[s] = dot(pick, normed_ref[:, s * width : (s + 1) * width]).astype(jnp.bfloat16)


def compact_body(where_ref, masks_ref, arrived_ref, out_ref):
    devices = masks_ref.shape[0]
    slots = arrived_ref.shape[0]
    per = slots // devices
    masks = masks_ref[...].astype(jnp.float32).astype(jnp.bfloat16)
    counts = counts_in_lanes(masks).astype(jnp.bfloat16)
    sender = iota((devices, slots), 1) // per
    device = iota((devices, slots), 0)
    start = dot(counts, as_bf16(device < sender))[0:1].astype(jnp.int32)
    count = dot(counts, as_bf16(device == sender))[0:1].astype(jnp.int32)
    offset = ((where_ref[1] - start) & 7) + 8 * (iota((1, slots), 1) % per)
    row = jnp.where(offset < count, (start + offset) >> 3, -1)
    arrived = arrived_ref[...]
    for r in range(0, out_ref.shape[0], 128):
        pick = as_bf16(iota((128, slots), 0) + r == row)
        out_ref[r : r + 128] = dot(pick, arrived).astype(jnp.bfloat16)


def line_body(*refs):
    blocks, (top_ref, bottom_ref) = refs[:-2], refs[-2:]
    half = top_ref.shape[0]
    width = blocks[0].shape[1]
    for i, block in enumerate(blocks):
        cols = slice(i * width, (i + 1) * width)
        top_ref[:, cols] = block[:half]
        bottom_ref[:, cols] = block[half:]


def plane_block(where_ref, outer, inner):
    first = where_ref[4] == 0
    y = jnp.where(first, RING[inner], RING[outer])
    x = jnp.where(first, RING[outer], RING[inner])
    return (where_ref[2] + y) % SIDE * SIDE + (where_ref[3] + x) % SIDE


def reorder_body(where_ref, weight_ref, out_ref, sems):
    width = weight_ref.shape[2]
    copies = []
    for outer in range(SIDE):
        for inner in range(SIDE):
            i = outer * SIDE + inner
            at = pl.multiple_of(plane_block(where_ref, outer, inner) * width, width)
            copies.append(
                pltpu.make_async_copy(
                    weight_ref.at[:, pl.ds(at, width), :],
                    out_ref.at[:, i * width : (i + 1) * width, :],
                    sems.at[i],
                )
            )
            copies[-1].start()
    for copy in copies:
        copy.wait()


def qkv_near_body(w_ref, *refs):
    lines, out_ref = refs[:-1], refs[-1]
    half, long = lines[0].shape
    for low in range(2):
        for t in range(3):
            total = None
            for i in range(3):
                product = dot(lines[2 * i + low][...], w_ref[t, i * long : (i + 1) * long])
                total = product if total is None else total + product
            out_ref[t, low * half : (low + 1) * half] = total


def qkv_far_body(where_ref, near_ref, w_ref, *refs):
    lines, (my_q, my_kv, other_q, other_kv) = refs[:2], refs[2:]
    half, long = lines[0].shape
    second = where_ref[4] == 1
    for low, line in enumerate(lines):
        rows = slice(low * half, (low + 1) * half)
        for t in range(3):
            total = near_ref[t, rows] + dot(line[...], w_ref[t, 3 * long :])
            both = total.astype(jnp.bfloat16)
            left, right = both[:, :HEAD_DIM], both[:, HEAD_DIM:]
            mine, other = (my_q, other_q) if t == 0 else (my_kv, other_kv)
            cols = slice(0, HEAD_DIM) if t < 2 else slice(HEAD_DIM, 2 * HEAD_DIM)
            mine[rows, cols] = jnp.where(second, right, left)
            other[rows, cols] = jnp.where(second, left, right)


def attend_body(has_state, last_side, keys, *refs):
    q_refs, kv_refs, refs = refs[:2], refs[2 : 2 + keys], refs[2 + keys :]
    state_refs, out_refs = (refs[:3], refs[3:]) if has_state else ((), refs)
    scale = math.log2(math.e) / math.sqrt(HEAD_DIM)
    rows = q_refs[0].shape[0]
    tile = 256
    per_side = rows // tile
    is_last = last_side is not None

    def one_tile(i):
        at = pl.ds(pl.multiple_of(i * tile, tile), tile)
        here = pl.ds(pl.multiple_of(i % per_side * tile, tile), tile)
        if is_last:
            q = q_refs[last_side][here]
        else:
            q = jnp.where(i < per_side, q_refs[0][here], q_refs[1][here])
        scores = [dot(q, kv_ref[:, :HEAD_DIM], ((1,), (1,))) for kv_ref in kv_refs]
        tops = [jnp.max(s, axis=1, keepdims=True) for s in scores]
        if has_state:
            acc = state_refs[0][at]
            top = state_refs[1][at][:, 0:1]
            total = state_refs[2][at][:, 0:1]
            tops.append(top)
        new_top = tops[0]
        for t in tops[1:]:
            new_top = jnp.maximum(new_top, t)
        product = block_total = None
        for s, kv_ref in zip(scores, kv_refs):
            expanded = jnp.exp2((s - new_top) * scale)
            part_total = jnp.sum(expanded, axis=1, keepdims=True)
            part = dot(expanded.astype(jnp.bfloat16), kv_ref[:, HEAD_DIM:])
            product = part if product is None else product + part
            block_total = part_total if block_total is None else block_total + part_total
        if has_state:
            factor = jnp.exp2((top - new_top) * scale)
            product = acc * factor + product
            block_total = total * factor + block_total
        if is_last:
            out_refs[0][here] = (product / block_total).astype(jnp.bfloat16)
        else:
            out_refs[0][at] = product
            out_refs[1][at] = jnp.broadcast_to(new_top, product.shape)
            out_refs[2][at] = jnp.broadcast_to(block_total, product.shape)

    if is_last:
        first_tile, tiles = last_side * per_side, per_side
    else:
        first_tile, tiles = 0, 2 * per_side
    lax.fori_loop(first_tile, first_tile + tiles, lambda i, _: one_tile(i), None)


def attend(q, kv_blocks, state=(), last_side=None):
    rows = q[0].shape[0]
    key_rows = sum(b.shape[0] for b in kv_blocks)
    kept = jax.ShapeDtypeStruct((2 * rows, HEAD_DIM), jnp.float32)
    last = jax.ShapeDtypeStruct((rows, HEAD_DIM), jnp.bfloat16)
    return call(
        functools.partial(attend_body, bool(state), last_side, len(kv_blocks)),
        (kept, kept, kept) if last_side is None else last,
        *q,
        *kv_blocks,
        *state,
        in_specs=[VMEM] * (2 + len(kv_blocks) + len(state)),
        flops=16 * rows * key_rows * HEAD_DIM,
    )


def return_pick_body(where_ref, masks_ref, pick_ref):
    devices = masks_ref.shape[0]
    slots, rows = pick_ref.shape
    per = slots // devices
    masks = masks_ref[...].astype(jnp.float32).astype(jnp.bfloat16)
    counts = dot(masks, jnp.ones((devices, 128), jnp.bfloat16)).astype(jnp.bfloat16)
    sender = iota((slots, devices), 0) // per
    device = iota((slots, devices), 1)
    start = dot(as_bf16(device < sender), counts).astype(jnp.int32)
    count = dot(as_bf16(device == sender), counts).astype(jnp.int32)
    offset = ((where_ref[1] - start) & 7) + 8 * (iota((slots, 128), 0) % per)
    row = jnp.where(offset < count, (start + offset) >> 3, -1)
    for r in range(0, rows, 128):
        pick_ref[:, r : r + 128] = as_bf16(row == iota((slots, 128), 1) + r)


def partial_line(where_ref, own_ref, other_ref, weight_ref, outer, rows):
    first = where_ref[4] == 0
    own, other = own_ref[rows], other_ref[rows]
    heads = jnp.concatenate([jnp.where(first, own, other), jnp.where(first, other, own)], axis=1)
    width = heads.shape[1]
    for inner in range(SIDE):
        at = pl.multiple_of(plane_block(where_ref, outer, inner) * width, width)
        cols = slice(inner * width, (inner + 1) * width)
        yield cols, dot(heads, weight_ref[:, pl.ds(at, width)])


def far_partial_body(*refs):
    args, (top_ref, bottom_ref) = refs[:4], refs[4:]
    half = top_ref.shape[0]
    for cols, product in partial_line(*args, 3, slice(None)):
        product = product.astype(jnp.bfloat16)
        top_ref[:, cols] = product[:half]
        bottom_ref[:, cols] = product[half:]


def near_partial_body(*refs):
    args, (kept_ref, ahead_ref, behind_ref) = refs[:4], refs[4:]
    half = ahead_ref.shape[0]
    for cols, product in partial_line(*args, 1, slice(half, None)):
        ahead_ref[:, cols] = product.astype(jnp.bfloat16)
    for cols, product in partial_line(*args, 2, slice(0, half)):
        behind_ref[:, cols] = product.astype(jnp.bfloat16)
    for cols, product in partial_line(*args, 0, slice(None)):
        kept_ref[:, cols] = product


def relay_partial_body(*refs):
    args, (up_ref, down_ref), (ahead_ref, behind_ref) = refs[:4], refs[4:6], refs[6:]
    half = up_ref.shape[0]
    for cols, product in partial_line(*args, 1, slice(0, half)):
        ahead_ref[:, cols] = (product + up_ref[:, cols].astype(jnp.float32)).astype(jnp.bfloat16)
    for cols, product in partial_line(*args, 2, slice(half, None)):
        behind_ref[:, cols] = (product + down_ref[:, cols].astype(jnp.float32)).astype(
            jnp.bfloat16
        )


def add_line_body(kept_ref, *refs):
    tops, bottoms, out_refs = refs[:2], refs[2:4], refs[4:]
    half = tops[0].shape[0]
    width = out_refs[0].shape[1]
    for low, pair in enumerate((tops, bottoms)):
        rows = slice(low * half, (low + 1) * half)
        for i, out_ref in enumerate(out_refs):
            cols = slice(i * width, (i + 1) * width)
            one, two = (r[:, cols].astype(jnp.float32) for r in pair)
            out_ref[rows] = (kept_ref[rows, cols] + (one + two)).astype(out_ref.dtype)


def send_back_body(pick_ref, *refs):
    blocks, out_ref = refs[:-1], refs[-1]
    a, b, c, d = (r[...].astype(jnp.float32) for r in blocks)
    projected = ((a + b) + (c + d)).astype(jnp.bfloat16)
    out_ref[...] = dot(pick_ref[...], projected).astype(jnp.bfloat16)


def finish_body(pick_ref, returned_ref, embedded_ref, filler_ref, out_ref):
    pick = pick_ref[...]
    width = returned_ref.shape[2]
    kept = dot(pick, jnp.ones((pick.shape[0], width), jnp.bfloat16), ((0,), (0,))) > 0.5
    for s in range(returned_ref.shape[0]):
        cols = slice(s * width, (s + 1) * width)
        projected = dot(pick, returned_ref[s], ((0,), (0,)))
        finished = embedded_ref[:, cols].astype(jnp.float32) + projected
        out_ref[:, cols] = jnp.where(kept, finished, filler_ref[:, cols])


def finish(pick, returned, embedded, filler):
    blocks, tokens, width = returned.shape
    step = 4
    by_column = lambda rows: pl.BlockSpec((rows, step * width), lambda i: (0, i))
    return pl.pallas_call(
        finish_body,
        grid=(blocks // step,),
        out_shape=jax.ShapeDtypeStruct(embedded.shape, jnp.float32),
        in_specs=[
            pl.BlockSpec(pick.shape, lambda i: (0, 0)),
            pl.BlockSpec((step, tokens, width), lambda i: (i, 0, 0)),
            by_column(tokens),
            by_column(1),
        ],
        out_specs=by_column(tokens),
        compiler_params=pltpu.CompilerParams(vmem_limit_bytes=16 * MIB),
    )(pick, returned, embedded, filler)


def position_table(positions, feature_width):
    half_width = feature_width // 2
    frequency = jnp.exp(-math.log(10000.0) * jnp.arange(half_width, dtype=jnp.float32) / half_width)
    angles = positions.astype(jnp.float32)[:, None] * frequency[None, :]
    return jnp.concatenate([jnp.sin(angles), jnp.cos(angles)], axis=1)


def embed(tokens, modality, positions, modal_table):
    table_rows = jnp.where(modality[:, None] == 1, modal_table[1][None, :], modal_table[0][None, :])
    summed = tokens.astype(jnp.float32) + position_table(positions, tokens.shape[1]) + table_rows
    return summed.astype(jnp.bfloat16)


def layer_norm(embedded, norm_gain, norm_bias):
    values = embedded.astype(jnp.float32)
    row_mean = jnp.mean(values, axis=1, keepdims=True)
    centered = values - row_mean
    row_var = jnp.mean(centered * centered, axis=1, keepdims=True)
    return (centered * lax.rsqrt(row_var + EPSILON) * norm_gain + norm_bias).astype(jnp.bfloat16)


def local(
    tokens,
    modality,
    keep_mask,
    positions,
    modal_table,
    norm_gain,
    norm_bias,
    qkv_weight,
    out_weight,
    mask_token,
):
    tok_rows, feature_width = tokens.shape
    seq_count = lax.axis_size("seq")
    ctx_count = lax.axis_size("ctx")
    devices = seq_count * ctx_count
    everyone = ("seq", "ctx")
    seq, ctx = lax.axis_index("seq"), lax.axis_index("ctx")
    core = ctx % 2
    where = jnp.stack([seq * ctx_count + ctx, ctx, seq // SIDE, seq % SIDE, core]).astype(jnp.int32)
    group_rows = tok_rows * seq_count // 4
    width = feature_width // seq_count
    per = tok_rows // ctx_count
    bf16 = lambda *shape: jax.ShapeDtypeStruct(shape, jnp.bfloat16)

    masks = call(
        repeat_body,
        jax.ShapeDtypeStruct((devices, 1, tok_rows), jnp.int32),
        keep_mask[None, :],
        in_specs=[VMEM],
    )
    masks = lax.all_to_all(masks, everyone, 0, 0, tiled=True).reshape(devices, tok_rows)
    embedded = embed(tokens, modality, positions, modal_table)
    normed = layer_norm(embedded, norm_gain, norm_bias)
    outgoing, pick = call(
        dispatch_body,
        (bf16(seq_count, tok_rows, width), bf16(tok_rows, tok_rows)),
        where,
        masks,
        keep_mask[None, :],
        normed,
        in_specs=[SMEM, VMEM, VMEM, VMEM],
        flops=2 * tok_rows * tok_rows * feature_width,
    )
    arrived = lax.all_to_all(outgoing.reshape(devices, per, width), everyone, 0, 0, tiled=True)
    block = call(
        compact_body,
        bf16(group_rows, width),
        where,
        masks,
        arrived.reshape(devices * per, width),
        in_specs=[SMEM, VMEM, VMEM],
        flops=2 * group_rows * devices * per * width,
    )
    half_line = bf16(group_rows // 2, SIDE * width)
    blocks = gather_line(block)
    qkv_weight, block = lax.optimization_barrier((qkv_weight, block))
    ordered = call(
        reorder_body,
        bf16(*qkv_weight.shape),
        where,
        qkv_weight,
        in_specs=[SMEM, HBM],
        scratch=(pltpu.SemaphoreType.DMA((SIDE * SIDE,)),),
        flops=1 << 32,
    )
    *blocks, ordered = lax.optimization_barrier((*blocks, ordered))
    line = call(line_body, (half_line, half_line), *blocks, in_specs=[VMEM] * SIDE)
    near_lines, far_lines = gather_long_line(*line)
    near = call(
        qkv_near_body,
        jax.ShapeDtypeStruct((3, group_rows, width), jnp.float32),
        ordered,
        *near_lines,
        in_specs=[VMEM] * 7,
        flops=6 * group_rows * feature_width * width * 3 // 4,
    )
    row_q, row_kv = bf16(group_rows, HEAD_DIM), bf16(group_rows, 2 * HEAD_DIM)
    my_q, my_kv, other_q, other_kv = call(
        qkv_far_body,
        (row_q, row_kv, row_q, row_kv),
        where,
        near,
        ordered,
        *far_lines,
        in_specs=[SMEM] + [VMEM] * 4,
        flops=6 * group_rows * feature_width * width // 4,
    )
    their_kv = lax.ppermute(other_kv, "ctx", CORE_SWAP)
    their_q = lax.ppermute(other_q, "ctx", CORE_SWAP)
    behind_mine = lax.ppermute(my_kv, "ctx", z_shift(1))
    ahead_theirs = lax.ppermute(their_kv, "ctx", z_shift(-1))
    behind_theirs = lax.ppermute(their_kv, "ctx", z_shift(1))
    ahead_mine = lax.ppermute(my_kv, "ctx", z_shift(-1))
    q = (my_q, their_q)
    state = attend(q, (my_kv, their_kv))
    behind_mine, ahead_theirs, *state = lax.optimization_barrier(
        (behind_mine, ahead_theirs, *state)
    )
    far = (
        lax.ppermute(behind_mine, "ctx", z_shift(1)),
        lax.ppermute(ahead_theirs, "ctx", z_shift(-1)),
    )
    state = attend(q, (behind_mine, ahead_theirs), state)
    state = attend(q, (behind_theirs, ahead_mine), state)
    for_other = attend(q, far, state, 1)
    from_other = lax.ppermute(for_other, "ctx", CORE_SWAP)
    *far, for_other = lax.optimization_barrier((*far, for_other))
    own_head = attend(q, far, state, 0)
    heads_args = (where, own_head, from_other, out_weight)
    heads_specs = [SMEM, VMEM, VMEM, VMEM]
    far_top, far_bottom = call(
        far_partial_body,
        (half_line, half_line),
        *heads_args,
        in_specs=heads_specs,
        flops=group_rows * feature_width * width // 2,
    )
    kept, ahead_bottom, behind_top = call(
        near_partial_body,
        (jax.ShapeDtypeStruct((group_rows, SIDE * width), jnp.float32), half_line, half_line),
        *heads_args,
        in_specs=heads_specs,
        flops=group_rows * feature_width * width,
    )
    ahead_top, behind_bottom = call(
        relay_partial_body,
        (half_line, half_line),
        *heads_args,
        send(far_top, 1, 1),
        send(far_bottom, 1, -1),
        in_specs=heads_specs + [VMEM] * 2,
        flops=group_rows * feature_width * width // 2,
    )
    sums = call(
        add_line_body,
        [jax.ShapeDtypeStruct((group_rows, width), jnp.float32)] + [bf16(group_rows, width)] * 3,
        kept,
        send(ahead_top, 1, 1),
        send(behind_top, 1, -1),
        send(ahead_bottom, 1, 1),
        send(behind_bottom, 1, -1),
        in_specs=[VMEM] * 5,
    )
    blocks = scatter_line(sums)
    masks, _ = lax.optimization_barrier((masks, own_head))
    return_pick = call(
        return_pick_body,
        bf16(devices * per, group_rows),
        where,
        masks,
        in_specs=[SMEM, VMEM],
        flops=2 * devices * per * tok_rows * group_rows,
    )
    returning = call(
        send_back_body,
        bf16(devices * per, width),
        return_pick,
        *blocks,
        in_specs=[VMEM] * (1 + SIDE),
        flops=2 * devices * per * group_rows * width,
    )
    returned = lax.all_to_all(returning.reshape(devices, per, width), everyone, 0, 0, tiled=True)
    return finish(
        pick, returned.reshape(seq_count, tok_rows, width), embedded, mask_token[None, :]
    )


def solution(mesh):
    in_specs = (
        P(("seq", "ctx"), None),
        P(("seq", "ctx")),
        P(("seq", "ctx")),
        P(("seq", "ctx")),
        P(),
        P(),
        P(),
        P(None, None, "seq"),
        P("seq", None),
        P(),
    )
    out_specs = P(("seq", "ctx"), None)
    return jax.shard_map(local, mesh=mesh, in_specs=in_specs, out_specs=out_specs, check_vma=False)
```

```python
import functools
import itertools
import math

import jax
import jax.numpy as jnp
from jax import lax
from jax.experimental import pallas as pl
from jax.experimental.pallas import tpu as pltpu
from jax.sharding import PartitionSpec as P

HEAD_DIM = 128
EPSILON = 1e-06
SIDE = 4
MIB = 1 << 20


EVERYONE = ("seq", "ctx")


def plane_shift(leg, d):
    pairs = []
    for y, x, z, k in itertools.product(range(SIDE), range(SIDE), range(SIDE), range(2)):
        to = ((y + d) % SIDE, x) if leg == k else (y, (x + d) % SIDE)
        pairs.append(tuple(((v * SIDE + u) * SIDE + z) * 2 + k for v, u in ((y, x), to)))
    return pairs


def z_shift(d):
    return [(z * 2 + k, (z + d) % SIDE * 2 + k) for z in range(SIDE) for k in range(2)]


CORE_SWAP = [(z * 2 + k, z * 2 + 1 - k) for z in range(SIDE) for k in range(2)]


RING = (0, 1, 3, 2)


def send(block, leg, d):
    return lax.ppermute(block, EVERYONE, plane_shift(leg, d))


def gather_line(block):
    return [block, send(block, 0, 2), send(block, 0, -1), send(block, 0, 1)]


def gather_long_line(top, bottom):
    behind_top, ahead_bottom = send(top, 1, 1), send(bottom, 1, -1)
    behind_bottom, ahead_top = send(bottom, 1, 1), send(top, 1, -1)
    far_top, far_bottom = send(behind_top, 1, 1), send(ahead_bottom, 1, -1)
    near = (top, bottom, ahead_top, ahead_bottom, behind_top, behind_bottom)
    return near, (far_top, far_bottom)


def scatter_line(blocks):
    own, ahead, behind, far = blocks
    return own, send(far, 0, 2), send(ahead, 0, 1), send(behind, 0, -1)


def call(body, outs, *args, scratch=(), limit=16, flops=0, in_specs=None):
    vmem = pl.BlockSpec(memory_space=pltpu.VMEM)
    many = isinstance(outs, (tuple, list))
    return pl.pallas_call(
        body,
        out_shape=outs,
        in_specs=in_specs,
        out_specs=[vmem] * len(outs) if many else vmem,
        scratch_shapes=list(scratch),
        compiler_params=pltpu.CompilerParams(vmem_limit_bytes=limit * MIB),
        cost_estimate=pl.CostEstimate(
            flops=flops, transcendentals=0, bytes_accessed=sum(a.size * 2 for a in args)
        ),
    )(*args)


VMEM = pl.BlockSpec(memory_space=pltpu.VMEM)
SMEM = pl.BlockSpec(memory_space=pltpu.SMEM)
ANY = pl.BlockSpec(memory_space=pl.ANY)
HBM = pl.BlockSpec(memory_space=pltpu.HBM)


def dot(a, b, dims=((1,), (0,))):
    return lax.dot_general(a, b, (dims, ((), ())), preferred_element_type=jnp.float32)


def iota(shape, dim):
    return lax.broadcasted_iota(jnp.int32, shape, dim)


def as_bf16(flag):
    return jnp.where(flag, 1.0, 0.0).astype(jnp.bfloat16)


def counts_in_lanes(masks):
    return dot(jnp.ones((8, masks.shape[1]), jnp.bfloat16), masks, ((1,), (1,)))


def repeat_body(row_ref, out_ref):
    out_ref[...] = jnp.broadcast_to(row_ref[...][None], out_ref.shape)


def dispatch_body(where_ref, masks_ref, own_ref, normed_ref, out_ref, pick_ref):
    tokens = own_ref.shape[1]
    masks = masks_ref[...].astype(jnp.float32).astype(jnp.bfloat16)
    counts = counts_in_lanes(masks)[0:1]
    start = jnp.sum(
        jnp.where(iota(counts.shape, 1) < where_ref[0], counts, 0.0), axis=1, keepdims=True
    ).astype(jnp.int32)
    own = own_ref[...]
    wide = jnp.broadcast_to(own.astype(jnp.float32).astype(jnp.bfloat16), (8, tokens))
    upto = as_bf16(iota((tokens, tokens), 0) <= iota((tokens, tokens), 1))
    rank = dot(wide, upto)[0:1].astype(jnp.int32) - 1
    slot = ((start + rank) & 7) * (tokens // 8) + (rank >> 3)
    slot = jnp.where(own == 1, slot, -1)
    pick = as_bf16(iota((tokens, tokens), 0) == slot)
    pick_ref[...] = pick
    width = out_ref.shape[2]
    for s in range(out_ref.shape[0]):
        out_ref[s] = dot(pick, normed_ref[:, s * width : (s + 1) * width]).astype(jnp.bfloat16)


def compact_body(where_ref, masks_ref, arrived_ref, out_ref):
    devices = masks_ref.shape[0]
    slots = arrived_ref.shape[0]
    per = slots // devices
    masks = masks_ref[...].astype(jnp.float32).astype(jnp.bfloat16)
    counts = counts_in_lanes(masks).astype(jnp.bfloat16)
    sender = iota((devices, slots), 1) // per
    device = iota((devices, slots), 0)
    start = dot(counts, as_bf16(device < sender))[0:1].astype(jnp.int32)
    count = dot(counts, as_bf16(device == sender))[0:1].astype(jnp.int32)
    offset = ((where_ref[1] - start) & 7) + 8 * (iota((1, slots), 1) % per)
    row = jnp.where(offset < count, (start + offset) >> 3, -1)
    arrived = arrived_ref[...]
    for r in range(0, out_ref.shape[0], 128):
        pick = as_bf16(iota((128, slots), 0) + r == row)
        out_ref[r : r + 128] = dot(pick, arrived).astype(jnp.bfloat16)


def line_body(*refs):
    blocks, (top_ref, bottom_ref) = refs[:-2], refs[-2:]
    half = top_ref.shape[0]
    width = blocks[0].shape[1]
    own, far, ahead, behind = blocks
    for i, block in enumerate((own, ahead, behind, far)):
        cols = slice(i * width, (i + 1) * width)
        top_ref[:, cols] = block[:half]
        bottom_ref[:, cols] = block[half:]


def plane_block(where_ref, outer, inner):
    first = where_ref[4] == 0
    y = jnp.where(first, RING[inner], RING[outer])
    x = jnp.where(first, RING[outer], RING[inner])
    return (where_ref[2] + y) % SIDE * SIDE + (where_ref[3] + x) % SIDE


def reorder_body(where_ref, weight_ref, out_ref, sems):
    width = weight_ref.shape[2]
    copies = []
    for outer in range(SIDE):
        for inner in range(SIDE):
            i = outer * SIDE + inner
            at = pl.multiple_of(plane_block(where_ref, outer, inner) * width, width)
            copies.append(
                pltpu.make_async_copy(
                    weight_ref.at[:, pl.ds(at, width), :],
                    out_ref.at[:, i * width : (i + 1) * width, :],
                    sems.at[i],
                )
            )
            copies[-1].start()
    for copy in copies:
        copy.wait()


def qkv_near_body(w_ref, *refs):
    lines, out_ref = refs[:-1], refs[-1]
    half, long = lines[0].shape
    for low in range(2):
        for t in range(3):
            total = None
            for i in range(3):
                product = dot(lines[2 * i + low][...], w_ref[t, i * long : (i + 1) * long])
                total = product if total is None else total + product
            out_ref[t, low * half : (low + 1) * half] = total


def qkv_far_body(where_ref, near_ref, w_ref, *refs):
    lines, (my_q, my_kv, other_q, other_kv) = refs[:2], refs[2:]
    half, long = lines[0].shape
    second = where_ref[4] == 1
    for low, line in enumerate(lines):
        rows = slice(low * half, (low + 1) * half)
        for t in range(3):
            total = near_ref[t, rows] + dot(line[...], w_ref[t, 3 * long :])
            both = total.astype(jnp.bfloat16)
            left, right = both[:, :HEAD_DIM], both[:, HEAD_DIM:]
            mine, other = (my_q, other_q) if t == 0 else (my_kv, other_kv)
            cols = slice(0, HEAD_DIM) if t < 2 else slice(HEAD_DIM, 2 * HEAD_DIM)
            mine[rows, cols] = jnp.where(second, right, left)
            other[rows, cols] = jnp.where(second, left, right)


def attend_body(has_state, last_side, keys, *refs):
    q_refs, kv_refs, refs = refs[:2], refs[2 : 2 + keys], refs[2 + keys :]
    state_refs, out_refs = (refs[:3], refs[3:]) if has_state else ((), refs)
    scale = math.log2(math.e) / math.sqrt(HEAD_DIM)
    rows = q_refs[0].shape[0]
    tile = 256
    per_side = rows // tile
    is_last = last_side is not None

    def one_tile(i):
        at = pl.ds(pl.multiple_of(i * tile, tile), tile)
        here = pl.ds(pl.multiple_of(i % per_side * tile, tile), tile)
        if is_last:
            q = q_refs[last_side][here]
        else:
            q = jnp.where(i < per_side, q_refs[0][here], q_refs[1][here])
        scores = [dot(q, kv_ref[:, :HEAD_DIM], ((1,), (1,))) for kv_ref in kv_refs]
        tops = [jnp.max(s, axis=1, keepdims=True) for s in scores]
        if has_state:
            acc = state_refs[0][at]
            top = state_refs[1][at][:, 0:1]
            total = state_refs[2][at][:, 0:1]
            tops.append(top)
        new_top = tops[0]
        for t in tops[1:]:
            new_top = jnp.maximum(new_top, t)
        product = block_total = None
        for s, kv_ref in zip(scores, kv_refs):
            expanded = jnp.exp2((s - new_top) * scale)
            part_total = jnp.sum(expanded, axis=1, keepdims=True)
            part = dot(expanded.astype(jnp.bfloat16), kv_ref[:, HEAD_DIM:])
            product = part if product is None else product + part
            block_total = part_total if block_total is None else block_total + part_total
        if has_state:
            factor = jnp.exp2((top - new_top) * scale)
            product = acc * factor + product
            block_total = total * factor + block_total
        if is_last:
            out_refs[0][here] = (product / block_total).astype(jnp.bfloat16)
        else:
            out_refs[0][at] = product
            out_refs[1][at] = jnp.broadcast_to(new_top, product.shape)
            out_refs[2][at] = jnp.broadcast_to(block_total, product.shape)

    if is_last:
        first_tile, tiles = last_side * per_side, per_side
    else:
        first_tile, tiles = 0, 2 * per_side
    lax.fori_loop(first_tile, first_tile + tiles, lambda i, _: one_tile(i), None)


def attend(q, kv_blocks, state=(), last_side=None):
    rows = q[0].shape[0]
    key_rows = sum(b.shape[0] for b in kv_blocks)
    kept = jax.ShapeDtypeStruct((2 * rows, HEAD_DIM), jnp.float32)
    last = jax.ShapeDtypeStruct((rows, HEAD_DIM), jnp.bfloat16)
    return call(
        functools.partial(attend_body, bool(state), last_side, len(kv_blocks)),
        (kept, kept, kept) if last_side is None else last,
        *q,
        *kv_blocks,
        *state,
        in_specs=[VMEM] * (2 + len(kv_blocks) + len(state)),
        flops=16 * rows * key_rows * HEAD_DIM,
    )


def return_pick_body(where_ref, masks_ref, pick_ref):
    devices = masks_ref.shape[0]
    slots, rows = pick_ref.shape
    per = slots // devices
    masks = masks_ref[...].astype(jnp.float32).astype(jnp.bfloat16)
    counts = dot(masks, jnp.ones((devices, 128), jnp.bfloat16)).astype(jnp.bfloat16)
    sender = iota((slots, devices), 0) // per
    device = iota((slots, devices), 1)
    start = dot(as_bf16(device < sender), counts).astype(jnp.int32)
    count = dot(as_bf16(device == sender), counts).astype(jnp.int32)
    offset = ((where_ref[1] - start) & 7) + 8 * (iota((slots, 128), 0) % per)
    row = jnp.where(offset < count, (start + offset) >> 3, -1)
    for r in range(0, rows, 128):
        pick_ref[:, r : r + 128] = as_bf16(row == iota((slots, 128), 1) + r)


def partial_line(where_ref, own_ref, other_ref, weight_ref, outer, rows):
    first = where_ref[4] == 0
    own, other = own_ref[rows], other_ref[rows]
    heads = jnp.concatenate([jnp.where(first, own, other), jnp.where(first, other, own)], axis=1)
    width = heads.shape[1]
    for inner in range(SIDE):
        at = pl.multiple_of(plane_block(where_ref, outer, inner) * width, width)
        cols = slice(inner * width, (inner + 1) * width)
        yield cols, dot(heads, weight_ref[:, pl.ds(at, width)])


def far_partial_body(*refs):
    args, (top_ref, bottom_ref) = refs[:4], refs[4:]
    half = top_ref.shape[0]
    for cols, product in partial_line(*args, 3, slice(None)):
        product = product.astype(jnp.bfloat16)
        top_ref[:, cols] = product[:half]
        bottom_ref[:, cols] = product[half:]


def near_partial_body(*refs):
    args, (kept_ref, ahead_ref, behind_ref) = refs[:4], refs[4:]
    half = ahead_ref.shape[0]
    for cols, product in partial_line(*args, 1, slice(half, None)):
        ahead_ref[:, cols] = product.astype(jnp.bfloat16)
    for cols, product in partial_line(*args, 2, slice(0, half)):
        behind_ref[:, cols] = product.astype(jnp.bfloat16)
    for cols, product in partial_line(*args, 0, slice(None)):
        kept_ref[:, cols] = product


def relay_partial_body(*refs):
    args, (up_ref, down_ref), (ahead_ref, behind_ref) = refs[:4], refs[4:6], refs[6:]
    half = up_ref.shape[0]
    for cols, product in partial_line(*args, 1, slice(0, half)):
        ahead_ref[:, cols] = (product + up_ref[:, cols].astype(jnp.float32)).astype(jnp.bfloat16)
    for cols, product in partial_line(*args, 2, slice(half, None)):
        behind_ref[:, cols] = (product + down_ref[:, cols].astype(jnp.float32)).astype(
            jnp.bfloat16
        )


def add_line_body(kept_ref, *refs):
    tops, bottoms, out_refs = refs[:2], refs[2:4], refs[4:]
    half = tops[0].shape[0]
    width = out_refs[0].shape[1]
    for low, pair in enumerate((tops, bottoms)):
        rows = slice(low * half, (low + 1) * half)
        for i, out_ref in enumerate(out_refs):
            cols = slice(i * width, (i + 1) * width)
            one, two = (r[:, cols].astype(jnp.float32) for r in pair)
            out_ref[rows] = (kept_ref[rows, cols] + (one + two)).astype(out_ref.dtype)


def send_back_body(pick_ref, *refs):
    blocks, out_ref = refs[:-1], refs[-1]
    a, b, c, d = (r[...].astype(jnp.float32) for r in blocks)
    projected = ((a + b) + (c + d)).astype(jnp.bfloat16)
    out_ref[...] = dot(pick_ref[...], projected).astype(jnp.bfloat16)


def finish_body(pick_ref, returned_ref, embedded_ref, filler_ref, out_ref):
    pick = pick_ref[...]
    width = returned_ref.shape[2]
    kept = dot(pick, jnp.ones((pick.shape[0], width), jnp.bfloat16), ((0,), (0,))) > 0.5
    for s in range(returned_ref.shape[0]):
        cols = slice(s * width, (s + 1) * width)
        projected = dot(pick, returned_ref[s], ((0,), (0,)))
        finished = embedded_ref[:, cols].astype(jnp.float32) + projected
        out_ref[:, cols] = jnp.where(kept, finished, filler_ref[:, cols])


def position_table(positions, feature_width):
    half_width = feature_width // 2
    frequency = jnp.exp(-math.log(10000.0) * jnp.arange(half_width, dtype=jnp.float32) / half_width)
    angles = positions.astype(jnp.float32)[:, None] * frequency[None, :]
    return jnp.concatenate([jnp.sin(angles), jnp.cos(angles)], axis=1)


def embed(tokens, modality, positions, modal_table):
    table_rows = jnp.where(modality[:, None] == 1, modal_table[1][None, :], modal_table[0][None, :])
    summed = tokens.astype(jnp.float32) + position_table(positions, tokens.shape[1]) + table_rows
    return summed.astype(jnp.bfloat16)


def layer_norm(embedded, norm_gain, norm_bias):
    values = embedded.astype(jnp.float32)
    row_mean = jnp.mean(values, axis=1, keepdims=True)
    centered = values - row_mean
    row_var = jnp.mean(centered * centered, axis=1, keepdims=True)
    return (centered * lax.rsqrt(row_var + EPSILON) * norm_gain + norm_bias).astype(jnp.bfloat16)


def local(
    tokens,
    modality,
    keep_mask,
    positions,
    modal_table,
    norm_gain,
    norm_bias,
    qkv_weight,
    out_weight,
    mask_token,
):
    tok_rows, feature_width = tokens.shape
    seq_count = lax.axis_size("seq")
    ctx_count = lax.axis_size("ctx")
    devices = seq_count * ctx_count
    everyone = ("seq", "ctx")
    seq, ctx = lax.axis_index("seq"), lax.axis_index("ctx")
    core = ctx % 2
    where = jnp.stack([seq * ctx_count + ctx, ctx, seq // SIDE, seq % SIDE, core]).astype(jnp.int32)
    group_rows = tok_rows * seq_count // 4
    width = feature_width // seq_count
    per = tok_rows // ctx_count
    bf16 = lambda *shape: jax.ShapeDtypeStruct(shape, jnp.bfloat16)

    masks = call(
        repeat_body,
        jax.ShapeDtypeStruct((devices, 1, tok_rows), jnp.int32),
        keep_mask[None, :],
        in_specs=[VMEM],
    )
    masks = lax.all_to_all(masks, everyone, 0, 0, tiled=True).reshape(devices, tok_rows)
    embedded = embed(tokens, modality, positions, modal_table)
    normed = layer_norm(embedded, norm_gain, norm_bias)
    outgoing, pick = call(
        dispatch_body,
        (bf16(seq_count, tok_rows, width), bf16(tok_rows, tok_rows)),
        where,
        masks,
        keep_mask[None, :],
        normed,
        in_specs=[SMEM, VMEM, VMEM, VMEM],
        flops=2 * tok_rows * tok_rows * feature_width,
    )
    arrived = lax.all_to_all(outgoing.reshape(devices, per, width), everyone, 0, 0, tiled=True)
    block = call(
        compact_body,
        bf16(group_rows, width),
        where,
        masks,
        arrived.reshape(devices * per, width),
        in_specs=[SMEM, VMEM, VMEM],
        flops=2 * group_rows * devices * per * width,
    )
    half_line = bf16(group_rows // 2, SIDE * width)
    blocks = gather_line(block)
    qkv_weight, block = lax.optimization_barrier((qkv_weight, block))
    ordered = call(
        reorder_body,
        bf16(*qkv_weight.shape),
        where,
        qkv_weight,
        in_specs=[SMEM, HBM],
        scratch=(pltpu.SemaphoreType.DMA((SIDE * SIDE,)),),
        flops=1 << 32,
    )
    *blocks, ordered = lax.optimization_barrier((*blocks, ordered))
    line = call(line_body, (half_line, half_line), *blocks, in_specs=[VMEM] * SIDE)
    near_lines, far_lines = gather_long_line(*line)
    near = call(
        qkv_near_body,
        jax.ShapeDtypeStruct((3, group_rows, width), jnp.float32),
        ordered,
        *near_lines,
        in_specs=[VMEM] * 7,
        flops=6 * group_rows * feature_width * width * 3 // 4,
    )
    row_q, row_kv = bf16(group_rows, HEAD_DIM), bf16(group_rows, 2 * HEAD_DIM)
    my_q, my_kv, other_q, other_kv = call(
        qkv_far_body,
        (row_q, row_kv, row_q, row_kv),
        where,
        near,
        ordered,
        *far_lines,
        in_specs=[SMEM] + [VMEM] * 4,
        flops=6 * group_rows * feature_width * width // 4,
    )
    their_kv = lax.ppermute(other_kv, "ctx", CORE_SWAP)
    their_q = lax.ppermute(other_q, "ctx", CORE_SWAP)
    behind_mine = lax.ppermute(my_kv, "ctx", z_shift(1))
    ahead_theirs = lax.ppermute(their_kv, "ctx", z_shift(-1))
    behind_theirs = lax.ppermute(their_kv, "ctx", z_shift(1))
    ahead_mine = lax.ppermute(my_kv, "ctx", z_shift(-1))
    q = (my_q, their_q)
    state = attend(q, (my_kv, their_kv))
    behind_mine, ahead_theirs, *state = lax.optimization_barrier(
        (behind_mine, ahead_theirs, *state)
    )
    far = (
        lax.ppermute(behind_mine, "ctx", z_shift(1)),
        lax.ppermute(ahead_theirs, "ctx", z_shift(-1)),
    )
    state = attend(q, (behind_mine, ahead_theirs), state)
    state = attend(q, (behind_theirs, ahead_mine), state)
    for_other = attend(q, far, state, 1)
    from_other = lax.ppermute(for_other, "ctx", CORE_SWAP)
    *far, for_other = lax.optimization_barrier((*far, for_other))
    own_head = attend(q, far, state, 0)
    heads_args = (where, own_head, from_other, out_weight)
    heads_specs = [SMEM, VMEM, VMEM, VMEM]
    far_top, far_bottom = call(
        far_partial_body,
        (half_line, half_line),
        *heads_args,
        in_specs=heads_specs,
        flops=group_rows * feature_width * width // 2,
    )
    kept, ahead_bottom, behind_top = call(
        near_partial_body,
        (jax.ShapeDtypeStruct((group_rows, SIDE * width), jnp.float32), half_line, half_line),
        *heads_args,
        in_specs=heads_specs,
        flops=group_rows * feature_width * width,
    )
    ahead_top, behind_bottom = call(
        relay_partial_body,
        (half_line, half_line),
        *heads_args,
        send(far_top, 1, 1),
        send(far_bottom, 1, -1),
        in_specs=heads_specs + [VMEM] * 2,
        flops=group_rows * feature_width * width // 2,
    )
    sums = call(
        add_line_body,
        [jax.ShapeDtypeStruct((group_rows, width), jnp.float32)] + [bf16(group_rows, width)] * 3,
        kept,
        send(ahead_top, 1, 1),
        send(behind_top, 1, -1),
        send(ahead_bottom, 1, 1),
        send(behind_bottom, 1, -1),
        in_specs=[VMEM] * 5,
    )
    blocks = scatter_line(sums)
    masks, _ = lax.optimization_barrier((masks, own_head))
    return_pick = call(
        return_pick_body,
        bf16(devices * per, group_rows),
        where,
        masks,
        in_specs=[SMEM, VMEM],
        flops=2 * devices * per * tok_rows * group_rows,
    )
    returning = call(
        send_back_body,
        bf16(devices * per, width),
        return_pick,
        *blocks,
        in_specs=[VMEM] * (1 + SIDE),
        flops=2 * devices * per * group_rows * width,
    )
    returned = lax.all_to_all(returning.reshape(devices, per, width), everyone, 0, 0, tiled=True)
    return call(
        finish_body,
        jax.ShapeDtypeStruct((tok_rows, feature_width), jnp.float32),
        pick,
        returned.reshape(seq_count, tok_rows, width),
        embedded,
        mask_token[None, :],
        in_specs=[VMEM] * 4,
        flops=2 * tok_rows * tok_rows * feature_width,
    )


def solution(mesh):
    in_specs = (
        P(("seq", "ctx"), None),
        P(("seq", "ctx")),
        P(("seq", "ctx")),
        P(("seq", "ctx")),
        P(),
        P(),
        P(),
        P(None, None, "seq"),
        P("seq", None),
        P(),
    )
    out_specs = P(("seq", "ctx"), None)
    return jax.shard_map(local, mesh=mesh, in_specs=in_specs, out_specs=out_specs, check_vma=False)
```

```python
import functools
import itertools
import math

import jax
import jax.numpy as jnp
from jax import lax
from jax.experimental import pallas as pl
from jax.experimental.pallas import tpu as pltpu
from jax.sharding import PartitionSpec as P

HEAD_DIM = 128
EPSILON = 1e-06
SIDE = 4
MIB = 1 << 20


EVERYONE = ("seq", "ctx")


def plane_shift(leg, d):
    pairs = []
    for y, x, z, k in itertools.product(range(SIDE), range(SIDE), range(SIDE), range(2)):
        to = ((y + d) % SIDE, x) if leg == k else (y, (x + d) % SIDE)
        pairs.append(tuple(((v * SIDE + u) * SIDE + z) * 2 + k for v, u in ((y, x), to)))
    return pairs


def z_shift(d, cross=False):
    return [
        (z * 2 + k, (z + d) % SIDE * 2 + (1 - k if cross else k))
        for z in range(SIDE)
        for k in range(2)
    ]


CORE_SWAP = [(z * 2 + k, z * 2 + 1 - k) for z in range(SIDE) for k in range(2)]


RING = (0, 1, 3, 2)


def send(block, leg, d):
    return lax.ppermute(block, EVERYONE, plane_shift(leg, d))


def gather_line(block):
    return [block, send(block, 0, 2), send(block, 0, -1), send(block, 0, 1)]


def gather_long_line(top, bottom):
    behind_top, ahead_bottom = send(top, 1, 1), send(bottom, 1, -1)
    behind_bottom, ahead_top = send(bottom, 1, 1), send(top, 1, -1)
    far_top, far_bottom = send(behind_top, 1, 1), send(ahead_bottom, 1, -1)
    near = (top, bottom, ahead_top, ahead_bottom, behind_top, behind_bottom)
    return near, (far_top, far_bottom)


def scatter_line(blocks):
    own, ahead, behind, far = blocks
    return own, send(far, 0, 2), send(ahead, 0, 1), send(behind, 0, -1)


def call(body, outs, *args, scratch=(), limit=16, flops=0, in_specs=None):
    vmem = pl.BlockSpec(memory_space=pltpu.VMEM)
    many = isinstance(outs, (tuple, list))
    return pl.pallas_call(
        body,
        out_shape=outs,
        in_specs=in_specs,
        out_specs=[vmem] * len(outs) if many else vmem,
        scratch_shapes=list(scratch),
        compiler_params=pltpu.CompilerParams(vmem_limit_bytes=limit * MIB),
        cost_estimate=pl.CostEstimate(
            flops=flops, transcendentals=0, bytes_accessed=sum(a.size * 2 for a in args)
        ),
    )(*args)


VMEM = pl.BlockSpec(memory_space=pltpu.VMEM)
SMEM = pl.BlockSpec(memory_space=pltpu.SMEM)
ANY = pl.BlockSpec(memory_space=pl.ANY)
HBM = pl.BlockSpec(memory_space=pltpu.HBM)


def dot(a, b, dims=((1,), (0,))):
    return lax.dot_general(a, b, (dims, ((), ())), preferred_element_type=jnp.float32)


def iota(shape, dim):
    return lax.broadcasted_iota(jnp.int32, shape, dim)


def as_bf16(flag):
    return jnp.where(flag, 1.0, 0.0).astype(jnp.bfloat16)


def counts_in_lanes(masks):
    return dot(jnp.ones((8, masks.shape[1]), jnp.bfloat16), masks, ((1,), (1,)))


def repeat_body(row_ref, out_ref):
    out_ref[...] = jnp.broadcast_to(row_ref[...][None], out_ref.shape)


def dispatch_body(where_ref, masks_ref, own_ref, normed_ref, out_ref, pick_ref):
    tokens = own_ref.shape[1]
    masks = masks_ref[...].astype(jnp.float32).astype(jnp.bfloat16)
    counts = counts_in_lanes(masks)[0:1]
    start = jnp.sum(
        jnp.where(iota(counts.shape, 1) < where_ref[0], counts, 0.0), axis=1, keepdims=True
    ).astype(jnp.int32)
    own = own_ref[...]
    wide = jnp.broadcast_to(own.astype(jnp.float32).astype(jnp.bfloat16), (8, tokens))
    upto = as_bf16(iota((tokens, tokens), 0) <= iota((tokens, tokens), 1))
    rank = dot(wide, upto)[0:1].astype(jnp.int32) - 1
    slot = ((start + rank) & 7) * (tokens // 8) + (rank >> 3)
    slot = jnp.where(own == 1, slot, -1)
    pick = as_bf16(iota((tokens, tokens), 0) == slot)
    pick_ref[...] = pick
    width = out_ref.shape[2]
    for s in range(out_ref.shape[0]):
        out_ref[s] = dot(pick, normed_ref[:, s * width : (s + 1) * width]).astype(jnp.bfloat16)


def compact_body(where_ref, masks_ref, arrived_ref, out_ref):
    devices = masks_ref.shape[0]
    slots = arrived_ref.shape[0]
    per = slots // devices
    masks = masks_ref[...].astype(jnp.float32).astype(jnp.bfloat16)
    counts = counts_in_lanes(masks).astype(jnp.bfloat16)
    sender = iota((devices, slots), 1) // per
    device = iota((devices, slots), 0)
    start = dot(counts, as_bf16(device < sender))[0:1].astype(jnp.int32)
    count = dot(counts, as_bf16(device == sender))[0:1].astype(jnp.int32)
    offset = ((where_ref[1] - start) & 7) + 8 * (iota((1, slots), 1) % per)
    row = jnp.where(offset < count, (start + offset) >> 3, -1)
    arrived = arrived_ref[...]
    for r in range(0, out_ref.shape[0], 128):
        pick = as_bf16(iota((128, slots), 0) + r == row)
        out_ref[r : r + 128] = dot(pick, arrived).astype(jnp.bfloat16)


def line_body(*refs):
    blocks, (top_ref, bottom_ref) = refs[:-2], refs[-2:]
    half = top_ref.shape[0]
    width = blocks[0].shape[1]
    own, far, ahead, behind = blocks
    for i, block in enumerate((own, ahead, behind, far)):
        cols = slice(i * width, (i + 1) * width)
        top_ref[:, cols] = block[:half]
        bottom_ref[:, cols] = block[half:]


def plane_block(where_ref, outer, inner):
    first = where_ref[4] == 0
    y = jnp.where(first, RING[inner], RING[outer])
    x = jnp.where(first, RING[outer], RING[inner])
    return (where_ref[2] + y) % SIDE * SIDE + (where_ref[3] + x) % SIDE


def reorder_body(where_ref, weight_ref, out_ref, sems):
    width = weight_ref.shape[2]
    copies = []
    for outer in range(SIDE):
        for inner in range(SIDE):
            i = outer * SIDE + inner
            at = pl.multiple_of(plane_block(where_ref, outer, inner) * width, width)
            copies.append(
                pltpu.make_async_copy(
                    weight_ref.at[:, pl.ds(at, width), :],
                    out_ref.at[:, i * width : (i + 1) * width, :],
                    sems.at[i],
                )
            )
            copies[-1].start()
    for copy in copies:
        copy.wait()


def qkv_near_body(w_ref, *refs):
    lines, out_ref = refs[:-1], refs[-1]
    half, long = lines[0].shape
    for low in range(2):
        for t in range(3):
            total = None
            for i in range(3):
                product = dot(lines[2 * i + low][...], w_ref[t, i * long : (i + 1) * long])
                total = product if total is None else total + product
            out_ref[t, low * half : (low + 1) * half] = total


def qkv_far_body(where_ref, near_ref, w_ref, *refs):
    lines, (my_q, my_kv, other_q, other_kv) = refs[:2], refs[2:]
    half, long = lines[0].shape
    second = where_ref[4] == 1
    for low, line in enumerate(lines):
        rows = slice(low * half, (low + 1) * half)
        for t in range(3):
            total = near_ref[t, rows] + dot(line[...], w_ref[t, 3 * long :])
            both = total.astype(jnp.bfloat16)
            left, right = both[:, :HEAD_DIM], both[:, HEAD_DIM:]
            mine, other = (my_q, other_q) if t == 0 else (my_kv, other_kv)
            cols = slice(0, HEAD_DIM) if t < 2 else slice(HEAD_DIM, 2 * HEAD_DIM)
            mine[rows, cols] = jnp.where(second, right, left)
            other[rows, cols] = jnp.where(second, left, right)


def attend_body(has_state, last_side, keys, *refs):
    q_refs, kv_refs, refs = refs[:2], refs[2 : 2 + keys], refs[2 + keys :]
    state_refs, out_refs = (refs[:3], refs[3:]) if has_state else ((), refs)
    scale = math.log2(math.e) / math.sqrt(HEAD_DIM)
    rows = q_refs[0].shape[0]
    tile = 256
    per_side = rows // tile
    is_last = last_side is not None

    def one_tile(i):
        at = pl.ds(pl.multiple_of(i * tile, tile), tile)
        here = pl.ds(pl.multiple_of(i % per_side * tile, tile), tile)
        if is_last:
            q = q_refs[last_side][here]
        else:
            q = jnp.where(i < per_side, q_refs[0][here], q_refs[1][here])
        scores = [dot(q, kv_ref[:, :HEAD_DIM], ((1,), (1,))) for kv_ref in kv_refs]
        tops = [jnp.max(s, axis=1, keepdims=True) for s in scores]
        if has_state:
            acc = state_refs[0][at]
            top = state_refs[1][at][:, 0:1]
            total = state_refs[2][at][:, 0:1]
            tops.append(top)
        new_top = tops[0]
        for t in tops[1:]:
            new_top = jnp.maximum(new_top, t)
        product = block_total = None
        for s, kv_ref in zip(scores, kv_refs):
            expanded = jnp.exp2((s - new_top) * scale)
            part_total = jnp.sum(expanded, axis=1, keepdims=True)
            part = dot(expanded.astype(jnp.bfloat16), kv_ref[:, HEAD_DIM:])
            product = part if product is None else product + part
            block_total = part_total if block_total is None else block_total + part_total
        if has_state:
            factor = jnp.exp2((top - new_top) * scale)
            product = acc * factor + product
            block_total = total * factor + block_total
        if is_last:
            out_refs[0][here] = (product / block_total).astype(jnp.bfloat16)
        else:
            out_refs[0][at] = product
            out_refs[1][at] = jnp.broadcast_to(new_top, product.shape)
            out_refs[2][at] = jnp.broadcast_to(block_total, product.shape)

    if is_last:
        first_tile, tiles = last_side * per_side, per_side
    else:
        first_tile, tiles = 0, 2 * per_side
    lax.fori_loop(first_tile, first_tile + tiles, lambda i, _: one_tile(i), None)


def attend(q, kv_blocks, state=(), last_side=None):
    rows = q[0].shape[0]
    key_rows = sum(b.shape[0] for b in kv_blocks)
    kept = jax.ShapeDtypeStruct((2 * rows, HEAD_DIM), jnp.float32)
    last = jax.ShapeDtypeStruct((rows, HEAD_DIM), jnp.bfloat16)
    return call(
        functools.partial(attend_body, bool(state), last_side, len(kv_blocks)),
        (kept, kept, kept) if last_side is None else last,
        *q,
        *kv_blocks,
        *state,
        in_specs=[VMEM] * (2 + len(kv_blocks) + len(state)),
        flops=16 * rows * key_rows * HEAD_DIM,
    )


def return_pick_body(where_ref, masks_ref, pick_ref):
    devices = masks_ref.shape[0]
    slots, rows = pick_ref.shape
    per = slots // devices
    masks = masks_ref[...].astype(jnp.float32).astype(jnp.bfloat16)
    counts = dot(masks, jnp.ones((devices, 128), jnp.bfloat16)).astype(jnp.bfloat16)
    sender = iota((slots, devices), 0) // per
    device = iota((slots, devices), 1)
    start = dot(as_bf16(device < sender), counts).astype(jnp.int32)
    count = dot(as_bf16(device == sender), counts).astype(jnp.int32)
    offset = ((where_ref[1] - start) & 7) + 8 * (iota((slots, 128), 0) % per)
    row = jnp.where(offset < count, (start + offset) >> 3, -1)
    for r in range(0, rows, 128):
        pick_ref[:, r : r + 128] = as_bf16(row == iota((slots, 128), 1) + r)


def partial_line(where_ref, own_ref, other_ref, weight_ref, outer, rows):
    first = where_ref[4] == 0
    own, other = own_ref[rows], other_ref[rows]
    heads = jnp.concatenate([jnp.where(first, own, other), jnp.where(first, other, own)], axis=1)
    width = heads.shape[1]
    for inner in range(SIDE):
        at = pl.multiple_of(plane_block(where_ref, outer, inner) * width, width)
        cols = slice(inner * width, (inner + 1) * width)
        yield cols, dot(heads, weight_ref[:, pl.ds(at, width)])


def far_partial_body(*refs):
    args, (top_ref, bottom_ref) = refs[:4], refs[4:]
    half = top_ref.shape[0]
    for cols, product in partial_line(*args, 3, slice(None)):
        product = product.astype(jnp.bfloat16)
        top_ref[:, cols] = product[:half]
        bottom_ref[:, cols] = product[half:]


def near_partial_body(*refs):
    args, (kept_ref, ahead_ref, behind_ref) = refs[:4], refs[4:]
    half = ahead_ref.shape[0]
    for cols, product in partial_line(*args, 1, slice(half, None)):
        ahead_ref[:, cols] = product.astype(jnp.bfloat16)
    for cols, product in partial_line(*args, 2, slice(0, half)):
        behind_ref[:, cols] = product.astype(jnp.bfloat16)
    for cols, product in partial_line(*args, 0, slice(None)):
        kept_ref[:, cols] = product


def relay_partial_body(*refs):
    args, (up_ref, down_ref), (ahead_ref, behind_ref) = refs[:4], refs[4:6], refs[6:]
    half = up_ref.shape[0]
    for cols, product in partial_line(*args, 1, slice(0, half)):
        ahead_ref[:, cols] = (product + up_ref[:, cols].astype(jnp.float32)).astype(jnp.bfloat16)
    for cols, product in partial_line(*args, 2, slice(half, None)):
        behind_ref[:, cols] = (product + down_ref[:, cols].astype(jnp.float32)).astype(
            jnp.bfloat16
        )


def add_line_body(kept_ref, *refs):
    tops, bottoms, out_refs = refs[:2], refs[2:4], refs[4:]
    half = tops[0].shape[0]
    width = out_refs[0].shape[1]
    for low, pair in enumerate((tops, bottoms)):
        rows = slice(low * half, (low + 1) * half)
        for i, out_ref in enumerate(out_refs):
            cols = slice(i * width, (i + 1) * width)
            one, two = (r[:, cols].astype(jnp.float32) for r in pair)
            out_ref[rows] = (kept_ref[rows, cols] + (one + two)).astype(out_ref.dtype)


def send_back_body(pick_ref, *refs):
    blocks, out_ref = refs[:-1], refs[-1]
    a, b, c, d = (r[...].astype(jnp.float32) for r in blocks)
    projected = ((a + b) + (c + d)).astype(jnp.bfloat16)
    out_ref[...] = dot(pick_ref[...], projected).astype(jnp.bfloat16)


def finish_body(pick_ref, returned_ref, embedded_ref, filler_ref, out_ref, rows_ref, sems):
    pick = pick_ref[...]
    blocks, _, width = returned_ref.shape
    kept = dot(pick, jnp.ones((pick.shape[0], width), jnp.bfloat16), ((0,), (0,))) > 0.5
    group = blocks // sems.shape[0]
    copies = []
    for s in range(blocks):
        cols = slice(s * width, (s + 1) * width)
        projected = dot(pick, returned_ref[s], ((0,), (0,)))
        finished = embedded_ref[:, cols].astype(jnp.float32) + projected
        rows_ref[:, cols] = jnp.where(kept, finished, filler_ref[:, cols])
        if (s + 1) % group == 0:
            done = slice((s + 1 - group) * width, (s + 1) * width)
            copies.append(
                pltpu.make_async_copy(rows_ref.at[:, done], out_ref.at[:, done], sems.at[s // group])
            )
            copies[-1].start()
    for copy in copies:
        copy.wait()


def position_table(positions, feature_width):
    half_width = feature_width // 2
    frequency = jnp.exp(-math.log(10000.0) * jnp.arange(half_width, dtype=jnp.float32) / half_width)
    angles = positions.astype(jnp.float32)[:, None] * frequency[None, :]
    return jnp.concatenate([jnp.sin(angles), jnp.cos(angles)], axis=1)


def embed(tokens, modality, positions, modal_table):
    table_rows = jnp.where(modality[:, None] == 1, modal_table[1][None, :], modal_table[0][None, :])
    summed = tokens.astype(jnp.float32) + position_table(positions, tokens.shape[1]) + table_rows
    return summed.astype(jnp.bfloat16)


def layer_norm(embedded, norm_gain, norm_bias):
    values = embedded.astype(jnp.float32)
    row_mean = jnp.mean(values, axis=1, keepdims=True)
    centered = values - row_mean
    row_var = jnp.mean(centered * centered, axis=1, keepdims=True)
    return (centered * lax.rsqrt(row_var + EPSILON) * norm_gain + norm_bias).astype(jnp.bfloat16)


def local(
    tokens,
    modality,
    keep_mask,
    positions,
    modal_table,
    norm_gain,
    norm_bias,
    qkv_weight,
    out_weight,
    mask_token,
):
    tok_rows, feature_width = tokens.shape
    seq_count = lax.axis_size("seq")
    ctx_count = lax.axis_size("ctx")
    devices = seq_count * ctx_count
    everyone = ("seq", "ctx")
    seq, ctx = lax.axis_index("seq"), lax.axis_index("ctx")
    core = ctx % 2
    where = jnp.stack([seq * ctx_count + ctx, ctx, seq // SIDE, seq % SIDE, core]).astype(jnp.int32)
    group_rows = tok_rows * seq_count // 4
    width = feature_width // seq_count
    per = tok_rows // ctx_count
    bf16 = lambda *shape: jax.ShapeDtypeStruct(shape, jnp.bfloat16)

    masks = call(
        repeat_body,
        jax.ShapeDtypeStruct((devices, 1, tok_rows), jnp.int32),
        keep_mask[None, :],
        in_specs=[VMEM],
    )
    masks = lax.all_to_all(masks, everyone, 0, 0, tiled=True).reshape(devices, tok_rows)
    embedded = embed(tokens, modality, positions, modal_table)
    normed = layer_norm(embedded, norm_gain, norm_bias)
    outgoing, pick = call(
        dispatch_body,
        (bf16(seq_count, tok_rows, width), bf16(tok_rows, tok_rows)),
        where,
        masks,
        keep_mask[None, :],
        normed,
        in_specs=[SMEM, VMEM, VMEM, VMEM],
        flops=2 * tok_rows * tok_rows * feature_width,
    )
    arrived = lax.all_to_all(outgoing.reshape(devices, per, width), everyone, 0, 0, tiled=True)
    block = call(
        compact_body,
        bf16(group_rows, width),
        where,
        masks,
        arrived.reshape(devices * per, width),
        in_specs=[SMEM, VMEM, VMEM],
        flops=2 * group_rows * devices * per * width,
    )
    half_line = bf16(group_rows // 2, SIDE * width)
    blocks = gather_line(block)
    qkv_weight, block = lax.optimization_barrier((qkv_weight, block))
    ordered = call(
        reorder_body,
        bf16(*qkv_weight.shape),
        where,
        qkv_weight,
        in_specs=[SMEM, HBM],
        scratch=(pltpu.SemaphoreType.DMA((SIDE * SIDE,)),),
        flops=1 << 32,
    )
    *blocks, ordered = lax.optimization_barrier((*blocks, ordered))
    line = call(line_body, (half_line, half_line), *blocks, in_specs=[VMEM] * SIDE)
    near_lines, far_lines = gather_long_line(*line)
    near = call(
        qkv_near_body,
        jax.ShapeDtypeStruct((3, group_rows, width), jnp.float32),
        ordered,
        *near_lines,
        in_specs=[VMEM] * 7,
        flops=6 * group_rows * feature_width * width * 3 // 4,
    )
    row_q, row_kv = bf16(group_rows, HEAD_DIM), bf16(group_rows, 2 * HEAD_DIM)
    my_q, my_kv, other_q, other_kv = call(
        qkv_far_body,
        (row_q, row_kv, row_q, row_kv),
        where,
        near,
        ordered,
        *far_lines,
        in_specs=[SMEM] + [VMEM] * 4,
        flops=6 * group_rows * feature_width * width // 4,
    )
    their_kv = lax.ppermute(other_kv, "ctx", CORE_SWAP)
    their_q = lax.ppermute(other_q, "ctx", CORE_SWAP)
    behind_mine = lax.ppermute(my_kv, "ctx", z_shift(1))
    ahead_theirs = lax.ppermute(other_kv, "ctx", z_shift(-1, cross=True))
    behind_theirs = lax.ppermute(other_kv, "ctx", z_shift(1, cross=True))
    ahead_mine = lax.ppermute(my_kv, "ctx", z_shift(-1))
    q = (my_q, their_q)
    state = attend(q, (my_kv, their_kv))
    behind_mine, ahead_theirs, *state = lax.optimization_barrier(
        (behind_mine, ahead_theirs, *state)
    )
    far = (
        lax.ppermute(behind_mine, "ctx", z_shift(1)),
        lax.ppermute(ahead_theirs, "ctx", z_shift(-1)),
    )
    state = attend(q, (behind_mine, ahead_theirs), state)
    state = attend(q, (behind_theirs, ahead_mine), state)
    for_other = attend(q, far, state, 1)
    from_other = lax.ppermute(for_other, "ctx", CORE_SWAP)
    *far, for_other = lax.optimization_barrier((*far, for_other))
    own_head = attend(q, far, state, 0)
    heads_args = (where, own_head, from_other, out_weight)
    heads_specs = [SMEM, VMEM, VMEM, VMEM]
    far_top, far_bottom = call(
        far_partial_body,
        (half_line, half_line),
        *heads_args,
        in_specs=heads_specs,
        flops=group_rows * feature_width * width // 2,
    )
    kept, ahead_bottom, behind_top = call(
        near_partial_body,
        (jax.ShapeDtypeStruct((group_rows, SIDE * width), jnp.float32), half_line, half_line),
        *heads_args,
        in_specs=heads_specs,
        flops=group_rows * feature_width * width,
    )
    ahead_top, behind_bottom = call(
        relay_partial_body,
        (half_line, half_line),
        *heads_args,
        send(far_top, 1, 1),
        send(far_bottom, 1, -1),
        in_specs=heads_specs + [VMEM] * 2,
        flops=group_rows * feature_width * width // 2,
    )
    sums = call(
        add_line_body,
        [jax.ShapeDtypeStruct((group_rows, width), jnp.float32)] + [bf16(group_rows, width)] * 3,
        kept,
        send(ahead_top, 1, 1),
        send(behind_top, 1, -1),
        send(ahead_bottom, 1, 1),
        send(behind_bottom, 1, -1),
        in_specs=[VMEM] * 5,
    )
    blocks = scatter_line(sums)
    masks, _ = lax.optimization_barrier((masks, own_head))
    return_pick = call(
        return_pick_body,
        bf16(devices * per, group_rows),
        where,
        masks,
        in_specs=[SMEM, VMEM],
        flops=2 * devices * per * tok_rows * group_rows,
    )
    returning = call(
        send_back_body,
        bf16(devices * per, width),
        return_pick,
        *blocks,
        in_specs=[VMEM] * (1 + SIDE),
        flops=2 * devices * per * group_rows * width,
    )
    returned = lax.all_to_all(returning.reshape(devices, per, width), everyone, 0, 0, tiled=True)
    return pl.pallas_call(
        finish_body,
        out_shape=jax.ShapeDtypeStruct((tok_rows, feature_width), jnp.float32),
        in_specs=[VMEM] * 4,
        out_specs=HBM,
        scratch_shapes=[
            pltpu.VMEM((tok_rows, feature_width), jnp.float32),
            pltpu.SemaphoreType.DMA((4,)),
        ],
        compiler_params=pltpu.CompilerParams(vmem_limit_bytes=16 * MIB),
    )(pick, returned.reshape(seq_count, tok_rows, width), embedded, mask_token[None, :])


def solution(mesh):
    in_specs = (
        P(("seq", "ctx"), None),
        P(("seq", "ctx")),
        P(("seq", "ctx")),
        P(("seq", "ctx")),
        P(),
        P(),
        P(),
        P(None, None, "seq"),
        P("seq", None),
        P(),
    )
    out_specs = P(("seq", "ctx"), None)
    return jax.shard_map(local, mesh=mesh, in_specs=in_specs, out_specs=out_specs, check_vma=False)
```

```python
import functools
import itertools
import math

import jax
import jax.numpy as jnp
from jax import lax
from jax.experimental import pallas as pl
from jax.experimental.pallas import tpu as pltpu
from jax.sharding import PartitionSpec as P

HEAD_DIM = 128
EPSILON = 1e-06
SIDE = 4
MIB = 1 << 20


EVERYONE = ("seq", "ctx")


def plane_shift(leg, d):
    pairs = []
    for y, x, z, k in itertools.product(range(SIDE), range(SIDE), range(SIDE), range(2)):
        to = ((y + d) % SIDE, x) if leg == k else (y, (x + d) % SIDE)
        pairs.append(tuple(((v * SIDE + u) * SIDE + z) * 2 + k for v, u in ((y, x), to)))
    return pairs


def z_shift(d, cross=False):
    return [
        (z * 2 + k, (z + d) % SIDE * 2 + (1 - k if cross else k))
        for z in range(SIDE)
        for k in range(2)
    ]


CORE_SWAP = [(z * 2 + k, z * 2 + 1 - k) for z in range(SIDE) for k in range(2)]


RING = (0, 1, 3, 2)


def send(block, leg, d):
    return lax.ppermute(block, EVERYONE, plane_shift(leg, d))


def gather_line(block):
    return [block, send(block, 0, 2), send(block, 0, -1), send(block, 0, 1)]


def gather_long_line(top, bottom):
    behind_top, ahead_bottom = send(top, 1, 1), send(bottom, 1, -1)
    behind_bottom, ahead_top = send(bottom, 1, 1), send(top, 1, -1)
    far_top, far_bottom = send(behind_top, 1, 1), send(ahead_bottom, 1, -1)
    near = (top, bottom, ahead_top, ahead_bottom, behind_top, behind_bottom)
    return near, (far_top, far_bottom)


def scatter_line(blocks):
    own, ahead, behind, far = blocks
    return own, send(far, 0, 2), send(ahead, 0, 1), send(behind, 0, -1)


def call(body, outs, *args, scratch=(), limit=16, flops=0, in_specs=None):
    vmem = pl.BlockSpec(memory_space=pltpu.VMEM)
    many = isinstance(outs, (tuple, list))
    return pl.pallas_call(
        body,
        out_shape=outs,
        in_specs=in_specs,
        out_specs=[vmem] * len(outs) if many else vmem,
        scratch_shapes=list(scratch),
        compiler_params=pltpu.CompilerParams(vmem_limit_bytes=limit * MIB),
        cost_estimate=pl.CostEstimate(
            flops=flops, transcendentals=0, bytes_accessed=sum(a.size * 2 for a in args)
        ),
    )(*args)


VMEM = pl.BlockSpec(memory_space=pltpu.VMEM)
SMEM = pl.BlockSpec(memory_space=pltpu.SMEM)
ANY = pl.BlockSpec(memory_space=pl.ANY)
HBM = pl.BlockSpec(memory_space=pltpu.HBM)


def dot(a, b, dims=((1,), (0,))):
    return lax.dot_general(a, b, (dims, ((), ())), preferred_element_type=jnp.float32)


def iota(shape, dim):
    return lax.broadcasted_iota(jnp.int32, shape, dim)


def as_bf16(flag):
    return jnp.where(flag, 1.0, 0.0).astype(jnp.bfloat16)


def counts_in_lanes(masks):
    return dot(jnp.ones((8, masks.shape[1]), jnp.bfloat16), masks, ((1,), (1,)))


def repeat_body(row_ref, out_ref):
    out_ref[...] = jnp.broadcast_to(row_ref[...][None], out_ref.shape)


def dispatch_body(where_ref, masks_ref, own_ref, normed_ref, out_ref, pick_ref):
    tokens = own_ref.shape[1]
    masks = masks_ref[...].astype(jnp.float32).astype(jnp.bfloat16)
    counts = counts_in_lanes(masks)[0:1]
    start = jnp.sum(
        jnp.where(iota(counts.shape, 1) < where_ref[0], counts, 0.0), axis=1, keepdims=True
    ).astype(jnp.int32)
    own = own_ref[...]
    wide = jnp.broadcast_to(own.astype(jnp.float32).astype(jnp.bfloat16), (8, tokens))
    upto = as_bf16(iota((tokens, tokens), 0) <= iota((tokens, tokens), 1))
    rank = dot(wide, upto)[0:1].astype(jnp.int32) - 1
    slot = ((start + rank) & 7) * (tokens // 8) + (rank >> 3)
    slot = jnp.where(own == 1, slot, -1)
    pick = as_bf16(iota((tokens, tokens), 0) == slot)
    pick_ref[...] = pick
    width = out_ref.shape[2]
    for s in range(out_ref.shape[0]):
        out_ref[s] = dot(pick, normed_ref[:, s * width : (s + 1) * width]).astype(jnp.bfloat16)


def compact_body(where_ref, masks_ref, arrived_ref, out_ref):
    devices = masks_ref.shape[0]
    slots = arrived_ref.shape[0]
    per = slots // devices
    masks = masks_ref[...].astype(jnp.float32).astype(jnp.bfloat16)
    counts = counts_in_lanes(masks).astype(jnp.bfloat16)
    sender = iota((devices, slots), 1) // per
    device = iota((devices, slots), 0)
    start = dot(counts, as_bf16(device < sender))[0:1].astype(jnp.int32)
    count = dot(counts, as_bf16(device == sender))[0:1].astype(jnp.int32)
    offset = ((where_ref[1] - start) & 7) + 8 * (iota((1, slots), 1) % per)
    row = jnp.where(offset < count, (start + offset) >> 3, -1)
    arrived = arrived_ref[...]
    for r in range(0, out_ref.shape[0], 128):
        pick = as_bf16(iota((128, slots), 0) + r == row)
        out_ref[r : r + 128] = dot(pick, arrived).astype(jnp.bfloat16)


def line_body(*refs):
    blocks, (top_ref, bottom_ref) = refs[:-2], refs[-2:]
    half = top_ref.shape[0]
    width = blocks[0].shape[1]
    own, far, ahead, behind = blocks
    for i, block in enumerate((own, ahead, behind, far)):
        cols = slice(i * width, (i + 1) * width)
        top_ref[:, cols] = block[:half]
        bottom_ref[:, cols] = block[half:]


def plane_block(where_ref, outer, inner):
    first = where_ref[4] == 0
    y = jnp.where(first, RING[inner], RING[outer])
    x = jnp.where(first, RING[outer], RING[inner])
    return (where_ref[2] + y) % SIDE * SIDE + (where_ref[3] + x) % SIDE


def reorder_body(where_ref, weight_ref, out_ref, sems):
    width = weight_ref.shape[2]
    copies = []
    for outer in range(SIDE):
        for inner in range(SIDE):
            i = outer * SIDE + inner
            at = pl.multiple_of(plane_block(where_ref, outer, inner) * width, width)
            copies.append(
                pltpu.make_async_copy(
                    weight_ref.at[:, pl.ds(at, width), :],
                    out_ref.at[:, i * width : (i + 1) * width, :],
                    sems.at[i],
                )
            )
            copies[-1].start()
    for copy in copies:
        copy.wait()


def qkv_near_body(w_ref, *refs):
    lines, out_ref = refs[:-1], refs[-1]
    half, long = lines[0].shape
    for low in range(2):
        for t in range(3):
            total = None
            for i in range(3):
                product = dot(lines[2 * i + low][...], w_ref[t, i * long : (i + 1) * long])
                total = product if total is None else total + product
            out_ref[t, low * half : (low + 1) * half] = total


def qkv_far_body(where_ref, near_ref, w_ref, *refs):
    lines, (my_q, my_kv, other_q, other_kv) = refs[:2], refs[2:]
    half, long = lines[0].shape
    second = where_ref[4] == 1
    for low, line in enumerate(lines):
        rows = slice(low * half, (low + 1) * half)
        for t in range(3):
            total = near_ref[t, rows] + dot(line[...], w_ref[t, 3 * long :])
            both = total.astype(jnp.bfloat16)
            left, right = both[:, :HEAD_DIM], both[:, HEAD_DIM:]
            mine, other = (my_q, other_q) if t == 0 else (my_kv, other_kv)
            cols = slice(0, HEAD_DIM) if t < 2 else slice(HEAD_DIM, 2 * HEAD_DIM)
            mine[rows, cols] = jnp.where(second, right, left)
            other[rows, cols] = jnp.where(second, left, right)


def attend_body(has_state, last_side, keys, *refs):
    q_refs, kv_refs, refs = refs[:2], refs[2 : 2 + keys], refs[2 + keys :]
    state_refs, out_refs = (refs[:3], refs[3:]) if has_state else ((), refs)
    scale = math.log2(math.e) / math.sqrt(HEAD_DIM)
    rows = q_refs[0].shape[0]
    tile = min(rows, 512)
    per_side = rows // tile
    is_last = last_side is not None

    def one_tile(i):
        at = pl.ds(pl.multiple_of(i * tile, tile), tile)
        here = pl.ds(pl.multiple_of(i % per_side * tile, tile), tile)
        if is_last:
            q = q_refs[last_side][here]
        else:
            q = jnp.where(i < per_side, q_refs[0][here], q_refs[1][here])
        scores = [dot(q, kv_ref[:, :HEAD_DIM], ((1,), (1,))) for kv_ref in kv_refs]
        tops = [jnp.max(s, axis=1, keepdims=True) for s in scores]
        if has_state:
            acc = state_refs[0][at]
            top = state_refs[1][at][:, 0:1]
            total = state_refs[2][at][:, 0:1]
            tops.append(top)
        new_top = tops[0]
        for t in tops[1:]:
            new_top = jnp.maximum(new_top, t)
        product = block_total = None
        for s, kv_ref in zip(scores, kv_refs):
            expanded = jnp.exp2((s - new_top) * scale)
            part_total = jnp.sum(expanded, axis=1, keepdims=True)
            part = dot(expanded.astype(jnp.bfloat16), kv_ref[:, HEAD_DIM:])
            product = part if product is None else product + part
            block_total = part_total if block_total is None else block_total + part_total
        if has_state:
            factor = jnp.exp2((top - new_top) * scale)
            product = acc * factor + product
            block_total = total * factor + block_total
        if is_last:
            out_refs[0][here] = (product / block_total).astype(jnp.bfloat16)
        else:
            out_refs[0][at] = product
            out_refs[1][at] = jnp.broadcast_to(new_top, product.shape)
            out_refs[2][at] = jnp.broadcast_to(block_total, product.shape)

    if is_last:
        first_tile, tiles = last_side * per_side, per_side
    else:
        first_tile, tiles = 0, 2 * per_side
    lax.fori_loop(first_tile, first_tile + tiles, lambda i, _: one_tile(i), None)


def attend(q, kv_blocks, state=(), last_side=None):
    rows = q[0].shape[0]
    key_rows = sum(b.shape[0] for b in kv_blocks)
    kept = jax.ShapeDtypeStruct((2 * rows, HEAD_DIM), jnp.float32)
    last = jax.ShapeDtypeStruct((rows, HEAD_DIM), jnp.bfloat16)
    return call(
        functools.partial(attend_body, bool(state), last_side, len(kv_blocks)),
        (kept, kept, kept) if last_side is None else last,
        *q,
        *kv_blocks,
        *state,
        in_specs=[VMEM] * (2 + len(kv_blocks) + len(state)),
        flops=16 * rows * key_rows * HEAD_DIM,
    )


def return_pick_body(where_ref, masks_ref, pick_ref):
    devices = masks_ref.shape[0]
    slots, rows = pick_ref.shape
    per = slots // devices
    masks = masks_ref[...].astype(jnp.float32).astype(jnp.bfloat16)
    counts = dot(masks, jnp.ones((devices, 128), jnp.bfloat16)).astype(jnp.bfloat16)
    sender = iota((slots, devices), 0) // per
    device = iota((slots, devices), 1)
    start = dot(as_bf16(device < sender), counts).astype(jnp.int32)
    count = dot(as_bf16(device == sender), counts).astype(jnp.int32)
    offset = ((where_ref[1] - start) & 7) + 8 * (iota((slots, 128), 0) % per)
    row = jnp.where(offset < count, (start + offset) >> 3, -1)
    for r in range(0, rows, 128):
        pick_ref[:, r : r + 128] = as_bf16(row == iota((slots, 128), 1) + r)


def partial_line(where_ref, own_ref, other_ref, weight_ref, outer, rows):
    first = where_ref[4] == 0
    own, other = own_ref[rows], other_ref[rows]
    heads = jnp.concatenate([jnp.where(first, own, other), jnp.where(first, other, own)], axis=1)
    width = heads.shape[1]
    for inner in range(SIDE):
        at = pl.multiple_of(plane_block(where_ref, outer, inner) * width, width)
        cols = slice(inner * width, (inner + 1) * width)
        yield cols, dot(heads, weight_ref[:, pl.ds(at, width)])


def far_partial_body(*refs):
    args, (top_ref, bottom_ref) = refs[:4], refs[4:]
    half = top_ref.shape[0]
    for cols, product in partial_line(*args, 3, slice(None)):
        product = product.astype(jnp.bfloat16)
        top_ref[:, cols] = product[:half]
        bottom_ref[:, cols] = product[half:]


def near_partial_body(*refs):
    args, (kept_ref, ahead_ref, behind_ref, up_ref, down_ref) = refs[:4], refs[4:]
    half = ahead_ref.shape[0]
    for cols, product in partial_line(*args, 1, slice(None)):
        up_ref[:, cols] = product[:half]
        ahead_ref[:, cols] = product[half:].astype(jnp.bfloat16)
    for cols, product in partial_line(*args, 2, slice(None)):
        behind_ref[:, cols] = product[:half].astype(jnp.bfloat16)
        down_ref[:, cols] = product[half:]
    for cols, product in partial_line(*args, 0, slice(None)):
        kept_ref[:, cols] = product


def relay_partial_body(up_ref, down_ref, up_sent_ref, down_sent_ref, ahead_ref, behind_ref):
    ahead_ref[...] = (up_ref[...] + up_sent_ref[...].astype(jnp.float32)).astype(jnp.bfloat16)
    behind_ref[...] = (down_ref[...] + down_sent_ref[...].astype(jnp.float32)).astype(jnp.bfloat16)


def add_line_body(kept_ref, *refs):
    tops, bottoms, out_refs = refs[:2], refs[2:4], refs[4:]
    half = tops[0].shape[0]
    width = out_refs[0].shape[1]
    for low, pair in enumerate((tops, bottoms)):
        rows = slice(low * half, (low + 1) * half)
        for i, out_ref in enumerate(out_refs):
            cols = slice(i * width, (i + 1) * width)
            one, two = (r[:, cols].astype(jnp.float32) for r in pair)
            out_ref[rows] = (kept_ref[rows, cols] + (one + two)).astype(out_ref.dtype)


def send_back_body(pick_ref, *refs):
    blocks, out_ref = refs[:-1], refs[-1]
    a, b, c, d = (r[...].astype(jnp.float32) for r in blocks)
    projected = ((a + b) + (c + d)).astype(jnp.bfloat16)
    out_ref[...] = dot(pick_ref[...], projected).astype(jnp.bfloat16)


def finish_body(pick_ref, returned_ref, embedded_ref, filler_ref, out_ref, rows_ref, sems):
    pick = pick_ref[...]
    blocks, _, width = returned_ref.shape
    kept = dot(pick, jnp.ones((pick.shape[0], width), jnp.bfloat16), ((0,), (0,))) > 0.5
    group = blocks // sems.shape[0]
    copies = []
    for s in range(blocks):
        cols = slice(s * width, (s + 1) * width)
        projected = dot(pick, returned_ref[s], ((0,), (0,)))
        finished = embedded_ref[:, cols].astype(jnp.float32) + projected
        rows_ref[:, cols] = jnp.where(kept, finished, filler_ref[:, cols])
        if (s + 1) % group == 0:
            done = slice((s + 1 - group) * width, (s + 1) * width)
            copies.append(
                pltpu.make_async_copy(rows_ref.at[:, done], out_ref.at[:, done], sems.at[s // group])
            )
            copies[-1].start()
    for copy in copies:
        copy.wait()


def position_table(positions, feature_width):
    half_width = feature_width // 2
    frequency = jnp.exp(-math.log(10000.0) * jnp.arange(half_width, dtype=jnp.float32) / half_width)
    angles = positions.astype(jnp.float32)[:, None] * frequency[None, :]
    return jnp.concatenate([jnp.sin(angles), jnp.cos(angles)], axis=1)


def embed(tokens, modality, positions, modal_table):
    table_rows = jnp.where(modality[:, None] == 1, modal_table[1][None, :], modal_table[0][None, :])
    summed = tokens.astype(jnp.float32) + position_table(positions, tokens.shape[1]) + table_rows
    return summed.astype(jnp.bfloat16)


def layer_norm(embedded, norm_gain, norm_bias):
    values = embedded.astype(jnp.float32)
    row_mean = jnp.mean(values, axis=1, keepdims=True)
    centered = values - row_mean
    row_var = jnp.mean(centered * centered, axis=1, keepdims=True)
    return (centered * lax.rsqrt(row_var + EPSILON) * norm_gain + norm_bias).astype(jnp.bfloat16)


def local(
    tokens,
    modality,
    keep_mask,
    positions,
    modal_table,
    norm_gain,
    norm_bias,
    qkv_weight,
    out_weight,
    mask_token,
):
    tok_rows, feature_width = tokens.shape
    seq_count = lax.axis_size("seq")
    ctx_count = lax.axis_size("ctx")
    devices = seq_count * ctx_count
    everyone = ("seq", "ctx")
    seq, ctx = lax.axis_index("seq"), lax.axis_index("ctx")
    core = ctx % 2
    where = jnp.stack([seq * ctx_count + ctx, ctx, seq // SIDE, seq % SIDE, core]).astype(jnp.int32)
    group_rows = tok_rows * seq_count // 4
    width = feature_width // seq_count
    per = tok_rows // ctx_count
    bf16 = lambda *shape: jax.ShapeDtypeStruct(shape, jnp.bfloat16)

    masks = call(
        repeat_body,
        jax.ShapeDtypeStruct((devices, 1, tok_rows), jnp.int32),
        keep_mask[None, :],
        in_specs=[VMEM],
    )
    masks = lax.all_to_all(masks, everyone, 0, 0, tiled=True).reshape(devices, tok_rows)
    embedded = embed(tokens, modality, positions, modal_table)
    normed = layer_norm(embedded, norm_gain, norm_bias)
    outgoing, pick = call(
        dispatch_body,
        (bf16(seq_count, tok_rows, width), bf16(tok_rows, tok_rows)),
        where,
        masks,
        keep_mask[None, :],
        normed,
        in_specs=[SMEM, VMEM, VMEM, VMEM],
        flops=2 * tok_rows * tok_rows * feature_width,
    )
    arrived = lax.all_to_all(outgoing.reshape(devices, per, width), everyone, 0, 0, tiled=True)
    block = call(
        compact_body,
        bf16(group_rows, width),
        where,
        masks,
        arrived.reshape(devices * per, width),
        in_specs=[SMEM, VMEM, VMEM],
        flops=2 * group_rows * devices * per * width,
    )
    half_line = bf16(group_rows // 2, SIDE * width)
    blocks = gather_line(block)
    qkv_weight, block = lax.optimization_barrier((qkv_weight, block))
    ordered = call(
        reorder_body,
        bf16(*qkv_weight.shape),
        where,
        qkv_weight,
        in_specs=[SMEM, HBM],
        scratch=(pltpu.SemaphoreType.DMA((SIDE * SIDE,)),),
        flops=1 << 32,
    )
    *blocks, ordered = lax.optimization_barrier((*blocks, ordered))
    line = call(line_body, (half_line, half_line), *blocks, in_specs=[VMEM] * SIDE)
    near_lines, far_lines = gather_long_line(*line)
    near = call(
        qkv_near_body,
        jax.ShapeDtypeStruct((3, group_rows, width), jnp.float32),
        ordered,
        *near_lines,
        in_specs=[VMEM] * 7,
        flops=6 * group_rows * feature_width * width * 3 // 4,
    )
    row_q, row_kv = bf16(group_rows, HEAD_DIM), bf16(group_rows, 2 * HEAD_DIM)
    my_q, my_kv, other_q, other_kv = call(
        qkv_far_body,
        (row_q, row_kv, row_q, row_kv),
        where,
        near,
        ordered,
        *far_lines,
        in_specs=[SMEM] + [VMEM] * 4,
        flops=6 * group_rows * feature_width * width // 4,
    )
    their_kv = lax.ppermute(other_kv, "ctx", CORE_SWAP)
    their_q = lax.ppermute(other_q, "ctx", CORE_SWAP)
    behind_mine = lax.ppermute(my_kv, "ctx", z_shift(1))
    ahead_theirs = lax.ppermute(other_kv, "ctx", z_shift(-1, cross=True))
    behind_theirs = lax.ppermute(other_kv, "ctx", z_shift(1, cross=True))
    ahead_mine = lax.ppermute(my_kv, "ctx", z_shift(-1))
    q = (my_q, their_q)
    state = attend(q, (my_kv, their_kv))
    behind_mine, ahead_theirs, *state = lax.optimization_barrier(
        (behind_mine, ahead_theirs, *state)
    )
    far = (
        lax.ppermute(behind_mine, "ctx", z_shift(1)),
        lax.ppermute(ahead_theirs, "ctx", z_shift(-1)),
    )
    state = attend(q, (behind_mine, ahead_theirs), state)
    state = attend(q, (behind_theirs, ahead_mine), state)
    for_other = attend(q, far, state, 1)
    from_other = lax.ppermute(for_other, "ctx", CORE_SWAP)
    *far, for_other = lax.optimization_barrier((*far, for_other))
    own_head = attend(q, far, state, 0)
    heads_args = (where, own_head, from_other, out_weight)
    heads_specs = [SMEM, VMEM, VMEM, VMEM]
    far_top, far_bottom = call(
        far_partial_body,
        (half_line, half_line),
        *heads_args,
        in_specs=heads_specs,
        flops=group_rows * feature_width * width // 2,
    )
    half_sum = jax.ShapeDtypeStruct(half_line.shape, jnp.float32)
    kept, ahead_bottom, behind_top, up, down = call(
        near_partial_body,
        (
            jax.ShapeDtypeStruct((group_rows, SIDE * width), jnp.float32),
            half_line,
            half_line,
            half_sum,
            half_sum,
        ),
        *heads_args,
        in_specs=heads_specs,
        flops=group_rows * feature_width * width * 3 // 2,
    )
    ahead_top, behind_bottom = call(
        relay_partial_body,
        (half_line, half_line),
        up,
        down,
        send(far_top, 1, 1),
        send(far_bottom, 1, -1),
        in_specs=[VMEM] * 4,
    )
    sums = call(
        add_line_body,
        [jax.ShapeDtypeStruct((group_rows, width), jnp.float32)] + [bf16(group_rows, width)] * 3,
        kept,
        send(ahead_top, 1, 1),
        send(behind_top, 1, -1),
        send(ahead_bottom, 1, 1),
        send(behind_bottom, 1, -1),
        in_specs=[VMEM] * 5,
    )
    blocks = scatter_line(sums)
    masks, _ = lax.optimization_barrier((masks, own_head))
    return_pick = call(
        return_pick_body,
        bf16(devices * per, group_rows),
        where,
        masks,
        in_specs=[SMEM, VMEM],
        flops=2 * devices * per * tok_rows * group_rows,
    )
    returning = call(
        send_back_body,
        bf16(devices * per, width),
        return_pick,
        *blocks,
        in_specs=[VMEM] * (1 + SIDE),
        flops=2 * devices * per * group_rows * width,
    )
    returned = lax.all_to_all(returning.reshape(devices, per, width), everyone, 0, 0, tiled=True)
    return pl.pallas_call(
        finish_body,
        out_shape=jax.ShapeDtypeStruct((tok_rows, feature_width), jnp.float32),
        in_specs=[VMEM] * 4,
        out_specs=HBM,
        scratch_shapes=[
            pltpu.VMEM((tok_rows, feature_width), jnp.float32),
            pltpu.SemaphoreType.DMA((4,)),
        ],
        compiler_params=pltpu.CompilerParams(vmem_limit_bytes=16 * MIB),
    )(pick, returned.reshape(seq_count, tok_rows, width), embedded, mask_token[None, :])


def solution(mesh):
    in_specs = (
        P(("seq", "ctx"), None),
        P(("seq", "ctx")),
        P(("seq", "ctx")),
        P(("seq", "ctx")),
        P(),
        P(),
        P(),
        P(None, None, "seq"),
        P("seq", None),
        P(),
    )
    out_specs = P(("seq", "ctx"), None)
    return jax.shard_map(local, mesh=mesh, in_specs=in_specs, out_specs=out_specs, check_vma=False)
```

```python
import functools
import itertools
import math

import jax
import jax.numpy as jnp
from jax import lax
from jax.experimental import pallas as pl
from jax.experimental.pallas import tpu as pltpu
from jax.sharding import PartitionSpec as P

HEAD_DIM = 128
EPSILON = 1e-06
SIDE = 4
MIB = 1 << 20


EVERYONE = ("seq", "ctx")


def plane_shift(leg, d):
    pairs = []
    for y, x, z, k in itertools.product(range(SIDE), range(SIDE), range(SIDE), range(2)):
        to = ((y + d) % SIDE, x) if leg == k else (y, (x + d) % SIDE)
        pairs.append(tuple(((v * SIDE + u) * SIDE + z) * 2 + k for v, u in ((y, x), to)))
    return pairs


def z_shift(d, cross=False):
    return [
        (z * 2 + k, (z + d) % SIDE * 2 + (1 - k if cross else k))
        for z in range(SIDE)
        for k in range(2)
    ]


CORE_SWAP = [(z * 2 + k, z * 2 + 1 - k) for z in range(SIDE) for k in range(2)]


RING = (0, 1, 3, 2)


def send(block, leg, d):
    return lax.ppermute(block, EVERYONE, plane_shift(leg, d))


def gather_line(block):
    return [block, send(block, 0, 2), send(block, 0, -1), send(block, 0, 1)]


def gather_long_line(top, bottom):
    behind_top, ahead_bottom = send(top, 1, 1), send(bottom, 1, -1)
    behind_bottom, ahead_top = send(bottom, 1, 1), send(top, 1, -1)
    far_top, far_bottom = send(behind_top, 1, 1), send(ahead_bottom, 1, -1)
    near = (top, bottom, ahead_top, ahead_bottom, behind_top, behind_bottom)
    return near, (far_top, far_bottom)


def scatter_line(blocks):
    own, ahead, behind, far = blocks
    return own, send(far, 0, 2), send(ahead, 0, 1), send(behind, 0, -1)


def call(body, outs, *args, scratch=(), limit=16, flops=0, in_specs=None):
    vmem = pl.BlockSpec(memory_space=pltpu.VMEM)
    many = isinstance(outs, (tuple, list))
    return pl.pallas_call(
        body,
        out_shape=outs,
        in_specs=in_specs,
        out_specs=[vmem] * len(outs) if many else vmem,
        scratch_shapes=list(scratch),
        compiler_params=pltpu.CompilerParams(vmem_limit_bytes=limit * MIB),
        cost_estimate=pl.CostEstimate(
            flops=flops, transcendentals=0, bytes_accessed=sum(a.size * 2 for a in args)
        ),
    )(*args)


VMEM = pl.BlockSpec(memory_space=pltpu.VMEM)
SMEM = pl.BlockSpec(memory_space=pltpu.SMEM)
ANY = pl.BlockSpec(memory_space=pl.ANY)
HBM = pl.BlockSpec(memory_space=pltpu.HBM)


def dot(a, b, dims=((1,), (0,))):
    return lax.dot_general(a, b, (dims, ((), ())), preferred_element_type=jnp.float32)


def iota(shape, dim):
    return lax.broadcasted_iota(jnp.int32, shape, dim)


def as_bf16(flag):
    return jnp.where(flag, 1.0, 0.0).astype(jnp.bfloat16)


def counts_in_lanes(masks):
    return dot(jnp.ones((8, masks.shape[1]), jnp.bfloat16), masks, ((1,), (1,)))


def repeat_body(row_ref, out_ref):
    out_ref[...] = jnp.broadcast_to(row_ref[...][None], out_ref.shape)


def dispatch_body(where_ref, masks_ref, own_ref, normed_ref, out_ref, pick_ref):
    tokens = own_ref.shape[1]
    masks = masks_ref[...].astype(jnp.float32).astype(jnp.bfloat16)
    counts = counts_in_lanes(masks)[0:1]
    start = jnp.sum(
        jnp.where(iota(counts.shape, 1) < where_ref[0], counts, 0.0), axis=1, keepdims=True
    ).astype(jnp.int32)
    own = own_ref[...]
    wide = jnp.broadcast_to(own.astype(jnp.float32).astype(jnp.bfloat16), (8, tokens))
    upto = as_bf16(iota((tokens, tokens), 0) <= iota((tokens, tokens), 1))
    rank = dot(wide, upto)[0:1].astype(jnp.int32) - 1
    slot = ((start + rank) & 7) * (tokens // 8) + (rank >> 3)
    slot = jnp.where(own == 1, slot, -1)
    pick = as_bf16(iota((tokens, tokens), 0) == slot)
    pick_ref[...] = pick
    width = out_ref.shape[2]
    for s in range(out_ref.shape[0]):
        out_ref[s] = dot(pick, normed_ref[:, s * width : (s + 1) * width]).astype(jnp.bfloat16)


def compact_body(where_ref, masks_ref, arrived_ref, out_ref):
    devices = masks_ref.shape[0]
    slots = arrived_ref.shape[0]
    per = slots // devices
    masks = masks_ref[...].astype(jnp.float32).astype(jnp.bfloat16)
    counts = counts_in_lanes(masks).astype(jnp.bfloat16)
    sender = iota((devices, slots), 1) // per
    device = iota((devices, slots), 0)
    start = dot(counts, as_bf16(device < sender))[0:1].astype(jnp.int32)
    count = dot(counts, as_bf16(device == sender))[0:1].astype(jnp.int32)
    offset = ((where_ref[1] - start) & 7) + 8 * (iota((1, slots), 1) % per)
    row = jnp.where(offset < count, (start + offset) >> 3, -1)
    arrived = arrived_ref[...]
    for r in range(0, out_ref.shape[0], 128):
        pick = as_bf16(iota((128, slots), 0) + r == row)
        out_ref[r : r + 128] = dot(pick, arrived).astype(jnp.bfloat16)


def line_body(*refs):
    blocks, (top_ref, bottom_ref) = refs[:-2], refs[-2:]
    half = top_ref.shape[0]
    width = blocks[0].shape[1]
    own, far, ahead, behind = blocks
    for i, block in enumerate((own, ahead, behind, far)):
        cols = slice(i * width, (i + 1) * width)
        top_ref[:, cols] = block[:half]
        bottom_ref[:, cols] = block[half:]


def plane_block(where_ref, outer, inner):
    first = where_ref[4] == 0
    y = jnp.where(first, RING[inner], RING[outer])
    x = jnp.where(first, RING[outer], RING[inner])
    return (where_ref[2] + y) % SIDE * SIDE + (where_ref[3] + x) % SIDE


def reorder_body(where_ref, weight_ref, out_ref, sems):
    width = weight_ref.shape[2]
    copies = []
    for outer in range(SIDE):
        for inner in range(SIDE):
            i = outer * SIDE + inner
            at = pl.multiple_of(plane_block(where_ref, outer, inner) * width, width)
            copies.append(
                pltpu.make_async_copy(
                    weight_ref.at[:, pl.ds(at, width), :],
                    out_ref.at[:, i * width : (i + 1) * width, :],
                    sems.at[i],
                )
            )
            copies[-1].start()
    for copy in copies:
        copy.wait()


def qkv_near_body(w_ref, *refs):
    lines, out_ref = refs[:-1], refs[-1]
    half, long = lines[0].shape
    for low in range(2):
        for t in range(3):
            total = None
            for i in range(3):
                product = dot(lines[2 * i + low][...], w_ref[t, i * long : (i + 1) * long])
                total = product if total is None else total + product
            out_ref[t, low * half : (low + 1) * half] = total


def qkv_far_body(where_ref, near_ref, w_ref, *refs):
    lines, (my_q, my_kv, other_q, other_kv) = refs[:2], refs[2:]
    half, long = lines[0].shape
    second = where_ref[4] == 1
    for low, line in enumerate(lines):
        rows = slice(low * half, (low + 1) * half)
        for t in range(3):
            total = near_ref[t, rows] + dot(line[...], w_ref[t, 3 * long :])
            both = total.astype(jnp.bfloat16)
            left, right = both[:, :HEAD_DIM], both[:, HEAD_DIM:]
            mine, other = (my_q, other_q) if t == 0 else (my_kv, other_kv)
            cols = slice(0, HEAD_DIM) if t < 2 else slice(HEAD_DIM, 2 * HEAD_DIM)
            mine[rows, cols] = jnp.where(second, right, left)
            other[rows, cols] = jnp.where(second, left, right)


def attend_body(has_state, last_side, keys, *refs):
    q_refs, kv_refs, refs = refs[:2], refs[2 : 2 + keys], refs[2 + keys :]
    state_refs, out_refs = (refs[:3], refs[3:]) if has_state else ((), refs)
    scale = math.log2(math.e) / math.sqrt(HEAD_DIM)
    rows = q_refs[0].shape[0]
    tile = 256
    per_side = rows // tile
    is_last = last_side is not None

    def one_tile(i):
        at = pl.ds(pl.multiple_of(i * tile, tile), tile)
        here = pl.ds(pl.multiple_of(i % per_side * tile, tile), tile)
        if is_last:
            q = q_refs[last_side][here]
        else:
            q = jnp.where(i < per_side, q_refs[0][here], q_refs[1][here])
        scores = [dot(q, kv_ref[:, :HEAD_DIM], ((1,), (1,))) for kv_ref in kv_refs]
        tops = [jnp.max(s, axis=1, keepdims=True) for s in scores]
        if has_state:
            acc = state_refs[0][at]
            top = state_refs[1][at][:, 0:1]
            total = state_refs[2][at][:, 0:1]
            tops.append(top)
        new_top = tops[0]
        for t in tops[1:]:
            new_top = jnp.maximum(new_top, t)
        product = block_total = None
        for s, kv_ref in zip(scores, kv_refs):
            expanded = jnp.exp2((s - new_top) * scale)
            part_total = jnp.sum(expanded, axis=1, keepdims=True)
            part = dot(expanded.astype(jnp.bfloat16), kv_ref[:, HEAD_DIM:])
            product = part if product is None else product + part
            block_total = part_total if block_total is None else block_total + part_total
        if has_state:
            factor = jnp.exp2((top - new_top) * scale)
            product = acc * factor + product
            block_total = total * factor + block_total
        if is_last:
            out_refs[0][here] = (product / block_total).astype(jnp.bfloat16)
        else:
            out_refs[0][at] = product
            out_refs[1][at] = jnp.broadcast_to(new_top, product.shape)
            out_refs[2][at] = jnp.broadcast_to(block_total, product.shape)

    if is_last:
        first_tile, tiles = last_side * per_side, per_side
    else:
        first_tile, tiles = 0, 2 * per_side
    lax.fori_loop(first_tile, first_tile + tiles, lambda i, _: one_tile(i), None)


def attend(q, kv_blocks, state=(), last_side=None):
    rows = q[0].shape[0]
    key_rows = sum(b.shape[0] for b in kv_blocks)
    kept = jax.ShapeDtypeStruct((2 * rows, HEAD_DIM), jnp.float32)
    last = jax.ShapeDtypeStruct((rows, HEAD_DIM), jnp.bfloat16)
    return call(
        functools.partial(attend_body, bool(state), last_side, len(kv_blocks)),
        (kept, kept, kept) if last_side is None else last,
        *q,
        *kv_blocks,
        *state,
        in_specs=[VMEM] * (2 + len(kv_blocks) + len(state)),
        flops=16 * rows * key_rows * HEAD_DIM,
    )


def return_pick_body(where_ref, masks_ref, pick_ref):
    devices = masks_ref.shape[0]
    slots, rows = pick_ref.shape
    per = slots // devices
    masks = masks_ref[...].astype(jnp.float32).astype(jnp.bfloat16)
    counts = dot(masks, jnp.ones((devices, 128), jnp.bfloat16)).astype(jnp.bfloat16)
    sender = iota((slots, devices), 0) // per
    device = iota((slots, devices), 1)
    start = dot(as_bf16(device < sender), counts).astype(jnp.int32)
    count = dot(as_bf16(device == sender), counts).astype(jnp.int32)
    offset = ((where_ref[1] - start) & 7) + 8 * (iota((slots, 128), 0) % per)
    row = jnp.where(offset < count, (start + offset) >> 3, -1)
    for r in range(0, rows, 128):
        pick_ref[:, r : r + 128] = as_bf16(row == iota((slots, 128), 1) + r)


def partial_line(where_ref, own_ref, other_ref, weight_ref, outer, rows):
    first = where_ref[4] == 0
    own, other = own_ref[rows], other_ref[rows]
    heads = jnp.concatenate([jnp.where(first, own, other), jnp.where(first, other, own)], axis=1)
    width = heads.shape[1]
    for inner in range(SIDE):
        at = pl.multiple_of(plane_block(where_ref, outer, inner) * width, width)
        cols = slice(inner * width, (inner + 1) * width)
        yield cols, dot(heads, weight_ref[:, pl.ds(at, width)])


def far_partial_body(*refs):
    args, (top_ref, bottom_ref) = refs[:4], refs[4:]
    half = top_ref.shape[0]
    for cols, product in partial_line(*args, 3, slice(None)):
        product = product.astype(jnp.bfloat16)
        top_ref[:, cols] = product[:half]
        bottom_ref[:, cols] = product[half:]


def near_partial_body(*refs):
    args, (kept_ref, ahead_ref, behind_ref, up_ref, down_ref) = refs[:4], refs[4:]
    half = ahead_ref.shape[0]
    for cols, product in partial_line(*args, 1, slice(None)):
        up_ref[:, cols] = product[:half]
        ahead_ref[:, cols] = product[half:].astype(jnp.bfloat16)
    for cols, product in partial_line(*args, 2, slice(None)):
        behind_ref[:, cols] = product[:half].astype(jnp.bfloat16)
        down_ref[:, cols] = product[half:]
    for cols, product in partial_line(*args, 0, slice(None)):
        kept_ref[:, cols] = product


def relay_partial_body(up_ref, down_ref, up_sent_ref, down_sent_ref, ahead_ref, behind_ref):
    ahead_ref[...] = (up_ref[...] + up_sent_ref[...].astype(jnp.float32)).astype(jnp.bfloat16)
    behind_ref[...] = (down_ref[...] + down_sent_ref[...].astype(jnp.float32)).astype(jnp.bfloat16)


def add_line_body(kept_ref, *refs):
    tops, bottoms, out_refs = refs[:2], refs[2:4], refs[4:]
    half = tops[0].shape[0]
    width = out_refs[0].shape[1]
    for low, pair in enumerate((tops, bottoms)):
        rows = slice(low * half, (low + 1) * half)
        for i, out_ref in enumerate(out_refs):
            cols = slice(i * width, (i + 1) * width)
            one, two = (r[:, cols].astype(jnp.float32) for r in pair)
            out_ref[rows] = (kept_ref[rows, cols] + (one + two)).astype(out_ref.dtype)


def send_back_body(pick_ref, *refs):
    blocks, out_ref = refs[:-1], refs[-1]
    a, b, c, d = (r[...].astype(jnp.float32) for r in blocks)
    projected = ((a + b) + (c + d)).astype(jnp.bfloat16)
    out_ref[...] = dot(pick_ref[...], projected).astype(jnp.bfloat16)


def finish_body(pick_ref, returned_ref, embedded_ref, filler_ref, out_ref, rows_ref, sems):
    pick = pick_ref[...]
    blocks, _, width = returned_ref.shape
    kept = dot(pick, jnp.ones((pick.shape[0], width), jnp.bfloat16), ((0,), (0,))) > 0.5
    group = blocks // sems.shape[0]
    copies = []
    for s in range(blocks):
        cols = slice(s * width, (s + 1) * width)
        projected = dot(pick, returned_ref[s], ((0,), (0,)))
        finished = embedded_ref[:, cols].astype(jnp.float32) + projected
        rows_ref[:, cols] = jnp.where(kept, finished, filler_ref[:, cols])
        if (s + 1) % group == 0:
            done = slice((s + 1 - group) * width, (s + 1) * width)
            copies.append(
                pltpu.make_async_copy(rows_ref.at[:, done], out_ref.at[:, done], sems.at[s // group])
            )
            copies[-1].start()
    for copy in copies:
        copy.wait()


def position_table(positions, feature_width):
    half_width = feature_width // 2
    frequency = jnp.exp(-math.log(10000.0) * jnp.arange(half_width, dtype=jnp.float32) / half_width)
    angles = positions.astype(jnp.float32)[:, None] * frequency[None, :]
    return jnp.concatenate([jnp.sin(angles), jnp.cos(angles)], axis=1)


def embed(tokens, modality, positions, modal_table):
    table_rows = jnp.where(modality[:, None] == 1, modal_table[1][None, :], modal_table[0][None, :])
    summed = tokens.astype(jnp.float32) + position_table(positions, tokens.shape[1]) + table_rows
    return summed.astype(jnp.bfloat16)


def layer_norm(embedded, norm_gain, norm_bias):
    values = embedded.astype(jnp.float32)
    row_mean = jnp.mean(values, axis=1, keepdims=True)
    centered = values - row_mean
    row_var = jnp.mean(centered * centered, axis=1, keepdims=True)
    return (centered * lax.rsqrt(row_var + EPSILON) * norm_gain + norm_bias).astype(jnp.bfloat16)


def local(
    tokens,
    modality,
    keep_mask,
    positions,
    modal_table,
    norm_gain,
    norm_bias,
    qkv_weight,
    out_weight,
    mask_token,
):
    tok_rows, feature_width = tokens.shape
    seq_count = lax.axis_size("seq")
    ctx_count = lax.axis_size("ctx")
    devices = seq_count * ctx_count
    everyone = ("seq", "ctx")
    seq, ctx = lax.axis_index("seq"), lax.axis_index("ctx")
    core = ctx % 2
    where = jnp.stack([seq * ctx_count + ctx, ctx, seq // SIDE, seq % SIDE, core]).astype(jnp.int32)
    group_rows = tok_rows * seq_count // 4
    width = feature_width // seq_count
    per = tok_rows // ctx_count
    bf16 = lambda *shape: jax.ShapeDtypeStruct(shape, jnp.bfloat16)

    masks = call(
        repeat_body,
        jax.ShapeDtypeStruct((devices, 1, tok_rows), jnp.int32),
        keep_mask[None, :],
        in_specs=[VMEM],
    )
    masks = lax.all_to_all(masks, everyone, 0, 0, tiled=True).reshape(devices, tok_rows)
    embedded = embed(tokens, modality, positions, modal_table)
    normed = layer_norm(embedded, norm_gain, norm_bias)
    outgoing, pick = call(
        dispatch_body,
        (bf16(seq_count, tok_rows, width), bf16(tok_rows, tok_rows)),
        where,
        masks,
        keep_mask[None, :],
        normed,
        in_specs=[SMEM, VMEM, VMEM, VMEM],
        flops=2 * tok_rows * tok_rows * feature_width,
    )
    arrived = lax.all_to_all(outgoing.reshape(devices, per, width), everyone, 0, 0, tiled=True)
    block = call(
        compact_body,
        bf16(group_rows, width),
        where,
        masks,
        arrived.reshape(devices * per, width),
        in_specs=[SMEM, VMEM, VMEM],
        flops=2 * group_rows * devices * per * width,
    )
    half_line = bf16(group_rows // 2, SIDE * width)
    blocks = gather_line(block)
    qkv_weight, block = lax.optimization_barrier((qkv_weight, block))
    ordered = call(
        reorder_body,
        bf16(*qkv_weight.shape),
        where,
        qkv_weight,
        in_specs=[SMEM, HBM],
        scratch=(pltpu.SemaphoreType.DMA((SIDE * SIDE,)),),
        flops=1 << 32,
    )
    *blocks, ordered = lax.optimization_barrier((*blocks, ordered))
    line = call(line_body, (half_line, half_line), *blocks, in_specs=[VMEM] * SIDE)
    near_lines, far_lines = gather_long_line(*line)
    near = call(
        qkv_near_body,
        jax.ShapeDtypeStruct((3, group_rows, width), jnp.float32),
        ordered,
        *near_lines,
        in_specs=[VMEM] * 7,
        flops=6 * group_rows * feature_width * width * 3 // 4,
    )
    row_q, row_kv = bf16(group_rows, HEAD_DIM), bf16(group_rows, 2 * HEAD_DIM)
    my_q, my_kv, other_q, other_kv = call(
        qkv_far_body,
        (row_q, row_kv, row_q, row_kv),
        where,
        near,
        ordered,
        *far_lines,
        in_specs=[SMEM] + [VMEM] * 4,
        flops=6 * group_rows * feature_width * width // 4,
    )
    their_kv = lax.ppermute(other_kv, "ctx", CORE_SWAP)
    their_q = lax.ppermute(other_q, "ctx", CORE_SWAP)
    behind_mine = lax.ppermute(my_kv, "ctx", z_shift(1))
    ahead_theirs = lax.ppermute(other_kv, "ctx", z_shift(-1, cross=True))
    behind_theirs = lax.ppermute(other_kv, "ctx", z_shift(1, cross=True))
    ahead_mine = lax.ppermute(my_kv, "ctx", z_shift(-1))
    q = (my_q, their_q)
    state = attend(q, (my_kv, their_kv))
    behind_mine, ahead_theirs, *state = lax.optimization_barrier(
        (behind_mine, ahead_theirs, *state)
    )
    far = (
        lax.ppermute(behind_mine, "ctx", z_shift(1)),
        lax.ppermute(ahead_theirs, "ctx", z_shift(-1)),
    )
    state = attend(q, (behind_mine, ahead_theirs), state)
    state = attend(q, (behind_theirs, ahead_mine), state)
    for_other = attend(q, far, state, 1)
    from_other = lax.ppermute(for_other, "ctx", CORE_SWAP)
    *far, for_other = lax.optimization_barrier((*far, for_other))
    own_head = attend(q, far, state, 0)
    heads_args = (where, own_head, from_other, out_weight)
    heads_specs = [SMEM, VMEM, VMEM, VMEM]
    far_top, far_bottom = call(
        far_partial_body,
        (half_line, half_line),
        *heads_args,
        in_specs=heads_specs,
        flops=group_rows * feature_width * width // 2,
    )
    half_sum = jax.ShapeDtypeStruct(half_line.shape, jnp.float32)
    kept, ahead_bottom, behind_top, up, down = call(
        near_partial_body,
        (
            jax.ShapeDtypeStruct((group_rows, SIDE * width), jnp.float32),
            half_line,
            half_line,
            half_sum,
            half_sum,
        ),
        *heads_args,
        in_specs=heads_specs,
        flops=group_rows * feature_width * width * 3 // 2,
    )
    ahead_top, behind_bottom = call(
        relay_partial_body,
        (half_line, half_line),
        up,
        down,
        send(far_top, 1, 1),
        send(far_bottom, 1, -1),
        in_specs=[VMEM] * 4,
    )
    sums = call(
        add_line_body,
        [jax.ShapeDtypeStruct((group_rows, width), jnp.float32)] + [bf16(group_rows, width)] * 3,
        kept,
        send(ahead_top, 1, 1),
        send(behind_top, 1, -1),
        send(ahead_bottom, 1, 1),
        send(behind_bottom, 1, -1),
        in_specs=[VMEM] * 5,
    )
    blocks = scatter_line(sums)
    masks, _ = lax.optimization_barrier((masks, own_head))
    return_pick = call(
        return_pick_body,
        bf16(devices * per, group_rows),
        where,
        masks,
        in_specs=[SMEM, VMEM],
        flops=2 * devices * per * tok_rows * group_rows,
    )
    returning = call(
        send_back_body,
        bf16(devices * per, width),
        return_pick,
        *blocks,
        in_specs=[VMEM] * (1 + SIDE),
        flops=2 * devices * per * group_rows * width,
    )
    returned = lax.all_to_all(returning.reshape(devices, per, width), everyone, 0, 0, tiled=True)
    return pl.pallas_call(
        finish_body,
        out_shape=jax.ShapeDtypeStruct((tok_rows, feature_width), jnp.float32),
        in_specs=[VMEM] * 4,
        out_specs=HBM,
        scratch_shapes=[
            pltpu.VMEM((tok_rows, feature_width), jnp.float32),
            pltpu.SemaphoreType.DMA((4,)),
        ],
        compiler_params=pltpu.CompilerParams(vmem_limit_bytes=16 * MIB),
    )(pick, returned.reshape(seq_count, tok_rows, width), embedded, mask_token[None, :])


def solution(mesh):
    in_specs = (
        P(("seq", "ctx"), None),
        P(("seq", "ctx")),
        P(("seq", "ctx")),
        P(("seq", "ctx")),
        P(),
        P(),
        P(),
        P(None, None, "seq"),
        P("seq", None),
        P(),
    )
    out_specs = P(("seq", "ctx"), None)
    return jax.shard_map(local, mesh=mesh, in_specs=in_specs, out_specs=out_specs, check_vma=False)
```
